128 devices in a mesh: box: 8 (over z, y_lo), dir: 16 (over y_hi, x, core).
Axes of the slice: x: 4, y: 4 (y_hi: 2, y_lo: 2; y = y_hi * 2 + y_lo), z: 4, core: 2. Of those that a mesh axis runs over, the one named last changes fastest.
Arguments:
- leaf_out: bfloat16 [2, 8192, 1024], P(None, ('box', 'dir')), may hold values from -6 to 6
- interp_mid: bfloat16 [1024, 4096], replicated, may hold values from -0.1875 to 0.1875
- shift_mid: float32 [8, 4096], replicated, may hold values from -3.140625 to 3.140625
- trans_mid: float32 [2, 316, 4096], P(None, None, 'dir'), may hold values from -0.5 to 0.5
- list_mid: int32 [1024, 64], replicated, may hold values from 0 to 1023
- offset_mid: int32 [1024, 64], replicated, may hold values from 0 to 315
- interp_top: bfloat16 [16, 256, 1024], P('dir'), may hold values from -0.375 to 0.375
- shift_top: float32 [8, 16, 1024], P(None, 'dir'), may hold values from -3.140625 to 3.140625
- trans_top: float32 [2, 316, 16, 1024], P(None, None, 'dir', 'box'), may hold values from -0.5 to 0.5
- list_top: int32 [128, 64], replicated, may hold values from 0 to 127
- offset_top: int32 [128, 64], replicated, may hold values from 0 to 315
Outputs:
- leaf_in: float32 [2, 8192, 1024], P(None, ('box', 'dir'))
The draws below stay inside these ranges and needn't reach their ends.
Inputs may be any that keep to these rules, and one draw needn't show every extreme that they name: `list_mid`: middle box indices. `offset_mid`: offset indices. `list_top`: top box indices. `offset_top`: offset indices.
All inputs are finite; a program needn't handle non-finite values.
Results may differ from the reference program's by a relative error of at most 0.014.
Values may be sent and summed in bfloat16 or wider, within the bound.
A program may use at most 64 MiB of HBM per device.

```python
import math
import jax
import jax.numpy as jnp
from jax import lax

K0 = 1024
K1 = 4096
K2 = 16384
NLIST = 64
NOFF = 316
LEAF_DEV = 64
LEAVES = 8192
MID_BOXES = 1024
TOP_BOXES = 128
SECT = 16
K1_SECT = 256
K2_SECT = 1024


def with_ends(values, stream_key, least, top_value):
    longest = values.shape.index(max(values.shape))
    spots = []
    for shift in (0, 1):
        where = [jax.random.randint(jax.random.fold_in(stream_key, axis), (), 0, length) for axis, length in enumerate(values.shape)]
        where[longest] = (where[longest] + shift) % values.shape[longest]
        spots.append(tuple(where))
    return values.at[spots[0]].set(least).at[spots[1]].set(top_value)


def block_scale(key, shape, pieces, least, top_value):
    def one(axis_at, shards_of):
        steps = jax.random.uniform(jax.random.fold_in(jax.random.fold_in(key, 6), axis_at), (shards_of,), jnp.float32, least / len(pieces), top_value / len(pieces))
        return jnp.repeat(jnp.exp(steps), shape[axis_at] // shards_of).reshape((-1,) + (1,) * (len(shape) - axis_at - 1))

    factor_of = one(*pieces[0])
    for cut in pieces[1:]:
        factor_of = factor_of * one(*cut)
    return factor_of


def scatter_about(stream_key, shape, width, most, pieces=(), dtype=jnp.bfloat16):
    result = width * jax.random.normal(stream_key, shape, jnp.float32)
    if pieces:
        result = result * block_scale(stream_key, shape, pieces, -0.22, 0.18)
    return jnp.clip(result, -most, most).astype(dtype)


def setup_inputs(seed: int = 0) -> dict:
    keys = jax.random.split(jax.random.key(seed), 12)
    leaf_out = scatter_about(keys[0], (2, LEAVES, K0), 1.0, 6.0, ((1, 128),))
    interp_mid = scatter_about(keys[1], (K0, K1), K0 ** -0.5, 0.1875)
    shift_mid = jnp.clip(jax.random.uniform(keys[2], (8, K1), jnp.float32, -3.140625, 3.140625), -3.140625, 3.140625)
    trans_mid = scatter_about(keys[3], (2, NOFF, K1), (2 * NLIST) ** -0.5, 0.5, ((2, 16),), jnp.float32)
    list_mid = with_ends(jax.random.randint(keys[4], (MID_BOXES, NLIST), 0, MID_BOXES), jax.random.fold_in(keys[4], 1), 0, MID_BOXES - 1).astype(jnp.int32)
    offset_mid = with_ends(jax.random.randint(keys[5], (MID_BOXES, NLIST), 0, NOFF), jax.random.fold_in(keys[5], 1), 0, NOFF - 1).astype(jnp.int32)
    interp_top = scatter_about(keys[6], (SECT, K1_SECT, K2_SECT), K1_SECT ** -0.5, 0.375, ((0, 16),))
    shift_top = jnp.clip(jax.random.uniform(keys[7], (8, SECT, K2_SECT), jnp.float32, -3.140625, 3.140625), -3.140625, 3.140625)
    trans_top = scatter_about(keys[8], (2, NOFF, SECT, K2_SECT), (2 * NLIST) ** -0.5, 0.5, ((2, 16), (3, 8)), jnp.float32)
    list_top = with_ends(jax.random.randint(keys[9], (TOP_BOXES, NLIST), 0, TOP_BOXES), jax.random.fold_in(keys[9], 1), 0, TOP_BOXES - 1).astype(jnp.int32)
    offset_top = with_ends(jax.random.randint(keys[10], (TOP_BOXES, NLIST), 0, NOFF), jax.random.fold_in(keys[10], 1), 0, NOFF - 1).astype(jnp.int32)
    return {"leaf_out": leaf_out, "interp_mid": interp_mid, "shift_mid": shift_mid, "trans_mid": trans_mid, "list_mid": list_mid, "offset_mid": offset_mid, "interp_top": interp_top, "shift_top": shift_top, "trans_top": trans_top, "list_top": list_top, "offset_top": offset_top}


def complex_translate(patterns, sources, offsets, operators, block_rows):
    row_count = sources.shape[0]
    source_blocks = sources.reshape(row_count // block_rows, block_rows, sources.shape[1])
    offset_blocks = offsets.reshape(row_count // block_rows, block_rows, offsets.shape[1])

    def one_block(indices):
        picked = jnp.take(patterns, indices[0], axis=1).astype(jnp.float32)
        factors = jnp.take(operators, indices[1], axis=1).astype(jnp.float32)
        real_part = jnp.sum(picked[0] * factors[0] - picked[1] * factors[1], axis=1)
        imag_part = jnp.sum(picked[0] * factors[1] + picked[1] * factors[0], axis=1)
        return jnp.stack([real_part, imag_part])

    blocks = lax.map(one_block, (source_blocks, offset_blocks))
    return jnp.transpose(blocks, (1, 0, 2, 3)).reshape(2, row_count, patterns.shape[2])


def aggregate(patterns, matrix, cos_table, sin_table):
    real_part = jnp.dot(patterns[0], matrix, preferred_element_type=jnp.float32)
    imag_part = jnp.dot(patterns[1], matrix, preferred_element_type=jnp.float32)
    parent_count = patterns.shape[1] // 8
    real_part = real_part.reshape(parent_count, 8, matrix.shape[1])
    imag_part = imag_part.reshape(parent_count, 8, matrix.shape[1])
    summed_real = jnp.sum(real_part * cos_table[None] - imag_part * sin_table[None], axis=1)
    summed_imag = jnp.sum(real_part * sin_table[None] + imag_part * cos_table[None], axis=1)
    return jnp.stack([summed_real, summed_imag]).astype(jnp.bfloat16)


def child_shift(parents, cos_table, sin_table):
    real_part = parents[0].astype(jnp.float32)[:, None, :]
    imag_part = parents[1].astype(jnp.float32)[:, None, :]
    new_real = real_part * cos_table[None] + imag_part * sin_table[None]
    new_imag = imag_part * cos_table[None] - real_part * sin_table[None]
    return jnp.stack([new_real, new_imag]).reshape(2, -1, cos_table.shape[1]).astype(jnp.bfloat16)


def adjoint_apply(children, matrix):
    dims = (((1,), (1,)), ((), ()))
    real_part = lax.dot_general(children[0], matrix, dims, preferred_element_type=jnp.float32)
    imag_part = lax.dot_general(children[1], matrix, dims, preferred_element_type=jnp.float32)
    return jnp.stack([real_part, imag_part])


def reference(leaf_out, interp_mid, shift_mid, trans_mid, list_mid, offset_mid, interp_top, shift_top, trans_top, list_top, offset_top):
    cos_mid = jnp.cos(shift_mid)
    sin_mid = jnp.sin(shift_mid)
    leaf_blocks = jnp.transpose(leaf_out.reshape(2, LEAVES // LEAF_DEV, LEAF_DEV, K0), (1, 0, 2, 3))
    mid_blocks = lax.map(lambda part: aggregate(part, interp_mid, cos_mid, sin_mid), leaf_blocks)
    mid_pattern = jnp.transpose(mid_blocks, (1, 0, 2, 3)).reshape(2, MID_BOXES, K1)
    mid_far = complex_translate(mid_pattern, list_mid, offset_mid, trans_mid, math.gcd(MID_BOXES, 16))
    sector_in = jnp.transpose(mid_pattern.reshape(2, MID_BOXES, SECT, K1_SECT), (2, 0, 1, 3))
    cos_top = jnp.transpose(jnp.cos(shift_top), (1, 0, 2))
    sin_top = jnp.transpose(jnp.sin(shift_top), (1, 0, 2))
    top_blocks = lax.map(lambda item: aggregate(item[0], item[1], item[2], item[3]), (sector_in, interp_top, cos_top, sin_top))
    top_pattern = jnp.transpose(top_blocks, (1, 2, 0, 3)).reshape(2, TOP_BOXES, K2)
    top_in = complex_translate(top_pattern, list_top, offset_top, trans_top.reshape(2, NOFF, K2), math.gcd(TOP_BOXES, 4)).astype(jnp.bfloat16)
    top_sectors = jnp.transpose(top_in.reshape(2, TOP_BOXES, SECT, K2_SECT), (2, 0, 1, 3))

    def descend(item):
        children = child_shift(item[0], item[2], item[3])
        return adjoint_apply(children, item[1]) * (K1_SECT / K2_SECT)

    down_blocks = lax.map(descend, (top_sectors, interp_top, cos_top, sin_top))
    down_top = jnp.transpose(down_blocks, (1, 2, 0, 3)).reshape(2, MID_BOXES, K1)
    mid_in = (mid_far + down_top).astype(jnp.bfloat16)
    parent_blocks = jnp.transpose(mid_in.reshape(2, LEAVES // LEAF_DEV, LEAF_DEV // 8, K1), (1, 0, 2, 3))
    leaf_blocks_in = lax.map(lambda part: adjoint_apply(child_shift(part, cos_mid, sin_mid), interp_mid), parent_blocks)
    leaf_in = jnp.transpose(leaf_blocks_in, (1, 0, 2, 3)).reshape(2, LEAVES, K0)
    return leaf_in * (K0 / K1)
```

```python
import jax
import jax.numpy as jnp
from jax import lax
from jax.experimental import pallas as pl
from jax.experimental.pallas import tpu as pltpu
from jax.sharding import PartitionSpec as P

MESH = pl.DeviceIdType.MESH
F32 = jnp.float32
BF16 = jnp.bfloat16
VMEM = pltpu.VMEM
DMA = pltpu.SemaphoreType.DMA
PLANES = 4
SECTORS = 16
LANES = 128


def place():
    box = lax.axis_index("box")
    way = lax.axis_index("dir")
    low = box % 2
    core = way % 2
    return box // 2, way - core + low, core


def device_of(plane, sector, core):
    low = sector % 2
    return (plane * 2 + low, sector - low + core)


def sin_cos(angle):
    half = angle * 0.5
    sq = half * half
    s = sq * (-1.0 / 39916800.0) + (1.0 / 362880.0)
    s = sq * s - (1.0 / 5040.0)
    s = sq * s + (1.0 / 120.0)
    s = sq * s - (1.0 / 6.0)
    s = half + half * (sq * s)
    c = sq * (1.0 / 479001600.0) - (1.0 / 3628800.0)
    c = sq * c + (1.0 / 40320.0)
    c = sq * c - (1.0 / 720.0)
    c = sq * c + (1.0 / 24.0)
    c = sq * c - 0.5
    c = sq * c + 1.0
    return 2.0 * s * c, 1.0 - 2.0 * s * s


class Spread:
    def __init__(self, ref, send, recv):
        z, sector, core = place()
        self.ref, self.send, self.recv = ref, send, recv
        self.core = core
        self.z = z
        self.left = (z + PLANES - 1) % PLANES
        self.right = (z + 1) % PLANES
        self.far = (z + 2) % PLANES
        self.to_right = device_of(self.right, sector, core)
        self.to_left = device_of(self.left, sector, core)
        self.partner = device_of(z, sector, 1 - core)
        self.rows = ref.shape[2]

    def copy(self, plane, core, half, index, target):
        rows = self.rows
        if half is None:
            part = self.ref.at[plane, core]
        else:
            part = self.ref.at[plane, core, pl.ds(half * (rows // 2), rows // 2)]
        return pltpu.make_async_remote_copy(
            src_ref=part,
            dst_ref=part,
            send_sem=self.send.at[index],
            recv_sem=self.recv.at[index],
            device_id=target,
            device_id_type=MESH,
        )

    def start_own(self):
        self.copy(self.z, self.core, None, 0, self.to_right).start()
        self.copy(self.z, self.core, None, 1, self.to_left).start()
        self.copy(self.z, self.core, None, 4, self.partner).start()

    def forward(self):
        self.copy(self.left, self.core, None, 0, self.to_right).wait_recv()
        self.copy(self.left, self.core, 0, 2, self.to_right).start()
        self.copy(self.left, self.core, None, 5, self.partner).start()
        self.copy(self.right, self.core, None, 1, self.to_left).wait_recv()
        self.copy(self.right, self.core, 1, 3, self.to_left).start()
        self.copy(self.right, self.core, None, 6, self.partner).start()

    def forward_far(self):
        self.copy(self.far, self.core, 0, 2, self.to_right).wait_recv()
        self.copy(self.far, self.core, 1, 3, self.to_left).wait_recv()
        self.copy(self.far, self.core, None, 7, self.partner).start()

    def finish(self):
        other = 1 - self.core
        for index, plane in ((4, self.z), (5, self.left), (6, self.right), (7, self.far)):
            self.copy(plane, other, None, index, self.partner).wait_recv()
        self.copy(self.z, self.core, None, 0, self.to_right).wait_send()
        self.copy(self.z, self.core, None, 1, self.to_left).wait_send()
        self.copy(self.left, self.core, 0, 2, self.to_right).wait_send()
        self.copy(self.right, self.core, 1, 3, self.to_left).wait_send()
        for index, plane in ((4, self.z), (5, self.left), (6, self.right), (7, self.far)):
            self.copy(plane, self.core, None, index, self.partner).wait_send()


def up_kernel(
    leaf_ref,
    matrix_ref,
    shift_ref,
    trans_top_ref,
    trans_mid_ref,
    interp_top_ref,
    shift_top_ref,
    p_all,
    tp_all,
    t_all,
    trans_mid_x,
    interp_top_x,
    shift_top_x,
    weights,
    leaf_rows,
    cos_mid,
    sin_mid,
    sending,
    stage,
    piece,
    block_f32,
    top_lhs,
    top_f32,
    cos_top,
    sin_top,
    weight_sem,
    a2a_send,
    a2a_recv,
    swap_sem,
    share_send,
    share_recv,
    share_local,
    t_send,
    t_recv,
    p_send,
    p_recv,
    tp_send,
    tp_recv,
):
    z, sector, core = place()
    low = sector % 2
    own = low == core
    partner = device_of(z, sector, 1 - core)
    swap = device_of(z, sector - low + core, low)
    right = device_of((z + 1) % PLANES, sector, core)
    left = device_of((z + PLANES - 1) % PLANES, sector, core)

    def weight_copy(s):
        return pltpu.make_async_copy(
            matrix_ref.at[:, pl.ds(pl.multiple_of(s * 256, 256), 256)], weights.at[s], weight_sem.at[s]
        )

    def start_weight(k, carry):
        weight_copy((sector + 1 + k) % SECTORS).start()
        return carry

    barrier = pltpu.get_barrier_semaphore()

    def signal_peer(k, carry):
        pl.semaphore_signal(
            barrier, inc=1, device_id=device_of(z, (sector + 1 + k) % SECTORS, core), device_id_type=MESH
        )
        return carry

    lax.fori_loop(0, SECTORS - 1, signal_peer, 0)
    for device in (right, left, partner):
        pl.semaphore_signal(barrier, inc=1, device_id=device, device_id_type=MESH)

    @pl.when(jnp.logical_not(own))
    def _():
        pl.semaphore_signal(barrier, inc=1, device_id=swap, device_id_type=MESH)

    lax.fori_loop(0, SECTORS, start_weight, 0)

    offsets = trans_top_ref.shape[1]
    piece[...] = jnp.zeros_like(piece)
    half_rows = piece.shape[0] // 2
    for part in range(2):
        piece[part * half_rows : part * half_rows + offsets, :] = trans_top_ref[part].astype(BF16)

    rows = 2 * leaf_ref.shape[1]
    target = lax.broadcasted_iota(jnp.int32, (rows, rows), 0)
    source = lax.broadcasted_iota(jnp.int32, (rows, rows), 1)
    wanted = (target & 64) + ((target & 7) << 3) + ((target >> 3) & 7)
    order = (source == wanted).astype(BF16)
    both = jnp.concatenate([leaf_ref[0], leaf_ref[1]], axis=0)
    leaf_rows[...] = jnp.dot(order, both, preferred_element_type=F32).astype(BF16)

    pl.semaphore_wait(barrier, SECTORS - 1 + 3 + (low + core) % 2)

    swap_copy = pltpu.make_async_remote_copy(
        src_ref=piece,
        dst_ref=t_all.at[z, low],
        send_sem=swap_sem.at[0],
        recv_sem=swap_sem.at[1],
        device_id=swap,
        device_id_type=MESH,
    )
    shared = ((trans_mid_ref, trans_mid_x), (interp_top_ref, interp_top_x), (shift_top_ref, shift_top_x))

    def share_copy(index):
        return pltpu.make_async_remote_copy(
            src_ref=shared[index][0],
            dst_ref=shared[index][1],
            send_sem=share_send.at[index],
            recv_sem=share_recv.at[index],
            device_id=partner,
            device_id_type=MESH,
        )

    def local_copy(index):
        return pltpu.make_async_copy(shared[index][0], shared[index][1], share_local.at[index])

    @pl.when(own)
    def _():
        for index in range(3):
            share_copy(index).start()
            local_copy(index).start()
        t_all[z, core] = piece[...]

    @pl.when(jnp.logical_not(own))
    def _():
        swap_copy.start()

    sines, cosines = sin_cos(shift_ref[...])
    cos_mid[...] = cosines
    sin_mid[...] = sines

    def parents(s):
        columns = pl.ds(pl.multiple_of(s * 256, 256), 256)
        weight_copy(s).wait()
        spread = jnp.dot(leaf_rows[...], weights[s], preferred_element_type=F32)
        real_sum = jnp.zeros((8, 256), F32)
        imag_sum = jnp.zeros((8, 256), F32)
        for child in range(8):
            real = spread[child * 8 : child * 8 + 8]
            imag = spread[64 + child * 8 : 64 + child * 8 + 8]
            c = cos_mid[child : child + 1, columns]
            n = sin_mid[child : child + 1, columns]
            real_sum += real * c - imag * n
            imag_sum += real * n + imag * c
        for part in range(2):
            lanes = slice(part * LANES, part * LANES + LANES)
            stage[pl.ds(part, 8, stride=4), :] = real_sum[:, lanes]
            stage[pl.ds(2 + part, 8, stride=4), :] = imag_sum[:, lanes]
        return stage[...].astype(BF16)

    def a2a_copy(s):
        return pltpu.make_async_remote_copy(
            src_ref=sending.at[s],
            dst_ref=p_all.at[z, core, pl.ds(pl.multiple_of(sector * 32, 32), 32)],
            send_sem=a2a_send.at[s],
            recv_sem=a2a_recv.at[sector],
            device_id=device_of(z, s, core),
            device_id_type=MESH,
        )

    def arrived(s):
        return pltpu.make_async_remote_copy(
            src_ref=sending.at[s],
            dst_ref=p_all.at[z, core, pl.ds(pl.multiple_of(s * 32, 32), 32)],
            send_sem=a2a_send.at[s],
            recv_sem=a2a_recv.at[s],
            device_id=device_of(z, s, core),
            device_id_type=MESH,
        )

    def send_sector(k, carry):
        s = (sector + 1 + k) % SECTORS
        sending[s] = parents(s)
        a2a_copy(s).start()
        return carry

    t_spread = Spread(t_all, t_send, t_recv)
    p_spread = Spread(p_all, p_send, p_recv)
    tp_spread = Spread(tp_all, tp_send, tp_recv)

    lax.fori_loop(0, 6, send_sector, 0)

    @pl.when(jnp.logical_not(own))
    def _():
        swap_copy.wait()

    t_spread.start_own()
    lax.fori_loop(6, SECTORS - 1, send_sector, 0)
    p_all[z, core, pl.ds(pl.multiple_of(sector * 32, 32), 32), :] = parents(sector)
    t_spread.forward()

    def wait_sector(k, carry):
        s = (sector + 1 + k) % SECTORS
        arrived(s).wait_recv()
        return carry

    lax.fori_loop(0, SECTORS - 1, wait_sector, 0)
    p_spread.start_own()

    block_f32[...] = p_all[z, core].astype(F32)

    @pl.when(own)
    def _():
        for index in range(3):
            local_copy(index).wait()

    @pl.when(jnp.logical_not(own))
    def _():
        for index in range(3):
            share_copy(index).wait_recv()

    sines_t, cosines_t = sin_cos(shift_top_x[...])
    cos_top[...] = cosines_t
    sin_top[...] = sines_t
    for child in range(8):
        for part in range(2):
            for side in range(2):
                first = child * 4 + part * 2 + side
                a = block_f32[pl.ds(first, 8, stride=32), :]
                b = block_f32[pl.ds(256 + first, 8, stride=32), :]
                top_lhs[
                    part * 128 + child * 16 : part * 128 + child * 16 + 16, side * LANES : side * LANES + LANES
                ] = jnp.concatenate([a, b], axis=0).astype(BF16)

    def top_columns(k, carry):
        columns = pl.ds(pl.multiple_of(k * 256, 256), 256)
        spread = jnp.dot(top_lhs[...], interp_top_x[:, columns], preferred_element_type=F32)
        real_sum = jnp.zeros((16, 256), F32)
        imag_sum = jnp.zeros((16, 256), F32)
        for child in range(8):
            real = spread[child * 16 : child * 16 + 16]
            imag = spread[128 + child * 16 : 128 + child * 16 + 16]
            c = cos_top[child : child + 1, columns]
            n = sin_top[child : child + 1, columns]
            real_sum += real * c - imag * n
            imag_sum += real * n + imag * c
        for part in range(2):
            lanes = slice(part * LANES, part * LANES + LANES)
            for half in range(2):
                group = slice(half * 8, half * 8 + 8)
                top_f32[pl.ds(half * 128 + k * 2 + part, 8, stride=16), :] = real_sum[group, lanes]
                top_f32[pl.ds(half * 128 + 8 + k * 2 + part, 8, stride=16), :] = imag_sum[group, lanes]
        return carry

    lax.fori_loop(0, 4, top_columns, 0)
    tp_all[z, core] = top_f32[...].astype(BF16)
    tp_spread.start_own()
    t_spread.forward_far()
    p_spread.forward()
    tp_spread.forward()
    p_spread.forward_far()
    tp_spread.forward_far()

    def wait_sent(k, carry):
        a2a_copy((sector + 1 + k) % SECTORS).wait_send()
        return carry

    lax.fori_loop(0, SECTORS - 1, wait_sent, 0)

    @pl.when(own)
    def _():
        for index in range(3):
            share_copy(index).wait_send()

    t_spread.finish()
    p_spread.finish()
    tp_spread.finish()


def translate_kernel(
    p_all,
    tp_all,
    t_all,
    trans_mid,
    interp_top,
    shift_top,
    list_mid,
    offset_mid,
    list_top,
    offset_top,
    out,
    p_tab,
    t_tab,
    p_top,
    t_top,
    mid_sum,
    top_sum,
    child_rows,
    down,
    lists_v,
    tops_v,
    lists_w,
    tops_w,
    list_s,
    offset_s,
    list_ts,
    offset_ts,
    fetch_sem,
    index_sem,
):
    z, sector, core = place()
    mids = ((list_mid, 0, list_s), (offset_mid, 1, offset_s))
    tops = ((list_top, 0, list_ts), (offset_top, 1, offset_ts))

    def fetch_rows(k):
        low = k % 2
        row = (2 * z + low) * 128 + (k - low + core) * 8
        return [
            pltpu.make_async_copy(
                ref.at[pl.ds(pl.multiple_of(row, 8), 8)],
                lists_v.at[which, pl.ds(pl.multiple_of(k * 8, 8), 8)],
                fetch_sem.at[2 + which * SECTORS + k],
            )
            for ref, which, _ in mids
        ]

    def start_rows(k, carry):
        for copy in fetch_rows(k):
            copy.start()
        return carry

    def wait_rows(k, carry):
        for copy in fetch_rows(k):
            copy.wait()
        return carry

    fetch_tops = [pltpu.make_async_copy(ref, tops_v.at[which], fetch_sem.at[which]) for ref, which, _ in tops]
    lax.fori_loop(0, SECTORS, start_rows, 0)
    for copy in fetch_tops:
        copy.start()

    upper = lax.broadcasted_iota(jnp.int32, (8, LANES), 0) < 4

    def mid_rows(k, carry):
        plane = k // 32
        cpart = (k // 16) % 2
        s = k % 16
        low = s % 2
        first = ((2 * plane + low) * 128 + (s - low + cpart) * 8) * 8
        rows = p_all[plane, cpart, pl.ds(pl.multiple_of(s * 32, 32), 32), :].astype(F32)
        made = []
        for pair in range(4):
            v = rows[pair * 8 : pair * 8 + 8]
            r = pltpu.roll(v, 4, 0)
            made += [jnp.where(upper, v, r), jnp.where(upper, r, v)]
        p_tab[pl.ds(pl.multiple_of(first, 64), 64), :] = jnp.concatenate(made, axis=0)
        top = (2 * plane + low) * 16 + (s - low + cpart)
        p_top[pl.ds(pl.multiple_of(top * 16, 16), 16), :] = tp_all[
            plane, cpart, pl.ds(pl.multiple_of(s * 16, 16), 16), :
        ].astype(F32)
        return carry

    lax.fori_loop(0, PLANES * 2 * SECTORS, mid_rows, 0)

    def put_offsets(start, source_start):
        for part in range(2):
            for side in range(2):
                v = trans_mid[part, source_start, side * LANES : side * LANES + LANES]
                t_tab[pl.ds(start + part * 4 + side, 8, stride=8), :] = v
                t_tab[pl.ds(start + part * 4 + 2 + side, 8, stride=8), :] = v

    offsets = trans_mid.shape[1]

    def mid_offsets(k, carry):
        put_offsets(pl.multiple_of(k * 64, 64), pl.ds(pl.multiple_of(k * 8, 8), 8))
        return carry

    lax.fori_loop(0, offsets // 8, mid_offsets, 0)
    if offsets % 8:
        put_offsets((offsets - 8) * 8, slice(offsets - 8, offsets))

    def top_offsets(k, carry):
        for piece in range(8):
            for part in range(2):
                rows = t_all[
                    piece // 2, piece % 2, pl.ds(pl.multiple_of(part * 320 + k * 16, 16), 16), :
                ].astype(F32)
                for half in range(2):
                    t_top[pl.ds((k * 16 + half * 8) * 16 + part * 8 + piece, 8, stride=16), :] = rows[
                        half * 8 : half * 8 + 8
                    ]
        return carry

    lax.fori_loop(0, 20, top_offsets, 0)

    lax.fori_loop(0, SECTORS, wait_rows, 0)
    for copy in fetch_tops:
        copy.wait()
    to_smem = []
    for _, which, target in mids:
        lists_w[which] = lists_v[which] * 8
        to_smem.append(pltpu.make_async_copy(lists_w.at[which], target, index_sem.at[which]))
    for _, which, target in tops:
        tops_w[which] = tops_v[which] * 16
        to_smem.append(pltpu.make_async_copy(tops_w.at[which], target, index_sem.at[2 + which]))
    for copy in to_smem:
        copy.start()
    for copy in to_smem:
        copy.wait()

    entries = list_mid.shape[1]

    def top_box(k, carry):
        low = k % 2
        row = (2 * z + low) * 16 + (k - low + core)
        sums = [jnp.zeros((8, LANES), F32) for _ in range(4)]
        for j in range(entries):
            n = list_ts[row, j]
            o = offset_ts[row, j]
            pr = p_top[pl.ds(pl.multiple_of(n, 8), 8), :]
            pi = p_top[pl.ds(pl.multiple_of(n + 8, 8), 8), :]
            tr = t_top[pl.ds(pl.multiple_of(o, 8), 8), :]
            ti = t_top[pl.ds(pl.multiple_of(o + 8, 8), 8), :]
            sums = [sums[0] + pr * tr, sums[1] + pi * ti, sums[2] + pr * ti, sums[3] + pi * tr]
        real = (sums[0] - sums[1]).astype(BF16).astype(F32)
        imag = (sums[2] + sums[3]).astype(BF16).astype(F32)
        top_sum[pl.ds(pl.multiple_of(k * 16, 16), 8), :] = real
        top_sum[pl.ds(pl.multiple_of(k * 16 + 8, 8), 8), :] = imag
        return carry

    lax.fori_loop(0, SECTORS, top_box, 0)

    sines, cosines = sin_cos(shift_top[...])

    def children(k, carry):
        for part in range(8):
            lanes = slice(part * LANES, part * LANES + LANES)
            c = cosines[:, lanes]
            n = sines[:, lanes]
            reals = []
            imags = []
            for half in range(2):
                first = k * 32 + half * 16 + part
                real = jnp.broadcast_to(top_sum[pl.ds(first, 1), :], (8, LANES))
                imag = jnp.broadcast_to(top_sum[pl.ds(first + 8, 1), :], (8, LANES))
                reals.append(real * c + imag * n)
                imags.append(imag * c - real * n)
            at = pl.multiple_of(k * 16, 16)
            child_rows[pl.ds(at, 16), lanes] = jnp.concatenate(reals, axis=0).astype(BF16)
            child_rows[pl.ds(128 + at, 16), lanes] = jnp.concatenate(imags, axis=0).astype(BF16)
        return carry

    lax.fori_loop(0, 8, children, 0)
    scale = interp_top.shape[0] / interp_top.shape[1]
    down[...] = scale * lax.dot_general(
        child_rows[...], interp_top[...], (((1,), (1,)), ((), ())), preferred_element_type=F32
    )

    def mid_box(k, carry):
        sums = [jnp.zeros((8, LANES), F32) for _ in range(4)]
        for j in range(entries):
            p = p_tab[pl.ds(pl.multiple_of(list_s[k, j], 8), 8), :]
            t = t_tab[pl.ds(pl.multiple_of(offset_s[k, j], 8), 8), :]
            sums[j % 4] = sums[j % 4] + p * t
        mid_sum[pl.ds(pl.multiple_of(k * 8, 8), 8), :] = (sums[0] + sums[1]) + (sums[2] + sums[3])
        return carry

    lax.fori_loop(0, SECTORS * 8, mid_box, 0)

    def combine(k, carry):
        at = pl.multiple_of(k * 8, 8)
        for side in range(2):
            lanes = slice(side * LANES, side * LANES + LANES)
            real = mid_sum[pl.ds(k * 64 + side, 8, stride=8), :] - mid_sum[pl.ds(k * 64 + 6 + side, 8, stride=8), :]
            imag = mid_sum[pl.ds(k * 64 + 2 + side, 8, stride=8), :] + mid_sum[pl.ds(k * 64 + 4 + side, 8, stride=8), :]
            real = real + down[pl.ds(at, 8), lanes]
            imag = imag + down[pl.ds(pl.multiple_of(128 + k * 8, 8), 8), lanes]
            out[k, :, lanes] = jnp.concatenate([real, imag], axis=0).astype(BF16)
        return carry

    lax.fori_loop(0, SECTORS, combine, 0)


def down_kernel(
    pieces,
    matrix_ref,
    shift_ref,
    out,
    weights,
    received,
    children,
    weight_sem,
    send_sem,
    recv_sem,
):
    z, sector, core = place()
    barrier = pltpu.get_barrier_semaphore()

    def signal_peer(k, carry):
        pl.semaphore_signal(
            barrier, inc=1, device_id=device_of(z, (sector + 1 + k) % SECTORS, core), device_id_type=MESH
        )
        return carry

    lax.fori_loop(0, SECTORS - 1, signal_peer, 0)
    chunk = 256
    count = matrix_ref.shape[0] // chunk
    copies = [
        pltpu.make_async_copy(matrix_ref.at[pl.ds(k * chunk, chunk)], weights.at[pl.ds(k * chunk, chunk)], weight_sem.at[k])
        for k in range(count)
    ]
    for copy in copies:
        copy.start()
    received[sector] = pieces[sector]
    pl.semaphore_wait(barrier, SECTORS - 1)

    def out_copy(s):
        return pltpu.make_async_remote_copy(
            src_ref=pieces.at[s],
            dst_ref=received.at[sector],
            send_sem=send_sem.at[s],
            recv_sem=recv_sem.at[sector],
            device_id=device_of(z, s, core),
            device_id_type=MESH,
        )

    def in_copy(s):
        return pltpu.make_async_remote_copy(
            src_ref=pieces.at[s],
            dst_ref=received.at[s],
            send_sem=send_sem.at[s],
            recv_sem=recv_sem.at[s],
            device_id=device_of(z, s, core),
            device_id_type=MESH,
        )

    def start(k, carry):
        out_copy((sector + 1 + k) % SECTORS).start()
        return carry

    lax.fori_loop(0, SECTORS - 1, start, 0)

    def make_children(s):
        columns = pl.ds(pl.multiple_of(s * 256, 256), 256)
        n, c = sin_cos(shift_ref[:, columns])
        rows = received[s].astype(F32)
        for pair in range(4):
            reals = []
            imags = []
            for half in range(2):
                box = pair * 2 + half
                real = jnp.broadcast_to(rows[box : box + 1], (8, 256))
                imag = jnp.broadcast_to(rows[8 + box : 9 + box], (8, 256))
                reals.append(real * c + imag * n)
                imags.append(imag * c - real * n)
            children[pair * 16 : pair * 16 + 16, columns] = jnp.concatenate(reals, axis=0).astype(BF16)
            children[64 + pair * 16 : 80 + pair * 16, columns] = jnp.concatenate(imags, axis=0).astype(BF16)

    make_children(sector)

    def take(k, carry):
        s = (sector + 1 + k) % SECTORS
        in_copy(s).wait_recv()
        make_children(s)
        return carry

    lax.fori_loop(0, SECTORS - 1, take, 0)
    scale = matrix_ref.shape[0] / matrix_ref.shape[1]
    for copy in copies:
        copy.wait()

    def columns_out(k, carry):
        at = pl.ds(pl.multiple_of(k * chunk, chunk), chunk)
        part = scale * lax.dot_general(
            children[...], weights[at, :], (((1,), (1,)), ((), ())), preferred_element_type=F32
        )
        out[0, :, at] = part[:64]
        out[1, :, at] = part[64:]
        return carry

    lax.fori_loop(0, count, columns_out, 0)

    def wait_sent(k, carry):
        out_copy((sector + 1 + k) % SECTORS).wait_send()
        return carry

    lax.fori_loop(0, SECTORS - 1, wait_sent, 0)


def in_vmem(count):
    return [pl.BlockSpec(memory_space=VMEM)] * count


def in_hbm(count):
    return [pl.BlockSpec(memory_space=pltpu.HBM)] * count


def anywhere(count):
    return [pl.BlockSpec(memory_space=pl.ANY)] * count


def on_device(
    leaf_out,
    interp_mid,
    shift_mid,
    trans_mid,
    list_mid,
    offset_mid,
    interp_top,
    shift_top,
    trans_top,
    list_top,
    offset_top,
):
    offsets = trans_mid.shape[1]
    padded = 320
    trans_top = trans_top[:, :, 0, :]
    interp_top = interp_top[0]
    shift_top = shift_top[:, 0, :]
    rows = 2 * leaf_out.shape[1]
    shapes = (
        jax.ShapeDtypeStruct((PLANES, 2, 512, LANES), BF16),
        jax.ShapeDtypeStruct((PLANES, 2, 256, LANES), BF16),
        jax.ShapeDtypeStruct((PLANES, 2, 2 * padded, LANES), BF16),
        jax.ShapeDtypeStruct(trans_mid.shape, F32),
        jax.ShapeDtypeStruct(interp_top.shape, BF16),
        jax.ShapeDtypeStruct(shift_top.shape, F32),
    )
    gathered = pl.pallas_call(
        up_kernel,
        out_shape=shapes,
        in_specs=in_vmem(1) + in_hbm(1) + in_vmem(2) + anywhere(3),
        out_specs=in_vmem(6),
        scratch_shapes=[
            VMEM((SECTORS, interp_mid.shape[0], 256), BF16),
            VMEM((rows, interp_mid.shape[0]), BF16),
            VMEM(shift_mid.shape, F32),
            VMEM(shift_mid.shape, F32),
            VMEM((SECTORS, 32, LANES), BF16),
            VMEM((32, LANES), F32),
            VMEM((2 * padded, LANES), BF16),
            VMEM((512, LANES), F32),
            VMEM((256, 256), BF16),
            VMEM((256, LANES), F32),
            VMEM(shift_top.shape, F32),
            VMEM(shift_top.shape, F32),
            DMA((SECTORS,)),
            DMA((SECTORS,)),
            DMA((SECTORS,)),
            DMA((2,)),
            DMA((3,)),
            DMA((3,)),
            DMA((3,)),
            DMA((8,)),
            DMA((8,)),
            DMA((8,)),
            DMA((8,)),
            DMA((8,)),
            DMA((8,)),
        ],
        compiler_params=pltpu.CompilerParams(
            collective_id=0, has_side_effects=True, vmem_limit_bytes=24 * 1024 * 1024
        ),
        name="up",
    )(leaf_out, interp_mid, shift_mid, trans_top, trans_mid, interp_top, shift_top)

    pieces = pl.pallas_call(
        translate_kernel,
        out_shape=jax.ShapeDtypeStruct((SECTORS, 16, 256), BF16),
        in_specs=in_vmem(6) + anywhere(4),
        out_specs=pl.BlockSpec(memory_space=VMEM),
        scratch_shapes=[
            VMEM((1024 * 8, LANES), F32),
            VMEM((padded * 8, LANES), F32),
            VMEM((128 * 16, LANES), F32),
            VMEM((padded * 16, LANES), F32),
            VMEM((128 * 8, LANES), F32),
            VMEM((16 * 16, LANES), F32),
            VMEM((256, 1024), BF16),
            VMEM((256, 256), F32),
            VMEM((2, 128, list_mid.shape[1]), jnp.int32),
            VMEM((2, 128, list_mid.shape[1]), jnp.int32),
            VMEM((2, 128, list_mid.shape[1]), jnp.int32),
            VMEM((2, 128, list_mid.shape[1]), jnp.int32),
            pltpu.SMEM((128, list_mid.shape[1]), jnp.int32),
            pltpu.SMEM((128, list_mid.shape[1]), jnp.int32),
            pltpu.SMEM((128, list_mid.shape[1]), jnp.int32),
            pltpu.SMEM((128, list_mid.shape[1]), jnp.int32),
            DMA((2 + 2 * SECTORS,)),
            DMA((4,)),
        ],
        compiler_params=pltpu.CompilerParams(vmem_limit_bytes=24 * 1024 * 1024),
        name="translate",
    )(*gathered, list_mid, offset_mid, list_top, offset_top)

    return pl.pallas_call(
        down_kernel,
        out_shape=jax.ShapeDtypeStruct(leaf_out.shape, F32),
        in_specs=in_vmem(1) + in_hbm(1) + in_vmem(1),
        out_specs=pl.BlockSpec(memory_space=VMEM),
        scratch_shapes=[
            VMEM(interp_mid.shape, BF16),
            VMEM((SECTORS, 16, 256), BF16),
            VMEM((rows, interp_mid.shape[1]), BF16),
            DMA((4,)),
            DMA((SECTORS,)),
            DMA((SECTORS,)),
        ],
        compiler_params=pltpu.CompilerParams(
            collective_id=1, has_side_effects=True, vmem_limit_bytes=20 * 1024 * 1024
        ),
        name="down",
    )(pieces, interp_mid, shift_mid)


def solution(mesh):
    return jax.shard_map(
        on_device,
        mesh=mesh,
        in_specs=(
            P(None, ("box", "dir"), None),
            P(),
            P(),
            P(None, None, "dir"),
            P(),
            P(),
            P("dir", None, None),
            P(None, "dir", None),
            P(None, None, "dir", "box"),
            P(),
            P(),
        ),
        out_specs=P(None, ("box", "dir"), None),
        check_vma=False,
    )
```

```python
import jax
import jax.numpy as jnp
from jax import lax
from jax.experimental import pallas as pl
from jax.experimental.pallas import tpu as pltpu
from jax.sharding import PartitionSpec as P

MESH = pl.DeviceIdType.MESH
F32 = jnp.float32
BF16 = jnp.bfloat16
VMEM = pltpu.VMEM
DMA = pltpu.SemaphoreType.DMA
PLANES = 4
SECTORS = 16
LANES = 128


def place():
    box = lax.axis_index("box")
    way = lax.axis_index("dir")
    low = box % 2
    core = way % 2
    return box // 2, way - core + low, core


def device_of(plane, sector, core):
    low = sector % 2
    return (plane * 2 + low, sector - low + core)


def sin_cos(angle):
    half = angle * 0.5
    sq = half * half
    s = sq * (-1.0 / 39916800.0) + (1.0 / 362880.0)
    s = sq * s - (1.0 / 5040.0)
    s = sq * s + (1.0 / 120.0)
    s = sq * s - (1.0 / 6.0)
    s = half + half * (sq * s)
    c = sq * (1.0 / 479001600.0) - (1.0 / 3628800.0)
    c = sq * c + (1.0 / 40320.0)
    c = sq * c - (1.0 / 720.0)
    c = sq * c + (1.0 / 24.0)
    c = sq * c - 0.5
    c = sq * c + 1.0
    return 2.0 * s * c, 1.0 - 2.0 * s * s


class Spread:
    def __init__(self, ref, send, recv):
        z, sector, core = place()
        self.ref, self.send, self.recv = ref, send, recv
        self.core = core
        self.z = z
        self.left = (z + PLANES - 1) % PLANES
        self.right = (z + 1) % PLANES
        self.far = (z + 2) % PLANES
        self.to_right = device_of(self.right, sector, core)
        self.to_left = device_of(self.left, sector, core)
        self.partner = device_of(z, sector, 1 - core)
        self.rows = ref.shape[2]
        self.crossing = ((4, self.z), (5, self.left), (6, self.right), (7, self.far))

    def copy(self, plane, core, half, index, target):
        rows = self.rows
        if half is None:
            part = self.ref.at[plane, core]
        else:
            part = self.ref.at[plane, core, pl.ds(half * (rows // 2), rows // 2)]
        return pltpu.make_async_remote_copy(
            src_ref=part,
            dst_ref=part,
            send_sem=self.send.at[index],
            recv_sem=self.recv.at[index],
            device_id=target,
            device_id_type=MESH,
        )

    def start_own(self):
        self.copy(self.z, self.core, None, 0, self.to_right).start()
        self.copy(self.z, self.core, None, 1, self.to_left).start()
        self.copy(self.z, self.core, None, 4, self.partner).start()

    def forward(self):
        self.copy(self.left, self.core, None, 0, self.to_right).wait_recv()
        self.copy(self.left, self.core, 0, 2, self.to_right).start()
        self.copy(self.left, self.core, None, 5, self.partner).start()
        self.copy(self.right, self.core, None, 1, self.to_left).wait_recv()
        self.copy(self.right, self.core, 1, 3, self.to_left).start()
        self.copy(self.right, self.core, None, 6, self.partner).start()

    def forward_far(self):
        self.copy(self.far, self.core, 0, 2, self.to_right).wait_recv()
        self.copy(self.far, self.core, 1, 3, self.to_left).wait_recv()
        self.copy(self.far, self.core, None, 7, self.partner).start()

    def take(self, which):
        index, plane = self.crossing[which]
        self.copy(plane, 1 - self.core, None, index, self.partner).wait_recv()
        return plane

    def sent(self):
        self.copy(self.z, self.core, None, 0, self.to_right).wait_send()
        self.copy(self.z, self.core, None, 1, self.to_left).wait_send()
        self.copy(self.left, self.core, 0, 2, self.to_right).wait_send()
        self.copy(self.right, self.core, 1, 3, self.to_left).wait_send()
        for index, plane in self.crossing:
            self.copy(plane, self.core, None, index, self.partner).wait_send()


def kernel(
    leaf_ref,
    matrix_ref,
    shift_mid_ref,
    trans_top_ref,
    trans_mid_ref,
    interp_top_ref,
    shift_top_ref,
    list_mid_ref,
    offset_mid_ref,
    list_top_ref,
    offset_top_ref,
    out_ref,
    leaf,
    weights,
    shift_mid,
    trans_top,
    trans_mid,
    interp_top,
    shift_top,
    lists_mid,
    lists_top,
    list_s,
    offset_s,
    list_ts,
    offset_ts,
    p_all,
    tp_all,
    t_all,
    leaf_rows,
    cos_mid,
    sin_mid,
    sending,
    stage,
    piece,
    block_f32,
    top_lhs,
    top_f32,
    cos_top,
    sin_top,
    p_tab,
    t_tab,
    p_top,
    t_top,
    mid_sum,
    top_sum,
    child_rows,
    down,
    pieces,
    received,
    children,
    total,
    weight_sem,
    load_sem,
    index_sem,
    a2a_send,
    a2a_recv,
    swap_sem,
    share_send,
    share_recv,
    t_send,
    t_recv,
    p_send,
    p_recv,
    tp_send,
    tp_recv,
    back_send,
    back_recv,
    out_sem,
):
    z, sector, core = place()
    low = sector % 2
    own = low == core
    partner = device_of(z, sector, 1 - core)
    swap = device_of(z, sector - low + core, low)
    right = device_of((z + 1) % PLANES, sector, core)
    left = device_of((z + PLANES - 1) % PLANES, sector, core)
    t_spread = Spread(t_all, t_send, t_recv)
    p_spread = Spread(p_all, p_send, p_recv)
    tp_spread = Spread(tp_all, tp_send, tp_recv)

    def nth(k):
        return (sector + 1 + k) % SECTORS

    def to_sector(s):
        return device_of(z, s, core)

    barrier = pltpu.get_barrier_semaphore()

    def signal_peer(k, carry):
        pl.semaphore_signal(barrier, inc=1, device_id=to_sector(nth(k)), device_id_type=MESH)
        return carry

    lax.fori_loop(0, SECTORS - 1, signal_peer, 0)
    for device in (right, left, partner):
        pl.semaphore_signal(barrier, inc=1, device_id=device, device_id_type=MESH)

    @pl.when(jnp.logical_not(own))
    def _():
        pl.semaphore_signal(barrier, inc=1, device_id=swap, device_id_type=MESH)

    slab = pl.ds(pl.multiple_of(z * 256, 256), 256)
    loads = [
        pltpu.make_async_copy(source, target, load_sem.at[index])
        for index, (source, target) in enumerate(
            (
                (leaf_ref, leaf),
                (trans_top_ref, trans_top),
                (shift_mid_ref, shift_mid),
                (list_mid_ref.at[:, slab], lists_mid.at[0]),
                (offset_mid_ref.at[:, slab], lists_mid.at[1]),
                (list_top_ref, lists_top.at[0]),
                (offset_top_ref, lists_top.at[1]),
            )
        )
    ]
    for copy in loads[:3]:
        copy.start()

    def weight_copy(s):
        return pltpu.make_async_copy(
            matrix_ref.at[:, pl.ds(pl.multiple_of(s * 256, 256), 256)], weights.at[s], weight_sem.at[s]
        )

    def start_weight(k, carry):
        weight_copy(nth(k)).start()
        return carry

    lax.fori_loop(0, SECTORS, start_weight, 0)
    for copy in loads[3:]:
        copy.start()

    loads[0].wait()
    rows = 2 * leaf.shape[1]
    target = lax.broadcasted_iota(jnp.int32, (rows, rows), 0)
    source = lax.broadcasted_iota(jnp.int32, (rows, rows), 1)
    wanted = (target & 64) + ((target & 7) << 3) + ((target >> 3) & 7)
    order = (source == wanted).astype(BF16)
    both = jnp.concatenate([leaf[0], leaf[1]], axis=0)
    leaf_rows[...] = jnp.dot(order, both, preferred_element_type=F32).astype(BF16)

    loads[1].wait()
    used = trans_top.shape[0]
    piece[0:used, :] = trans_top[...].astype(BF16)
    piece[used:, :] = jnp.zeros((piece.shape[0] - used, LANES), BF16)

    pl.semaphore_wait(barrier, SECTORS - 1 + 3 + (low + core) % 2)

    swap_copy = pltpu.make_async_remote_copy(
        src_ref=piece,
        dst_ref=t_all.at[z, low],
        send_sem=swap_sem.at[0],
        recv_sem=swap_sem.at[1],
        device_id=swap,
        device_id_type=MESH,
    )
    shared = ((trans_mid_ref, trans_mid), (interp_top_ref, interp_top), (shift_top_ref, shift_top))

    def share_copy(index):
        return pltpu.make_async_remote_copy(
            src_ref=shared[index][0],
            dst_ref=shared[index][1],
            send_sem=share_send.at[index],
            recv_sem=share_recv.at[index],
            device_id=partner,
            device_id_type=MESH,
        )

    def local_copy(index):
        return pltpu.make_async_copy(shared[index][0], shared[index][1], share_recv.at[index])

    @pl.when(own)
    def _():
        for index in range(3):
            share_copy(index).start()
            local_copy(index).start()
        t_all[z, core] = piece[...]

    @pl.when(jnp.logical_not(own))
    def _():
        swap_copy.start()

    loads[2].wait()
    sines, cosines = sin_cos(shift_mid[...])
    cos_mid[...] = cosines
    sin_mid[...] = sines

    def parents(s, slot):
        columns = pl.ds(pl.multiple_of(s * 256, 256), 256)
        weight_copy(s).wait()
        spread = jnp.dot(leaf_rows[...], weights[s], preferred_element_type=F32)
        real_sum = jnp.zeros((8, 256), F32)
        imag_sum = jnp.zeros((8, 256), F32)
        for child in range(8):
            real = spread[child * 8 : child * 8 + 8]
            imag = spread[64 + child * 8 : 64 + child * 8 + 8]
            c = cos_mid[child : child + 1, columns]
            n = sin_mid[child : child + 1, columns]
            real_sum += real * c - imag * n
            imag_sum += real * n + imag * c
        for part in range(2):
            lanes = slice(part * LANES, part * LANES + LANES)
            stage[pl.ds(slot * 32 + part, 8, stride=4), :] = real_sum[:, lanes]
            stage[pl.ds(slot * 32 + 2 + part, 8, stride=4), :] = imag_sum[:, lanes]
        return stage[slot * 32 : slot * 32 + 32, :].astype(BF16)

    def rows_of(s):
        return p_all.at[z, core, pl.ds(pl.multiple_of(s * 32, 32), 32)]

    def a2a_copy(s, landing):
        return pltpu.make_async_remote_copy(
            src_ref=sending.at[s],
            dst_ref=rows_of(landing),
            send_sem=a2a_send.at[s],
            recv_sem=a2a_recv.at[landing],
            device_id=to_sector(s),
            device_id_type=MESH,
        )

    def send_pair(k, carry):
        first, second = nth(2 * k), nth(2 * k + 1)
        sending[first] = parents(first, 0)
        sending[second] = parents(second, 1)
        a2a_copy(first, sector).start()
        a2a_copy(second, sector).start()
        return carry

    lax.fori_loop(0, 3, send_pair, 0)

    @pl.when(jnp.logical_not(own))
    def _():
        swap_copy.wait()

    t_spread.start_own()
    lax.fori_loop(3, 7, send_pair, 0)
    last = nth(SECTORS - 2)
    sending[last] = parents(last, 0)
    a2a_copy(last, sector).start()
    p_all[z, core, pl.ds(pl.multiple_of(sector * 32, 32), 32), :] = parents(sector, 1)
    t_spread.forward()

    for copy in loads[3:]:
        copy.wait()
    to_smem = [
        pltpu.make_async_copy(source, target, index_sem.at[index])
        for index, (source, target) in enumerate(
            (
                (lists_mid.at[0], list_s),
                (lists_mid.at[1], offset_s),
                (lists_top.at[0], list_ts),
                (lists_top.at[1], offset_ts),
            )
        )
    ]
    for copy in to_smem:
        copy.start()

    @pl.when(own)
    def _():
        for index in range(3):
            local_copy(index).wait()

    @pl.when(jnp.logical_not(own))
    def _():
        for index in range(3):
            share_copy(index).wait_recv()

    offsets = trans_mid.shape[0] // 4
    t_rows = t_tab.reshape(offsets * 8, LANES)

    def put_offsets(first, row):
        for quarter, places in enumerate(((0, 2), (4, 6), (1, 3), (5, 7))):
            v = trans_mid[pl.ds(first + quarter, 8, stride=4), :]
            for at in places:
                t_rows[pl.ds(row + at, 8, stride=8), :] = v

    def mid_offsets(k, carry):
        put_offsets(pl.multiple_of(k * 32, 32), pl.multiple_of(k * 64, 64))
        return carry

    lax.fori_loop(0, offsets // 8, mid_offsets, 0)
    if offsets % 8:
        put_offsets((offsets - 8) * 4, (offsets - 8) * 8)

    sines_t, cosines_t = sin_cos(shift_top[...])
    cos_top[...] = cosines_t
    sin_top[...] = sines_t

    def wait_sector(k, carry):
        s = nth(k)
        a2a_copy(s, s).wait_recv()
        return carry

    lax.fori_loop(0, SECTORS - 1, wait_sector, 0)
    p_spread.start_own()

    block_f32[...] = p_all[z, core].astype(F32)
    for child in range(8):
        for part in range(2):
            for side in range(2):
                first = child * 4 + part * 2 + side
                a = block_f32[pl.ds(first, 8, stride=32), :]
                b = block_f32[pl.ds(256 + first, 8, stride=32), :]
                top_lhs[
                    part * 128 + child * 16 : part * 128 + child * 16 + 16, side * LANES : side * LANES + LANES
                ] = jnp.concatenate([a, b], axis=0).astype(BF16)

    def top_columns(k, carry):
        columns = pl.ds(pl.multiple_of(k * 256, 256), 256)
        spread = jnp.dot(top_lhs[...], interp_top[:, columns], preferred_element_type=F32)
        for part in range(2):
            lanes = slice(part * LANES, part * LANES + LANES)
            group = k * 2 + part
            real_sum = jnp.zeros((16, LANES), F32)
            imag_sum = jnp.zeros((16, LANES), F32)
            for child in range(8):
                real = spread[child * 16 : child * 16 + 16, lanes]
                imag = spread[128 + child * 16 : 128 + child * 16 + 16, lanes]
                c = cos_top[pl.ds(child * 8 + group, 1), :]
                n = sin_top[pl.ds(child * 8 + group, 1), :]
                real_sum += real * c - imag * n
                imag_sum += real * n + imag * c
            for half in range(2):
                boxes = slice(half * 8, half * 8 + 8)
                top_f32[pl.ds(half * 128 + group, 8, stride=16), :] = real_sum[boxes]
                top_f32[pl.ds(half * 128 + 8 + group, 8, stride=16), :] = imag_sum[boxes]
        return carry

    lax.fori_loop(0, 4, top_columns, 0)
    tp_all[z, core] = top_f32[...].astype(BF16)
    tp_spread.start_own()

    upper = lax.broadcasted_iota(jnp.int32, (8, LANES), 0) < 4

    def mid_table(plane, side):
        def one(s, carry):
            odd = s % 2
            first = (2 * plane + odd) * 128 + (s - odd + side) * 8
            found = p_all[plane, side, pl.ds(pl.multiple_of(s * 32, 32), 32), :].astype(F32)
            for pair in range(4):
                v = found[pair * 8 : pair * 8 + 8]
                r = pltpu.roll(v, 4, 0)
                p_tab[first + pair * 2] = jnp.where(upper, v, r)
                p_tab[first + pair * 2 + 1] = jnp.where(upper, r, v)
            return carry

        lax.fori_loop(0, SECTORS, one, 0)

    def top_table(plane, side):
        def one(s, carry):
            odd = s % 2
            found = tp_all[plane, side, pl.ds(pl.multiple_of(s * 16, 16), 16), :].astype(F32)
            first = (2 * plane + odd) * 16 + (s - odd + side)
            p_top[first, 0] = found[:8]
            p_top[first, 1] = found[8:]
            return carry

        lax.fori_loop(0, SECTORS, one, 0)

    def offset_table(plane, side):
        at = plane * 2 + side
        t_rows = t_top.reshape(t_top.shape[0] * 8, LANES)

        def one(k, carry):
            found = t_all[plane, side, pl.ds(pl.multiple_of(k * 16, 16), 16), :].astype(F32)
            for half in range(2):
                t_rows[pl.ds(k * 128 + half * 64 + at, 8, stride=8), :] = found[half * 8 : half * 8 + 8]
            return carry

        lax.fori_loop(0, t_all.shape[2] // 16, one, 0)

    mid_table(z, core)
    top_table(z, core)
    t_spread.forward_far()
    offset_table(z, core)
    offset_table(t_spread.left, core)
    offset_table(t_spread.right, core)
    p_spread.forward()
    tp_spread.forward()
    mid_table(p_spread.left, core)
    mid_table(p_spread.right, core)
    offset_table(t_spread.far, core)
    for which in range(3):
        mid_table(p_spread.take(which), 1 - core)
    p_spread.forward_far()
    tp_spread.forward_far()
    mid_table(p_spread.far, core)
    for which in range(4):
        offset_table(t_spread.take(which), 1 - core)
    mid_table(p_spread.take(3), 1 - core)
    for copy in to_smem:
        copy.wait()

    entries = list_mid_ref.shape[0]

    def mid_box(k, carry):
        s = k // 8
        odd = s % 2
        column = odd * 128 + (s - odd + core) * 8 + k % 8
        kept = jnp.zeros((8, LANES), F32)
        for j in range(entries):
            p = p_tab[list_s[j, column]]
            t = t_tab[offset_s[j, column]]
            kept = kept + p * t
        mid_sum[pl.ds(pl.multiple_of(k * 8, 8), 8), :] = kept
        return carry

    lax.fori_loop(0, SECTORS * 8, mid_box, 0)

    for plane in (tp_spread.left, tp_spread.right, tp_spread.far):
        top_table(plane, core)
    for which in range(4):
        top_table(tp_spread.take(which), 1 - core)

    behind = trans_top_ref.shape[0] // 2

    def top_box(k, carry):
        odd = k % 2
        column = (2 * z + odd) * 16 + (k - odd + core)
        sums = [jnp.zeros((8, LANES), F32) for _ in range(4)]
        for j in range(entries):
            n = list_ts[j, column]
            o = offset_ts[j, column]
            pr = p_top[n, 0]
            pi = p_top[n, 1]
            tr = t_top[o]
            ti = t_top[o + behind]
            sums = [sums[0] + pr * tr, sums[1] + pi * ti, sums[2] + pr * ti, sums[3] + pi * tr]
        real = (sums[0] - sums[1]).astype(BF16).astype(F32)
        imag = (sums[2] + sums[3]).astype(BF16).astype(F32)
        top_sum[pl.ds(pl.multiple_of(k * 16, 16), 8), :] = real
        top_sum[pl.ds(pl.multiple_of(k * 16 + 8, 8), 8), :] = imag
        return carry

    lax.fori_loop(0, SECTORS, top_box, 0)

    def top_children(part, carry):
        lanes = pl.ds(pl.multiple_of(part * LANES, LANES), LANES)
        c = cos_top[pl.ds(part, 8, stride=8), :]
        n = sin_top[pl.ds(part, 8, stride=8), :]
        for pair in range(8):
            reals = []
            imags = []
            for half in range(2):
                first = pair * 32 + half * 16
                real = jnp.broadcast_to(top_sum[pl.ds(first + part, 1), :], (8, LANES))
                imag = jnp.broadcast_to(top_sum[pl.ds(first + 8 + part, 1), :], (8, LANES))
                reals.append(real * c + imag * n)
                imags.append(imag * c - real * n)
            child_rows[pair * 16 : pair * 16 + 16, lanes] = jnp.concatenate(reals, axis=0).astype(BF16)
            child_rows[128 + pair * 16 : 144 + pair * 16, lanes] = jnp.concatenate(imags, axis=0).astype(BF16)
        return carry

    lax.fori_loop(0, 8, top_children, 0)
    scale = interp_top.shape[0] / interp_top.shape[1]
    down[...] = scale * lax.dot_general(
        child_rows[...], interp_top[...], (((1,), (1,)), ((), ())), preferred_element_type=F32
    )

    def back_copy(s, landing):
        return pltpu.make_async_remote_copy(
            src_ref=pieces.at[s],
            dst_ref=received.at[landing],
            send_sem=back_send.at[s],
            recv_sem=back_recv.at[landing],
            device_id=to_sector(s),
            device_id_type=MESH,
        )

    def combine(k):
        at = pl.multiple_of(k * 8, 8)
        sides = []
        for side in range(2):
            lanes = slice(side * LANES, side * LANES + LANES)
            parts = [mid_sum[pl.ds(k * 64 + side + 2 * quarter, 8, stride=8), :] for quarter in range(4)]
            real = (parts[0] - parts[3]) + down[pl.ds(at, 8), lanes]
            imag = (parts[1] + parts[2]) + down[pl.ds(pl.multiple_of(128 + k * 8, 8), 8), lanes]
            sides.append(jnp.concatenate([real, imag], axis=0).astype(BF16))
        return jnp.concatenate(sides, axis=1)

    def send_back(k, carry):
        s = nth(k)
        pieces[s] = combine(s)
        back_copy(s, sector).start()
        return carry

    lax.fori_loop(0, SECTORS - 1, send_back, 0)
    received[sector] = combine(sector)
    total[...] = jnp.zeros_like(total)

    def finish_sector(s):
        columns = pl.ds(pl.multiple_of(s * 256, 256), 256)
        c = cos_mid[:, columns]
        n = sin_mid[:, columns]
        found = received[s].astype(F32)
        for pair in range(4):
            reals = []
            imags = []
            for half in range(2):
                box = pair * 2 + half
                real = jnp.broadcast_to(found[box : box + 1], (8, 256))
                imag = jnp.broadcast_to(found[8 + box : 9 + box], (8, 256))
                reals.append(real * c + imag * n)
                imags.append(imag * c - real * n)
            children[pair * 16 : pair * 16 + 16, :] = jnp.concatenate(reals, axis=0).astype(BF16)
            children[64 + pair * 16 : 80 + pair * 16, :] = jnp.concatenate(imags, axis=0).astype(BF16)
        total[...] += lax.dot_general(
            children[...], weights[s], (((1,), (1,)), ((), ())), preferred_element_type=F32
        )

    finish_sector(sector)

    def take_back(k, carry):
        s = nth(k)
        back_copy(s, s).wait_recv()
        finish_sector(s)
        return carry

    lax.fori_loop(0, SECTORS - 1, take_back, 0)
    total[...] = total[...] * (matrix_ref.shape[0] / matrix_ref.shape[1])
    half_rows = total.shape[0] // 2
    outs = [
        pltpu.make_async_copy(total.at[pl.ds(part * half_rows, half_rows)], out_ref.at[part], out_sem.at[part])
        for part in range(2)
    ]
    for copy in outs:
        copy.start()

    def wait_sent(k, carry):
        s = nth(k)
        a2a_copy(s, sector).wait_send()
        back_copy(s, sector).wait_send()
        return carry

    lax.fori_loop(0, SECTORS - 1, wait_sent, 0)

    @pl.when(own)
    def _():
        for index in range(3):
            share_copy(index).wait_send()

    for each in (t_spread, p_spread, tp_spread):
        each.sent()
    for copy in outs:
        copy.wait()


def on_device(
    leaf_out,
    interp_mid,
    shift_mid,
    trans_mid,
    list_mid,
    offset_mid,
    interp_top,
    shift_top,
    trans_top,
    list_top,
    offset_top,
):
    offsets = trans_mid.shape[1]
    entries = list_mid.shape[1]
    rows = 2 * leaf_out.shape[1]
    operands = (
        leaf_out,
        interp_mid,
        shift_mid,
        trans_top.reshape(2 * offsets, LANES),
        jnp.transpose(trans_mid.reshape(2, offsets, 2, LANES), (1, 2, 0, 3)).reshape(4 * offsets, LANES),
        interp_top[0],
        shift_top.reshape(64, LANES),
        list_mid.T,
        offset_mid.T,
        list_top.T,
        offset_top.T,
    )
    padded = 640
    return pl.pallas_call(
        kernel,
        out_shape=jax.ShapeDtypeStruct(leaf_out.shape, F32),
        in_specs=[pl.BlockSpec(memory_space=pltpu.HBM)] * len(operands),
        out_specs=pl.BlockSpec(memory_space=pltpu.HBM),
        scratch_shapes=[
            VMEM(leaf_out.shape, BF16),
            VMEM((SECTORS, interp_mid.shape[0], 256), BF16),
            VMEM(shift_mid.shape, F32),
            VMEM((2 * offsets, LANES), F32),
            VMEM((4 * offsets, LANES), F32),
            VMEM((256, 1024), BF16),
            VMEM((64, LANES), F32),
            VMEM((2, entries, 256), jnp.int32),
            VMEM((2, entries, 128), jnp.int32),
            pltpu.SMEM((entries, 256), jnp.int32),
            pltpu.SMEM((entries, 256), jnp.int32),
            pltpu.SMEM((entries, 128), jnp.int32),
            pltpu.SMEM((entries, 128), jnp.int32),
            VMEM((PLANES, 2, 512, LANES), BF16),
            VMEM((PLANES, 2, 256, LANES), BF16),
            VMEM((PLANES, 2, padded, LANES), BF16),
            VMEM((rows, interp_mid.shape[0]), BF16),
            VMEM(shift_mid.shape, F32),
            VMEM(shift_mid.shape, F32),
            VMEM((SECTORS, 32, LANES), BF16),
            VMEM((64, LANES), F32),
            VMEM((padded, LANES), BF16),
            VMEM((512, LANES), F32),
            VMEM((256, 256), BF16),
            VMEM((256, LANES), F32),
            VMEM((64, LANES), F32),
            VMEM((64, LANES), F32),
            VMEM((1024, 8, LANES), F32),
            VMEM((offsets, 8, LANES), F32),
            VMEM((128, 2, 8, LANES), F32),
            VMEM((padded, 8, LANES), F32),
            VMEM((128 * 8, LANES), F32),
            VMEM((16 * 16, LANES), F32),
            VMEM((256, 1024), BF16),
            VMEM((256, 256), F32),
            VMEM((SECTORS, 16, 256), BF16),
            VMEM((SECTORS, 16, 256), BF16),
            VMEM((rows, 256), BF16),
            VMEM((rows, interp_mid.shape[0]), F32),
            DMA((SECTORS,)),
            DMA((7,)),
            DMA((4,)),
            DMA((SECTORS,)),
            DMA((SECTORS,)),
            DMA((2,)),
            DMA((3,)),
            DMA((3,)),
            DMA((8,)),
            DMA((8,)),
            DMA((8,)),
            DMA((8,)),
            DMA((8,)),
            DMA((8,)),
            DMA((SECTORS,)),
            DMA((SECTORS,)),
            DMA((2,)),
        ],
        compiler_params=pltpu.CompilerParams(
            collective_id=0, has_side_effects=True, vmem_limit_bytes=60 * 1024 * 1024
        ),
        name="far_field",
    )(*operands)


def solution(mesh):
    return jax.shard_map(
        on_device,
        mesh=mesh,
        in_specs=(
            P(None, ("box", "dir"), None),
            P(),
            P(),
            P(None, None, "dir"),
            P(),
            P(),
            P("dir", None, None),
            P(None, "dir", None),
            P(None, None, "dir", "box"),
            P(),
            P(),
        ),
        out_specs=P(None, ("box", "dir"), None),
        check_vma=False,
    )
```

```python
import jax
import jax.numpy as jnp
from jax import lax
from jax.experimental import pallas as pl
from jax.experimental.pallas import tpu as pltpu
from jax.sharding import PartitionSpec as P

MESH = pl.DeviceIdType.MESH
F32 = jnp.float32
BF16 = jnp.bfloat16
VMEM = pltpu.VMEM
DMA = pltpu.SemaphoreType.DMA
PLANES = 4
SECTORS = 16
LANES = 128
EARLY = 3


def place():
    box = lax.axis_index("box")
    way = lax.axis_index("dir")
    low = box % 2
    core = way % 2
    return box // 2, way - core + low, core


def device_of(plane, sector, core):
    low = sector % 2
    return (plane * 2 + low, sector - low + core)


def sin_cos(angle):
    half = angle * 0.5
    sq = half * half
    s = sq * (-1.0 / 39916800.0) + (1.0 / 362880.0)
    s = sq * s - (1.0 / 5040.0)
    s = sq * s + (1.0 / 120.0)
    s = sq * s - (1.0 / 6.0)
    s = half + half * (sq * s)
    c = sq * (1.0 / 479001600.0) - (1.0 / 3628800.0)
    c = sq * c + (1.0 / 40320.0)
    c = sq * c - (1.0 / 720.0)
    c = sq * c + (1.0 / 24.0)
    c = sq * c - 0.5
    c = sq * c + 1.0
    return 2.0 * s * c, 1.0 - 2.0 * s * s


class Spread:
    def __init__(self, ref, send, recv):
        z, sector, core = place()
        self.ref, self.send, self.recv = ref, send, recv
        self.core = core
        self.z = z
        self.left = (z + PLANES - 1) % PLANES
        self.right = (z + 1) % PLANES
        self.far = (z + 2) % PLANES
        self.to_right = device_of(self.right, sector, core)
        self.to_left = device_of(self.left, sector, core)
        self.partner = device_of(z, sector, 1 - core)
        self.rows = ref.shape[2]
        self.crossing = ((4, self.z), (5, self.left), (6, self.right), (7, self.far))

    def copy(self, plane, core, half, index, target):
        rows = self.rows
        if half is None:
            part = self.ref.at[plane, core]
        else:
            part = self.ref.at[plane, core, pl.ds(half * (rows // 2), rows // 2)]
        return pltpu.make_async_remote_copy(
            src_ref=part,
            dst_ref=part,
            send_sem=self.send.at[index],
            recv_sem=self.recv.at[index],
            device_id=target,
            device_id_type=MESH,
        )

    def start_own(self):
        self.copy(self.z, self.core, None, 0, self.to_right).start()
        self.copy(self.z, self.core, None, 1, self.to_left).start()
        self.copy(self.z, self.core, None, 4, self.partner).start()

    def forward(self):
        self.copy(self.left, self.core, None, 0, self.to_right).wait_recv()
        self.copy(self.left, self.core, 0, 2, self.to_right).start()
        self.copy(self.left, self.core, None, 5, self.partner).start()
        self.copy(self.right, self.core, None, 1, self.to_left).wait_recv()
        self.copy(self.right, self.core, 1, 3, self.to_left).start()
        self.copy(self.right, self.core, None, 6, self.partner).start()

    def forward_far(self):
        self.copy(self.far, self.core, 0, 2, self.to_right).wait_recv()
        self.copy(self.far, self.core, 1, 3, self.to_left).wait_recv()
        self.copy(self.far, self.core, None, 7, self.partner).start()

    def take(self, which):
        index, plane = self.crossing[which]
        self.copy(plane, 1 - self.core, None, index, self.partner).wait_recv()
        return plane

    def sent(self):
        self.copy(self.z, self.core, None, 0, self.to_right).wait_send()
        self.copy(self.z, self.core, None, 1, self.to_left).wait_send()
        self.copy(self.left, self.core, 0, 2, self.to_right).wait_send()
        self.copy(self.right, self.core, 1, 3, self.to_left).wait_send()
        for index, plane in self.crossing:
            self.copy(plane, self.core, None, index, self.partner).wait_send()


def kernel(
    leaf_ref,
    matrix_ref,
    shift_mid_ref,
    trans_top_ref,
    trans_mid_ref,
    interp_top_ref,
    shift_top_ref,
    list_mid_ref,
    offset_mid_ref,
    list_top_ref,
    offset_top_ref,
    out_ref,
    leaf,
    weights,
    shift_mid,
    trans_top,
    trans_mid,
    interp_top,
    shift_top,
    lists_mid,
    lists_top,
    scaled_mid,
    scaled_top,
    list_s,
    offset_s,
    list_ts,
    offset_ts,
    p_all,
    tp_all,
    t_all,
    leaf_rows,
    cos_mid,
    sin_mid,
    sending,
    stage,
    piece,
    block_f32,
    top_lhs,
    top_f32,
    cos_top,
    sin_top,
    p_tab,
    t_tab,
    p_top,
    t_top,
    mid_sum,
    top_sum,
    child_rows,
    down,
    pieces,
    received,
    children,
    total,
    weight_sem,
    load_sem,
    index_sem,
    a2a_send,
    a2a_recv,
    swap_sem,
    share_send,
    share_recv,
    t_send,
    t_recv,
    p_send,
    p_recv,
    tp_send,
    tp_recv,
    back_send,
    back_recv,
    out_sem,
):
    z, sector, core = place()
    low = sector % 2
    own = low == core
    partner = device_of(z, sector, 1 - core)
    swap = device_of(z, sector - low + core, low)
    right = device_of((z + 1) % PLANES, sector, core)
    left = device_of((z + PLANES - 1) % PLANES, sector, core)
    t_spread = Spread(t_all, t_send, t_recv)
    p_spread = Spread(p_all, p_send, p_recv)
    tp_spread = Spread(tp_all, tp_send, tp_recv)

    def nth(k):
        return (sector + 1 + k) % SECTORS

    def to_sector(s):
        return device_of(z, s, core)

    barrier = pltpu.get_barrier_semaphore()

    def signal_peer(k, carry):
        pl.semaphore_signal(barrier, inc=1, device_id=to_sector(nth(k)), device_id_type=MESH)
        return carry

    lax.fori_loop(0, SECTORS - 1, signal_peer, 0)
    for device in (right, left, partner):
        pl.semaphore_signal(barrier, inc=1, device_id=device, device_id_type=MESH)

    @pl.when(jnp.logical_not(own))
    def _():
        pl.semaphore_signal(barrier, inc=1, device_id=swap, device_id_type=MESH)

    slab = pl.ds(pl.multiple_of(z * 256, 256), 256)
    loads = [
        pltpu.make_async_copy(source, target, load_sem.at[index])
        for index, (source, target) in enumerate(
            (
                (leaf_ref, leaf),
                (trans_top_ref, trans_top),
                (shift_mid_ref, shift_mid),
                (list_mid_ref.at[:, slab], lists_mid.at[0]),
                (offset_mid_ref.at[:, slab], lists_mid.at[1]),
                (list_top_ref, lists_top.at[0]),
                (offset_top_ref, lists_top.at[1]),
            )
        )
    ]
    for copy in loads[:3]:
        copy.start()

    def weight_copy(s):
        return pltpu.make_async_copy(
            matrix_ref.at[:, pl.ds(pl.multiple_of(s * 256, 256), 256)], weights.at[s], weight_sem.at[s]
        )

    def start_weight(k, carry):
        weight_copy(nth(k)).start()
        return carry

    lax.fori_loop(0, SECTORS, start_weight, 0)
    for copy in loads[3:]:
        copy.start()

    loads[0].wait()
    rows = 2 * leaf.shape[1]
    target = lax.broadcasted_iota(jnp.int32, (rows, rows), 0)
    source = lax.broadcasted_iota(jnp.int32, (rows, rows), 1)
    wanted = (target & 64) + ((target & 7) << 3) + ((target >> 3) & 7)
    order = (source == wanted).astype(BF16)
    both = jnp.concatenate([leaf[0], leaf[1]], axis=0)
    leaf_rows[...] = jnp.dot(order, both, preferred_element_type=F32).astype(BF16)

    loads[1].wait()
    used = trans_top.shape[0]
    piece[0:used, :] = trans_top[...].astype(BF16)
    piece[used:, :] = jnp.zeros((piece.shape[0] - used, LANES), BF16)

    swap_copy = pltpu.make_async_remote_copy(
        src_ref=piece,
        dst_ref=t_all.at[z, low],
        send_sem=swap_sem.at[0],
        recv_sem=swap_sem.at[1],
        device_id=swap,
        device_id_type=MESH,
    )
    shared = ((trans_mid_ref, trans_mid), (interp_top_ref, interp_top), (shift_top_ref, shift_top))

    def share_copy(index):
        return pltpu.make_async_remote_copy(
            src_ref=shared[index][0],
            dst_ref=shared[index][1],
            send_sem=share_send.at[index],
            recv_sem=share_recv.at[index],
            device_id=partner,
            device_id_type=MESH,
        )

    def local_copy(index):
        return pltpu.make_async_copy(shared[index][0], shared[index][1], share_recv.at[index])

    loads[2].wait()
    sines, cosines = sin_cos(shift_mid[...])
    cos_mid[...] = cosines
    sin_mid[...] = sines

    def parents(s, slot):
        columns = pl.ds(pl.multiple_of(s * 256, 256), 256)
        weight_copy(s).wait()
        spread = jnp.dot(leaf_rows[...], weights[s], preferred_element_type=F32)
        real_sum = jnp.zeros((8, 256), F32)
        imag_sum = jnp.zeros((8, 256), F32)
        for child in range(8):
            real = spread[child * 8 : child * 8 + 8]
            imag = spread[64 + child * 8 : 64 + child * 8 + 8]
            c = cos_mid[child : child + 1, columns]
            n = sin_mid[child : child + 1, columns]
            real_sum += real * c - imag * n
            imag_sum += real * n + imag * c
        for part in range(2):
            lanes = slice(part * LANES, part * LANES + LANES)
            stage[pl.ds(slot * 32 + part, 8, stride=4), :] = real_sum[:, lanes]
            stage[pl.ds(slot * 32 + 2 + part, 8, stride=4), :] = imag_sum[:, lanes]
        return stage[slot * 32 : slot * 32 + 32, :].astype(BF16)

    def rows_of(s):
        return p_all.at[z, core, pl.ds(pl.multiple_of(s * 32, 32), 32)]

    def a2a_copy(s, landing):
        return pltpu.make_async_remote_copy(
            src_ref=sending.at[s],
            dst_ref=rows_of(landing),
            send_sem=a2a_send.at[s],
            recv_sem=a2a_recv.at[landing],
            device_id=to_sector(s),
            device_id_type=MESH,
        )

    def make_pair(k, carry):
        first, second = nth(2 * k), nth(2 * k + 1)
        sending[first] = parents(first, 0)
        sending[second] = parents(second, 1)
        return carry

    def start_pair(k, carry):
        a2a_copy(nth(2 * k), sector).start()
        a2a_copy(nth(2 * k + 1), sector).start()
        return carry

    def send_pair(k, carry):
        make_pair(k, carry)
        return start_pair(k, carry)

    lax.fori_loop(0, EARLY, make_pair, 0)
    pl.semaphore_wait(barrier, SECTORS - 1 + 3 + (low + core) % 2)

    @pl.when(own)
    def _():
        for index in range(3):
            share_copy(index).start()
            local_copy(index).start()
        t_all[z, core] = piece[...]

    @pl.when(jnp.logical_not(own))
    def _():
        swap_copy.start()

    lax.fori_loop(0, EARLY, start_pair, 0)
    lax.fori_loop(EARLY, 7, send_pair, 0)
    last = nth(SECTORS - 2)
    sending[last] = parents(last, 0)
    a2a_copy(last, sector).start()
    p_all[z, core, pl.ds(pl.multiple_of(sector * 32, 32), 32), :] = parents(sector, 1)

    @pl.when(jnp.logical_not(own))
    def _():
        swap_copy.wait()

    t_spread.start_own()

    for copy in loads[3:]:
        copy.wait()
    scaled_mid[...] = lists_mid[...] * 8
    scaled_top[0] = lists_top[0] * 16
    scaled_top[1] = lists_top[1] * 8
    to_smem = [
        pltpu.make_async_copy(source, target, index_sem.at[index])
        for index, (source, target) in enumerate(
            (
                (scaled_mid.at[0, :, 0:128], list_s.at[0]),
                (scaled_mid.at[0, :, 128:256], list_s.at[1]),
                (scaled_mid.at[1, :, 0:128], offset_s.at[0]),
                (scaled_mid.at[1, :, 128:256], offset_s.at[1]),
                (scaled_top.at[0], list_ts),
                (scaled_top.at[1], offset_ts),
            )
        )
    ]
    for copy in to_smem:
        copy.start()

    @pl.when(own)
    def _():
        for index in range(3):
            local_copy(index).wait()

    @pl.when(jnp.logical_not(own))
    def _():
        for index in range(3):
            share_copy(index).wait_recv()

    offsets = trans_mid.shape[0] // 4

    def put_offsets(first, row):
        for quarter, places in enumerate(((0, 2), (4, 6), (1, 3), (5, 7))):
            v = trans_mid[pl.ds(first + quarter, 8, stride=4), :]
            for at in places:
                t_tab[pl.ds(row + at, 8, stride=8), :] = v

    def mid_offsets(k, carry):
        put_offsets(pl.multiple_of(k * 32, 32), pl.multiple_of(k * 64, 64))
        return carry

    lax.fori_loop(0, offsets // 8, mid_offsets, 0)
    if offsets % 8:
        put_offsets((offsets - 8) * 4, (offsets - 8) * 8)

    sines_t, cosines_t = sin_cos(shift_top[...])
    cos_top[...] = cosines_t
    sin_top[...] = sines_t

    def wait_sector(k, carry):
        s = nth(k)
        a2a_copy(s, s).wait_recv()
        return carry

    lax.fori_loop(0, SECTORS - 1, wait_sector, 0)
    p_spread.start_own()

    block_f32[...] = p_all[z, core].astype(F32)
    for child in range(8):
        for part in range(2):
            for side in range(2):
                first = child * 4 + part * 2 + side
                a = block_f32[pl.ds(first, 8, stride=32), :]
                b = block_f32[pl.ds(256 + first, 8, stride=32), :]
                top_lhs[
                    part * 128 + child * 16 : part * 128 + child * 16 + 16, side * LANES : side * LANES + LANES
                ] = jnp.concatenate([a, b], axis=0).astype(BF16)

    def top_columns(k, carry):
        columns = pl.ds(pl.multiple_of(k * 256, 256), 256)
        spread = jnp.dot(top_lhs[...], interp_top[:, columns], preferred_element_type=F32)
        for part in range(2):
            lanes = slice(part * LANES, part * LANES + LANES)
            group = k * 2 + part
            real_sum = jnp.zeros((16, LANES), F32)
            imag_sum = jnp.zeros((16, LANES), F32)
            for child in range(8):
                real = spread[child * 16 : child * 16 + 16, lanes]
                imag = spread[128 + child * 16 : 128 + child * 16 + 16, lanes]
                c = cos_top[pl.ds(child * 8 + group, 1), :]
                n = sin_top[pl.ds(child * 8 + group, 1), :]
                real_sum += real * c - imag * n
                imag_sum += real * n + imag * c
            for half in range(2):
                boxes = slice(half * 8, half * 8 + 8)
                top_f32[pl.ds(half * 128 + group, 8, stride=16), :] = real_sum[boxes]
                top_f32[pl.ds(half * 128 + 8 + group, 8, stride=16), :] = imag_sum[boxes]
        return carry

    lax.fori_loop(0, 4, top_columns, 0)
    tp_all[z, core] = top_f32[...].astype(BF16)
    tp_spread.start_own()

    upper = lax.broadcasted_iota(jnp.int32, (8, LANES), 0) < 4

    def mid_table(plane, side):
        def one(s, carry):
            odd = s % 2
            first = ((2 * plane + odd) * 128 + (s - odd + side) * 8) * 8
            found = p_all[plane, side, pl.ds(pl.multiple_of(s * 32, 32), 32), :].astype(F32)
            for pair in range(4):
                v = found[pair * 8 : pair * 8 + 8]
                r = pltpu.roll(v, 4, 0)
                at = first + pair * 16
                p_tab[pl.ds(pl.multiple_of(at, 8), 8), :] = jnp.where(upper, v, r)
                p_tab[pl.ds(pl.multiple_of(at + 8, 8), 8), :] = jnp.where(upper, r, v)
            return carry

        lax.fori_loop(0, SECTORS, one, 0)

    def top_table(plane, side):
        def one(s, carry):
            odd = s % 2
            found = tp_all[plane, side, pl.ds(pl.multiple_of(s * 16, 16), 16), :].astype(F32)
            first = ((2 * plane + odd) * 16 + (s - odd + side)) * 16
            p_top[pl.ds(pl.multiple_of(first, 16), 16), :] = found
            return carry

        lax.fori_loop(0, SECTORS, one, 0)

    def offset_table(plane, side):
        at = plane * 2 + side

        def one(k, carry):
            found = t_all[plane, side, pl.ds(pl.multiple_of(k * 16, 16), 16), :].astype(F32)
            for half in range(2):
                t_top[pl.ds(k * 128 + half * 64 + at, 8, stride=8), :] = found[half * 8 : half * 8 + 8]
            return carry

        lax.fori_loop(0, t_all.shape[2] // 16, one, 0)

    mid_table(z, core)
    top_table(z, core)
    offset_table(z, core)
    t_spread.forward()
    p_spread.forward()
    tp_spread.forward()
    mid_table(p_spread.left, core)
    mid_table(p_spread.right, core)
    mid_table(p_spread.take(0), 1 - core)
    p_spread.forward_far()
    t_spread.forward_far()
    tp_spread.forward_far()
    for plane in (p_spread.left, p_spread.right, p_spread.far):
        offset_table(plane, core)
        top_table(plane, core)
    mid_table(p_spread.take(1), 1 - core)
    mid_table(p_spread.take(2), 1 - core)
    mid_table(p_spread.far, core)
    mid_table(p_spread.take(3), 1 - core)
    for which in range(4):
        offset_table(t_spread.take(which), 1 - core)
        top_table(tp_spread.take(which), 1 - core)
    for copy in to_smem:
        copy.wait()

    entries = list_mid_ref.shape[0]

    behind = (trans_top_ref.shape[0] // 2) * 8

    def top_box(k, carry):
        odd = k % 2
        column = (2 * z + odd) * 16 + (k - odd + core)
        sums = [jnp.zeros((8, LANES), F32) for _ in range(4)]
        for j in range(entries):
            n = list_ts[j, column]
            o = offset_ts[j, column]
            pr = p_top[pl.ds(n, 8), :]
            pi = p_top[pl.ds(n + 8, 8), :]
            tr = t_top[pl.ds(o, 8), :]
            ti = t_top[pl.ds(o + behind, 8), :]
            sums = [sums[0] + pr * tr, sums[1] + pi * ti, sums[2] + pr * ti, sums[3] + pi * tr]
        real = (sums[0] - sums[1]).astype(BF16).astype(F32)
        imag = (sums[2] + sums[3]).astype(BF16).astype(F32)
        top_sum[pl.ds(pl.multiple_of(k * 16, 16), 8), :] = real
        top_sum[pl.ds(pl.multiple_of(k * 16 + 8, 8), 8), :] = imag
        return carry

    lax.fori_loop(0, SECTORS, top_box, 0)

    def top_children(part, carry):
        lanes = pl.ds(pl.multiple_of(part * LANES, LANES), LANES)
        c = cos_top[pl.ds(part, 8, stride=8), :]
        n = sin_top[pl.ds(part, 8, stride=8), :]
        for pair in range(8):
            reals = []
            imags = []
            for half in range(2):
                first = pair * 32 + half * 16
                real = jnp.broadcast_to(top_sum[pl.ds(first + part, 1), :], (8, LANES))
                imag = jnp.broadcast_to(top_sum[pl.ds(first + 8 + part, 1), :], (8, LANES))
                reals.append(real * c + imag * n)
                imags.append(imag * c - real * n)
            child_rows[pair * 16 : pair * 16 + 16, lanes] = jnp.concatenate(reals, axis=0).astype(BF16)
            child_rows[128 + pair * 16 : 144 + pair * 16, lanes] = jnp.concatenate(imags, axis=0).astype(BF16)
        return carry

    lax.fori_loop(0, 8, top_children, 0)
    scale = interp_top.shape[0] / interp_top.shape[1]
    down[...] = scale * lax.dot_general(
        child_rows[...], interp_top[...], (((1,), (1,)), ((), ())), preferred_element_type=F32
    )

    def back_copy(s, landing):
        return pltpu.make_async_remote_copy(
            src_ref=pieces.at[s],
            dst_ref=received.at[landing],
            send_sem=back_send.at[s],
            recv_sem=back_recv.at[landing],
            device_id=to_sector(s),
            device_id_type=MESH,
        )

    def combine(k):
        odd = k % 2
        column = (k - odd + core) * 8

        def mid_box(i, carry):
            kept = jnp.zeros((8, LANES), F32)
            for j in range(entries):
                p = p_tab[pl.ds(list_s[odd, j, column + i], 8), :]
                t = t_tab[pl.ds(offset_s[odd, j, column + i], 8), :]
                kept = kept + p * t
            mid_sum[pl.ds(pl.multiple_of(i * 8, 8), 8), :] = kept
            return carry

        lax.fori_loop(0, 8, mid_box, 0)
        at = pl.multiple_of(k * 8, 8)
        sides = []
        for side in range(2):
            lanes = slice(side * LANES, side * LANES + LANES)
            parts = [mid_sum[pl.ds(side + 2 * quarter, 8, stride=8), :] for quarter in range(4)]
            real = (parts[0] - parts[3]) + down[pl.ds(at, 8), lanes]
            imag = (parts[1] + parts[2]) + down[pl.ds(pl.multiple_of(128 + k * 8, 8), 8), lanes]
            sides.append(jnp.concatenate([real, imag], axis=0).astype(BF16))
        return jnp.concatenate(sides, axis=1)

    def send_back(k, carry):
        s = nth(k)
        pieces[s] = combine(s)
        back_copy(s, sector).start()
        return carry

    lax.fori_loop(0, SECTORS - 1, send_back, 0)
    received[sector] = combine(sector)
    total[...] = jnp.zeros_like(total)

    def finish_sector(s):
        columns = pl.ds(pl.multiple_of(s * 256, 256), 256)
        c = cos_mid[:, columns]
        n = sin_mid[:, columns]
        found = received[s].astype(F32)
        for pair in range(4):
            reals = []
            imags = []
            for half in range(2):
                box = pair * 2 + half
                real = jnp.broadcast_to(found[box : box + 1], (8, 256))
                imag = jnp.broadcast_to(found[8 + box : 9 + box], (8, 256))
                reals.append(real * c + imag * n)
                imags.append(imag * c - real * n)
            children[pair * 16 : pair * 16 + 16, :] = jnp.concatenate(reals, axis=0).astype(BF16)
            children[64 + pair * 16 : 80 + pair * 16, :] = jnp.concatenate(imags, axis=0).astype(BF16)
        total[...] += lax.dot_general(
            children[...], weights[s], (((1,), (1,)), ((), ())), preferred_element_type=F32
        )

    finish_sector(sector)

    def take_back(k, carry):
        s = nth(k)
        back_copy(s, s).wait_recv()
        finish_sector(s)
        return carry

    lax.fori_loop(0, SECTORS - 1, take_back, 0)
    total[...] = total[...] * (matrix_ref.shape[0] / matrix_ref.shape[1])
    half_rows = total.shape[0] // 2
    outs = [
        pltpu.make_async_copy(total.at[pl.ds(part * half_rows, half_rows)], out_ref.at[part], out_sem.at[part])
        for part in range(2)
    ]
    for copy in outs:
        copy.start()

    def wait_sent(k, carry):
        s = nth(k)
        a2a_copy(s, sector).wait_send()
        back_copy(s, sector).wait_send()
        return carry

    lax.fori_loop(0, SECTORS - 1, wait_sent, 0)

    @pl.when(own)
    def _():
        for index in range(3):
            share_copy(index).wait_send()

    for each in (t_spread, p_spread, tp_spread):
        each.sent()
    for copy in outs:
        copy.wait()


def on_device(
    leaf_out,
    interp_mid,
    shift_mid,
    trans_mid,
    list_mid,
    offset_mid,
    interp_top,
    shift_top,
    trans_top,
    list_top,
    offset_top,
):
    offsets = trans_mid.shape[1]
    entries = list_mid.shape[1]
    rows = 2 * leaf_out.shape[1]
    operands = (
        leaf_out,
        interp_mid,
        shift_mid,
        trans_top.reshape(2 * offsets, LANES),
        jnp.transpose(trans_mid.reshape(2, offsets, 2, LANES), (1, 2, 0, 3)).reshape(4 * offsets, LANES),
        interp_top[0],
        shift_top.reshape(64, LANES),
        list_mid.T,
        offset_mid.T,
        list_top.T,
        offset_top.T,
    )
    padded = 640
    return pl.pallas_call(
        kernel,
        out_shape=jax.ShapeDtypeStruct(leaf_out.shape, F32),
        in_specs=[pl.BlockSpec(memory_space=pltpu.HBM)] * len(operands),
        out_specs=pl.BlockSpec(memory_space=pltpu.HBM),
        scratch_shapes=[
            VMEM(leaf_out.shape, BF16),
            VMEM((SECTORS, interp_mid.shape[0], 256), BF16),
            VMEM(shift_mid.shape, F32),
            VMEM((2 * offsets, LANES), F32),
            VMEM((4 * offsets, LANES), F32),
            VMEM((256, 1024), BF16),
            VMEM((64, LANES), F32),
            VMEM((2, entries, 256), jnp.int32),
            VMEM((2, entries, 128), jnp.int32),
            VMEM((2, entries, 256), jnp.int32),
            VMEM((2, entries, 128), jnp.int32),
            pltpu.SMEM((2, entries, 128), jnp.int32),
            pltpu.SMEM((2, entries, 128), jnp.int32),
            pltpu.SMEM((entries, 128), jnp.int32),
            pltpu.SMEM((entries, 128), jnp.int32),
            VMEM((PLANES, 2, 512, LANES), BF16),
            VMEM((PLANES, 2, 256, LANES), BF16),
            VMEM((PLANES, 2, padded, LANES), BF16),
            VMEM((rows, interp_mid.shape[0]), BF16),
            VMEM(shift_mid.shape, F32),
            VMEM(shift_mid.shape, F32),
            VMEM((SECTORS, 32, LANES), BF16),
            VMEM((64, LANES), F32),
            VMEM((padded, LANES), BF16),
            VMEM((512, LANES), F32),
            VMEM((256, 256), BF16),
            VMEM((256, LANES), F32),
            VMEM((64, LANES), F32),
            VMEM((64, LANES), F32),
            VMEM((1024 * 8, LANES), F32),
            VMEM((offsets * 8, LANES), F32),
            VMEM((128 * 16, LANES), F32),
            VMEM((padded * 8, LANES), F32),
            VMEM((8 * 8, LANES), F32),
            VMEM((16 * 16, LANES), F32),
            VMEM((256, 1024), BF16),
            VMEM((256, 256), F32),
            VMEM((SECTORS, 16, 256), BF16),
            VMEM((SECTORS, 16, 256), BF16),
            VMEM((rows, 256), BF16),
            VMEM((rows, interp_mid.shape[0]), F32),
            DMA((SECTORS,)),
            DMA((7,)),
            DMA((6,)),
            DMA((SECTORS,)),
            DMA((SECTORS,)),
            DMA((2,)),
            DMA((3,)),
            DMA((3,)),
            DMA((8,)),
            DMA((8,)),
            DMA((8,)),
            DMA((8,)),
            DMA((8,)),
            DMA((8,)),
            DMA((SECTORS,)),
            DMA((SECTORS,)),
            DMA((2,)),
        ],
        compiler_params=pltpu.CompilerParams(
            collective_id=0, has_side_effects=True, vmem_limit_bytes=60 * 1024 * 1024
        ),
        name="far_field",
    )(*operands)


def solution(mesh):
    return jax.shard_map(
        on_device,
        mesh=mesh,
        in_specs=(
            P(None, ("box", "dir"), None),
            P(),
            P(),
            P(None, None, "dir"),
            P(),
            P(),
            P("dir", None, None),
            P(None, "dir", None),
            P(None, None, "dir", "box"),
            P(),
            P(),
        ),
        out_specs=P(None, ("box", "dir"), None),
        check_vma=False,
    )
```

```python
import jax
import jax.numpy as jnp
from jax import lax
from jax.experimental import pallas as pl
from jax.experimental.pallas import tpu as pltpu
from jax.sharding import PartitionSpec as P

MESH = pl.DeviceIdType.MESH
F32 = jnp.float32
BF16 = jnp.bfloat16
VMEM = pltpu.VMEM
DMA = pltpu.SemaphoreType.DMA
PLANES = 4
SECTORS = 16
LANES = 128


def place():
    box = lax.axis_index("box")
    way = lax.axis_index("dir")
    low = box % 2
    core = way % 2
    return box // 2, way - core + low, core


def device_of(plane, sector, core):
    low = sector % 2
    return (plane * 2 + low, sector - low + core)


def sin_cos(angle):
    half = angle * 0.5
    sq = half * half
    s = sq * (-1.0 / 39916800.0) + (1.0 / 362880.0)
    s = sq * s - (1.0 / 5040.0)
    s = sq * s + (1.0 / 120.0)
    s = sq * s - (1.0 / 6.0)
    s = half + half * (sq * s)
    c = sq * (1.0 / 479001600.0) - (1.0 / 3628800.0)
    c = sq * c + (1.0 / 40320.0)
    c = sq * c - (1.0 / 720.0)
    c = sq * c + (1.0 / 24.0)
    c = sq * c - 0.5
    c = sq * c + 1.0
    return 2.0 * s * c, 1.0 - 2.0 * s * s


class Spread:
    def __init__(self, ref, send, recv):
        z, sector, core = place()
        self.ref, self.send, self.recv = ref, send, recv
        self.core = core
        self.z = z
        self.left = (z + PLANES - 1) % PLANES
        self.right = (z + 1) % PLANES
        self.far = (z + 2) % PLANES
        self.to_right = device_of(self.right, sector, core)
        self.to_left = device_of(self.left, sector, core)
        self.partner = device_of(z, sector, 1 - core)
        self.rows = ref.shape[2]
        self.crossing = ((4, self.z), (5, self.left), (6, self.right), (7, self.far))

    def copy(self, plane, core, half, index, target):
        rows = self.rows
        if half is None:
            part = self.ref.at[plane, core]
        else:
            part = self.ref.at[plane, core, pl.ds(half * (rows // 2), rows // 2)]
        return pltpu.make_async_remote_copy(
            src_ref=part,
            dst_ref=part,
            send_sem=self.send.at[index],
            recv_sem=self.recv.at[index],
            device_id=target,
            device_id_type=MESH,
        )

    def start_own(self):
        self.copy(self.z, self.core, None, 0, self.to_right).start()
        self.copy(self.z, self.core, None, 1, self.to_left).start()
        self.copy(self.z, self.core, None, 4, self.partner).start()

    def forward(self):
        self.copy(self.left, self.core, None, 0, self.to_right).wait_recv()
        self.copy(self.left, self.core, 0, 2, self.to_right).start()
        self.copy(self.left, self.core, None, 5, self.partner).start()
        self.copy(self.right, self.core, None, 1, self.to_left).wait_recv()
        self.copy(self.right, self.core, 1, 3, self.to_left).start()
        self.copy(self.right, self.core, None, 6, self.partner).start()

    def forward_far(self):
        self.copy(self.far, self.core, 0, 2, self.to_right).wait_recv()
        self.copy(self.far, self.core, 1, 3, self.to_left).wait_recv()
        self.copy(self.far, self.core, None, 7, self.partner).start()

    def take(self, which):
        index, plane = self.crossing[which]
        self.copy(plane, 1 - self.core, None, index, self.partner).wait_recv()
        return plane

    def sent(self):
        self.copy(self.z, self.core, None, 0, self.to_right).wait_send()
        self.copy(self.z, self.core, None, 1, self.to_left).wait_send()
        self.copy(self.left, self.core, 0, 2, self.to_right).wait_send()
        self.copy(self.right, self.core, 1, 3, self.to_left).wait_send()
        for index, plane in self.crossing:
            self.copy(plane, self.core, None, index, self.partner).wait_send()


def kernel(
    leaf_ref,
    matrix_ref,
    shift_mid_ref,
    trans_top_ref,
    trans_mid_ref,
    interp_top_ref,
    shift_top_ref,
    list_mid_ref,
    offset_mid_ref,
    list_top_ref,
    offset_top_ref,
    out_ref,
    leaf,
    weights,
    shift_mid,
    trans_top,
    trans_mid,
    interp_top,
    shift_top,
    lists_mid,
    lists_top,
    scaled_mid,
    scaled_top,
    list_s,
    offset_s,
    list_ts,
    offset_ts,
    p_all,
    tp_all,
    t_all,
    leaf_rows,
    cos_mid,
    sin_mid,
    sending,
    stage,
    piece,
    block_f32,
    top_lhs,
    top_f32,
    cos_top,
    sin_top,
    p_tab,
    t_tab,
    p_top,
    t_top,
    mid_sum,
    top_sum,
    child_rows,
    down,
    pieces,
    received,
    children,
    total,
    weight_sem,
    load_sem,
    index_sem,
    a2a_send,
    a2a_recv,
    swap_sem,
    share_send,
    share_recv,
    t_send,
    t_recv,
    p_send,
    p_recv,
    tp_send,
    tp_recv,
    back_send,
    back_recv,
):
    z, sector, core = place()
    entries = list_mid_ref.shape[0]
    low = sector % 2
    own = low == core
    partner = device_of(z, sector, 1 - core)
    swap = device_of(z, sector - low + core, low)
    right = device_of((z + 1) % PLANES, sector, core)
    left = device_of((z + PLANES - 1) % PLANES, sector, core)
    t_spread = Spread(t_all, t_send, t_recv)
    p_spread = Spread(p_all, p_send, p_recv)
    tp_spread = Spread(tp_all, tp_send, tp_recv)

    group = sector // 4
    inside = sector % 4

    def nth(k):
        return ((group + 1 + k // 4) % 4) * 4 + (inside + 1 + k % 4) % 4

    def from_nth(k):
        return ((group + 7 - k // 4) % 4) * 4 + (inside + 7 - k % 4) % 4

    def to_sector(s):
        return device_of(z, s, core)

    barrier = pltpu.get_barrier_semaphore()

    def signal_peer(k, carry):
        pl.semaphore_signal(barrier, inc=1, device_id=to_sector(nth(k)), device_id_type=MESH)
        return carry

    lax.fori_loop(0, SECTORS - 1, signal_peer, 0)
    for device in (right, left, partner):
        pl.semaphore_signal(barrier, inc=1, device_id=device, device_id_type=MESH)

    @pl.when(jnp.logical_not(own))
    def _():
        pl.semaphore_signal(barrier, inc=1, device_id=swap, device_id_type=MESH)

    slab = pl.ds(pl.multiple_of(z * 256, 256), 256)
    loads = [
        pltpu.make_async_copy(source, target, load_sem.at[index])
        for index, (source, target) in enumerate(
            (
                (leaf_ref, leaf),
                (trans_top_ref, trans_top),
                (shift_mid_ref, shift_mid),
                (list_mid_ref.at[:, slab], lists_mid.at[0]),
                (offset_mid_ref.at[:, slab], lists_mid.at[1]),
                (list_top_ref, lists_top.at[0]),
                (offset_top_ref, lists_top.at[1]),
            )
        )
    ]
    for copy in loads[:3]:
        copy.start()

    def weight_copy(piece_at):
        columns = pl.ds(pl.multiple_of((group + 1 + piece_at) % 4 * 1024, 1024), 1024)
        return pltpu.make_async_copy(matrix_ref.at[:, columns], weights.at[:, columns], weight_sem.at[piece_at])

    for piece_at in range(4):
        weight_copy(piece_at).start()
    for copy in loads[3:]:
        copy.start()

    loads[0].wait()
    rows = 2 * leaf.shape[1]
    target = lax.broadcasted_iota(jnp.int32, (rows, rows), 0)
    source = lax.broadcasted_iota(jnp.int32, (rows, rows), 1)
    wanted = (target & 64) + ((target & 7) << 3) + ((target >> 3) & 7)
    order = (source == wanted).astype(BF16)
    both = jnp.concatenate([leaf[0], leaf[1]], axis=0)
    leaf_rows[...] = jnp.dot(order, both, preferred_element_type=F32).astype(BF16)

    loads[1].wait()
    used = trans_top.shape[0]
    piece[0:used, :] = trans_top[...].astype(BF16)
    piece[used:, :] = jnp.zeros((piece.shape[0] - used, LANES), BF16)

    swap_copy = pltpu.make_async_remote_copy(
        src_ref=piece,
        dst_ref=t_all.at[z, low],
        send_sem=swap_sem.at[0],
        recv_sem=swap_sem.at[1],
        device_id=swap,
        device_id_type=MESH,
    )
    shared = ((trans_mid_ref, trans_mid), (interp_top_ref, interp_top), (shift_top_ref, shift_top))

    def share_copy(index):
        return pltpu.make_async_remote_copy(
            src_ref=shared[index][0],
            dst_ref=shared[index][1],
            send_sem=share_send.at[index],
            recv_sem=share_recv.at[index],
            device_id=partner,
            device_id_type=MESH,
        )

    def local_copy(index):
        return pltpu.make_async_copy(shared[index][0], shared[index][1], share_recv.at[index])

    loads[2].wait()
    sines, cosines = sin_cos(shift_mid[...])
    cos_mid[...] = cosines
    sin_mid[...] = sines

    def parents(s, slot):
        columns = pl.ds(pl.multiple_of(s * 256, 256), 256)
        spread = jnp.dot(leaf_rows[...], weights[:, columns], preferred_element_type=F32)
        real_sum = jnp.zeros((8, 256), F32)
        imag_sum = jnp.zeros((8, 256), F32)
        for child in range(8):
            real = spread[child * 8 : child * 8 + 8]
            imag = spread[64 + child * 8 : 64 + child * 8 + 8]
            c = cos_mid[child : child + 1, columns]
            n = sin_mid[child : child + 1, columns]
            real_sum += real * c - imag * n
            imag_sum += real * n + imag * c
        for part in range(2):
            lanes = slice(part * LANES, part * LANES + LANES)
            stage[pl.ds(slot * 32 + part, 8, stride=4), :] = real_sum[:, lanes]
            stage[pl.ds(slot * 32 + 2 + part, 8, stride=4), :] = imag_sum[:, lanes]
        return stage[slot * 32 : slot * 32 + 32, :].astype(BF16)

    def rows_of(s):
        return p_all.at[z, core, pl.ds(pl.multiple_of(s * 32, 32), 32)]

    def a2a_copy(s, landing):
        return pltpu.make_async_remote_copy(
            src_ref=sending.at[s],
            dst_ref=rows_of(landing),
            send_sem=a2a_send.at[s],
            recv_sem=a2a_recv.at[landing],
            device_id=to_sector(s),
            device_id_type=MESH,
        )

    def make_four(piece_at):
        weight_copy(piece_at).wait()
        for slot in range(4):
            s = nth(piece_at * 4 + slot)
            sending[s] = parents(s, slot)

    def start_four(piece_at):
        for slot in range(4):
            a2a_copy(nth(piece_at * 4 + slot), sector).start()

    make_four(0)
    pl.semaphore_wait(barrier, SECTORS - 1 + 3 + (low + core) % 2)

    @pl.when(own)
    def _():
        for index in range(3):
            share_copy(index).start()
            local_copy(index).start()
        t_all[z, core] = piece[...]
        t_spread.start_own()

    @pl.when(jnp.logical_not(own))
    def _():
        swap_copy.start()

    start_four(0)

    def send_four(piece_at, carry):
        make_four(piece_at)
        start_four(piece_at)
        return carry

    lax.fori_loop(1, 3, send_four, 0)
    weight_copy(3).wait()
    for slot in range(3):
        s = nth(12 + slot)
        sending[s] = parents(s, slot)
        a2a_copy(s, sector).start()
    p_all[z, core, pl.ds(pl.multiple_of(sector * 32, 32), 32), :] = parents(sector, 3)

    @pl.when(jnp.logical_not(own))
    def _():
        swap_copy.wait()
        t_spread.start_own()


    for copy in loads[3:]:
        copy.wait()
    scaled = jnp.transpose(jnp.concatenate([lists_mid[0], lists_mid[1]], axis=0) * 8)
    scaled_mid[0] = scaled[:, :entries]
    scaled_mid[1] = scaled[:, entries:]
    scaled = jnp.transpose(jnp.concatenate([lists_top[0] * 16, lists_top[1] * 8], axis=0))
    scaled_top[0] = scaled[:, :entries]
    scaled_top[1] = scaled[:, entries:]
    to_smem = [
        pltpu.make_async_copy(scaled_mid.at[0], list_s, index_sem.at[0]),
        pltpu.make_async_copy(scaled_mid.at[1], offset_s, index_sem.at[1]),
        pltpu.make_async_copy(scaled_top.at[0], list_ts, index_sem.at[2]),
        pltpu.make_async_copy(scaled_top.at[1], offset_ts, index_sem.at[3]),
    ]
    for copy in to_smem:
        copy.start()

    @pl.when(own)
    def _():
        for index in range(3):
            local_copy(index).wait()

    @pl.when(jnp.logical_not(own))
    def _():
        for index in range(3):
            share_copy(index).wait_recv()

    offsets = trans_mid.shape[0] // 4

    def put_offsets(first, row):
        for quarter, places in enumerate(((0, 2), (4, 6), (1, 3), (5, 7))):
            v = trans_mid[pl.ds(first + quarter, 8, stride=4), :]
            for at in places:
                t_tab[pl.ds(row + at, 8, stride=8), :] = v

    def mid_offsets(k, carry):
        put_offsets(pl.multiple_of(k * 32, 32), pl.multiple_of(k * 64, 64))
        return carry

    lax.fori_loop(0, offsets // 8, mid_offsets, 0)
    if offsets % 8:
        put_offsets((offsets - 8) * 4, (offsets - 8) * 8)

    sines_t, cosines_t = sin_cos(shift_top[...])
    cos_top[...] = cosines_t
    sin_top[...] = sines_t

    def wait_sector(k, carry):
        s = nth(k)
        a2a_copy(s, s).wait_recv()
        return carry

    lax.fori_loop(0, SECTORS - 1, wait_sector, 0)
    p_spread.start_own()

    block_f32[...] = p_all[z, core].astype(F32)
    for child in range(8):
        for part in range(2):
            for side in range(2):
                first = child * 4 + part * 2 + side
                a = block_f32[pl.ds(first, 8, stride=32), :]
                b = block_f32[pl.ds(256 + first, 8, stride=32), :]
                top_lhs[
                    part * 128 + child * 16 : part * 128 + child * 16 + 16, side * LANES : side * LANES + LANES
                ] = jnp.concatenate([a, b], axis=0).astype(BF16)

    def top_columns(k, carry):
        columns = pl.ds(pl.multiple_of(k * 256, 256), 256)
        spread = jnp.dot(top_lhs[...], interp_top[:, columns], preferred_element_type=F32)
        for part in range(2):
            lanes = slice(part * LANES, part * LANES + LANES)
            group = k * 2 + part
            real_sum = jnp.zeros((16, LANES), F32)
            imag_sum = jnp.zeros((16, LANES), F32)
            for child in range(8):
                real = spread[child * 16 : child * 16 + 16, lanes]
                imag = spread[128 + child * 16 : 128 + child * 16 + 16, lanes]
                c = cos_top[pl.ds(child * 8 + group, 1), :]
                n = sin_top[pl.ds(child * 8 + group, 1), :]
                real_sum += real * c - imag * n
                imag_sum += real * n + imag * c
            for half in range(2):
                boxes = slice(half * 8, half * 8 + 8)
                top_f32[pl.ds(half * 128 + group, 8, stride=16), :] = real_sum[boxes]
                top_f32[pl.ds(half * 128 + 8 + group, 8, stride=16), :] = imag_sum[boxes]
        return carry

    lax.fori_loop(0, 4, top_columns, 0)
    tp_all[z, core] = top_f32[...].astype(BF16)
    tp_spread.start_own()

    upper = lax.broadcasted_iota(jnp.int32, (8, LANES), 0) < 4

    def mid_table(plane, side):
        def four(k, carry):
            for part in range(4):
                odd = part % 2
                found = p_all[plane, side, pl.ds(pl.multiple_of(k * 128 + part * 32, 32), 32), :].astype(F32)
                first = ((2 * plane + odd) * 128 + (k * 4 + part - odd + side) * 8) * 8
                for pair in range(4):
                    v = found[pair * 8 : pair * 8 + 8]
                    r = pltpu.roll(v, 4, 0)
                    at = first + pair * 16
                    p_tab[pl.ds(pl.multiple_of(at, 8), 8), :] = jnp.where(upper, v, r)
                    p_tab[pl.ds(pl.multiple_of(at + 8, 8), 8), :] = jnp.where(upper, r, v)
            return carry

        lax.fori_loop(0, SECTORS // 4, four, 0)

    def top_table(plane, side):
        def four(k, carry):
            for part in range(4):
                odd = part % 2
                found = tp_all[plane, side, pl.ds(pl.multiple_of(k * 64 + part * 16, 16), 16), :].astype(F32)
                first = ((2 * plane + odd) * 16 + (k * 4 + part - odd + side)) * 16
                p_top[pl.ds(pl.multiple_of(first, 16), 16), :] = found
            return carry

        lax.fori_loop(0, SECTORS // 4, four, 0)

    def offset_table(plane, side):
        at = plane * 2 + side

        def four(k, carry):
            for part in range(4):
                found = t_all[plane, side, pl.ds(pl.multiple_of(k * 64 + part * 16, 16), 16), :].astype(F32)
                for half in range(2):
                    t_top[pl.ds(k * 512 + part * 128 + half * 64 + at, 8, stride=8), :] = found[
                        half * 8 : half * 8 + 8
                    ]
            return carry

        lax.fori_loop(0, t_all.shape[2] // 64, four, 0)

    mid_table(z, core)
    top_table(z, core)
    offset_table(z, core)
    t_spread.forward()
    offset_table(t_spread.left, core)
    offset_table(t_spread.right, core)
    p_spread.forward()
    tp_spread.forward()
    mid_table(p_spread.left, core)
    mid_table(p_spread.right, core)
    t_spread.forward_far()
    offset_table(t_spread.far, core)
    offset_table(t_spread.take(0), 1 - core)
    mid_table(p_spread.take(0), 1 - core)
    top_table(tp_spread.left, core)
    top_table(tp_spread.right, core)
    p_spread.forward_far()
    tp_spread.forward_far()
    mid_table(p_spread.far, core)
    top_table(tp_spread.far, core)
    mid_table(p_spread.take(1), 1 - core)
    mid_table(p_spread.take(2), 1 - core)
    for which in range(1, 4):
        offset_table(t_spread.take(which), 1 - core)
    for which in range(4):
        top_table(tp_spread.take(which), 1 - core)
    mid_table(p_spread.take(3), 1 - core)
    for copy in to_smem:
        copy.wait()


    behind = (trans_top_ref.shape[0] // 2) * 8

    def top_box(k, carry):
        odd = k % 2
        column = (2 * z + odd) * 16 + (k - odd + core)
        sums = [jnp.zeros((8, LANES), F32) for _ in range(4)]
        for j in range(entries):
            n = list_ts[column, j]
            o = offset_ts[column, j]
            pr = p_top[pl.ds(n, 8), :]
            pi = p_top[pl.ds(n + 8, 8), :]
            tr = t_top[pl.ds(o, 8), :]
            ti = t_top[pl.ds(o + behind, 8), :]
            sums = [sums[0] + pr * tr, sums[1] + pi * ti, sums[2] + pr * ti, sums[3] + pi * tr]
        real = (sums[0] - sums[1]).astype(BF16).astype(F32)
        imag = (sums[2] + sums[3]).astype(BF16).astype(F32)
        top_sum[pl.ds(pl.multiple_of(k * 16, 16), 8), :] = real
        top_sum[pl.ds(pl.multiple_of(k * 16 + 8, 8), 8), :] = imag
        return carry

    lax.fori_loop(0, SECTORS, top_box, 0)

    def top_children(part, carry):
        lanes = pl.ds(pl.multiple_of(part * LANES, LANES), LANES)
        c = cos_top[pl.ds(part, 8, stride=8), :]
        n = sin_top[pl.ds(part, 8, stride=8), :]
        for pair in range(8):
            reals = []
            imags = []
            for half in range(2):
                first = pair * 32 + half * 16
                real = jnp.broadcast_to(top_sum[pl.ds(first + part, 1), :], (8, LANES))
                imag = jnp.broadcast_to(top_sum[pl.ds(first + 8 + part, 1), :], (8, LANES))
                reals.append(real * c + imag * n)
                imags.append(imag * c - real * n)
            child_rows[pair * 16 : pair * 16 + 16, lanes] = jnp.concatenate(reals, axis=0).astype(BF16)
            child_rows[128 + pair * 16 : 144 + pair * 16, lanes] = jnp.concatenate(imags, axis=0).astype(BF16)
        return carry

    lax.fori_loop(0, 8, top_children, 0)
    scale = interp_top.shape[0] / interp_top.shape[1]
    down[...] = scale * lax.dot_general(
        child_rows[...], interp_top[...], (((1,), (1,)), ((), ())), preferred_element_type=F32
    )

    def back_copy(s, landing):
        return pltpu.make_async_remote_copy(
            src_ref=pieces.at[s],
            dst_ref=received.at[landing],
            send_sem=back_send.at[s],
            recv_sem=back_recv.at[landing],
            device_id=to_sector(s),
            device_id_type=MESH,
        )

    def combine(k):
        odd = k % 2
        first = odd * 128 + (k - odd + core) * 8

        def mid_box(i, carry):
            kept = jnp.zeros((8, LANES), F32)
            for j in range(entries):
                p = p_tab[pl.ds(list_s[first + i, j], 8), :]
                t = t_tab[pl.ds(offset_s[first + i, j], 8), :]
                kept = kept + p * t
            mid_sum[pl.ds(pl.multiple_of(i * 8, 8), 8), :] = kept
            return carry

        lax.fori_loop(0, 8, mid_box, 0)
        at = pl.multiple_of(k * 8, 8)
        sides = []
        for side in range(2):
            lanes = slice(side * LANES, side * LANES + LANES)
            parts = [mid_sum[pl.ds(side + 2 * quarter, 8, stride=8), :] for quarter in range(4)]
            real = (parts[0] - parts[3]) + down[pl.ds(at, 8), lanes]
            imag = (parts[1] + parts[2]) + down[pl.ds(pl.multiple_of(128 + k * 8, 8), 8), lanes]
            sides.append(jnp.concatenate([real, imag], axis=0).astype(BF16))
        return jnp.concatenate(sides, axis=1)

    def finish_sector(s):
        columns = pl.ds(pl.multiple_of(s * 256, 256), 256)
        c = cos_mid[:, columns]
        n = sin_mid[:, columns]
        found = received[s].astype(F32)
        for pair in range(4):
            reals = []
            imags = []
            for half in range(2):
                box = pair * 2 + half
                real = jnp.broadcast_to(found[box : box + 1], (8, 256))
                imag = jnp.broadcast_to(found[8 + box : 9 + box], (8, 256))
                reals.append(real * c + imag * n)
                imags.append(imag * c - real * n)
            children[pair * 16 : pair * 16 + 16, :] = jnp.concatenate(reals, axis=0).astype(BF16)
            children[64 + pair * 16 : 80 + pair * 16, :] = jnp.concatenate(imags, axis=0).astype(BF16)
        total[...] += lax.dot_general(
            children[...], weights[:, columns], (((1,), (1,)), ((), ())), preferred_element_type=F32
        )

    total[...] = jnp.zeros_like(total)
    late = 3

    def send_back(k, carry):
        s = nth(k)
        pieces[s] = combine(s)
        back_copy(s, sector).start()
        return carry

    def take_back(k, carry):
        s = from_nth(k)
        back_copy(s, s).wait_recv()
        finish_sector(s)
        return carry

    def send_and_take(k, carry):
        send_back(k, carry)
        return take_back(k - late, carry)

    lax.fori_loop(0, late, send_back, 0)
    lax.fori_loop(late, SECTORS - 1, send_and_take, 0)
    received[sector] = combine(sector)
    finish_sector(sector)
    lax.fori_loop(SECTORS - 1 - late, SECTORS - 1, take_back, 0)
    half_rows = total.shape[0] // 2
    for part in range(2):
        out_ref[part] = total[part * half_rows : part * half_rows + half_rows, :]

    def wait_sent(k, carry):
        s = nth(k)
        a2a_copy(s, sector).wait_send()
        back_copy(s, sector).wait_send()
        return carry

    lax.fori_loop(0, SECTORS - 1, wait_sent, 0)

    @pl.when(own)
    def _():
        for index in range(3):
            share_copy(index).wait_send()

    for each in (t_spread, p_spread, tp_spread):
        each.sent()


def on_device(
    leaf_out,
    interp_mid,
    shift_mid,
    trans_mid,
    list_mid,
    offset_mid,
    interp_top,
    shift_top,
    trans_top,
    list_top,
    offset_top,
):
    offsets = trans_mid.shape[1]
    entries = list_mid.shape[1]
    rows = 2 * leaf_out.shape[1]
    operands = (
        leaf_out,
        interp_mid,
        shift_mid,
        trans_top.reshape(2 * offsets, LANES),
        jnp.transpose(trans_mid.reshape(2, offsets, 2, LANES), (1, 2, 0, 3)).reshape(4 * offsets, LANES),
        interp_top[0],
        shift_top.reshape(64, LANES),
        list_mid.T,
        offset_mid.T,
        list_top.T,
        offset_top.T,
    )
    padded = 640
    result = pl.pallas_call(
        kernel,
        out_shape=jax.ShapeDtypeStruct(leaf_out.shape, F32),
        in_specs=[pl.BlockSpec(memory_space=pltpu.HBM)] * len(operands),
        out_specs=pl.BlockSpec(memory_space=VMEM),
        scratch_shapes=[
            VMEM(leaf_out.shape, BF16),
            VMEM(interp_mid.shape, BF16),
            VMEM(shift_mid.shape, F32),
            VMEM((2 * offsets, LANES), F32),
            VMEM((4 * offsets, LANES), F32),
            VMEM((256, 1024), BF16),
            VMEM((64, LANES), F32),
            VMEM((2, entries, 256), jnp.int32),
            VMEM((2, entries, 128), jnp.int32),
            VMEM((2, 256, entries), jnp.int32),
            VMEM((2, 128, entries), jnp.int32),
            pltpu.SMEM((256, entries), jnp.int32),
            pltpu.SMEM((256, entries), jnp.int32),
            pltpu.SMEM((128, entries), jnp.int32),
            pltpu.SMEM((128, entries), jnp.int32),
            VMEM((PLANES, 2, 512, LANES), BF16),
            VMEM((PLANES, 2, 256, LANES), BF16),
            VMEM((PLANES, 2, padded, LANES), BF16),
            VMEM((rows, interp_mid.shape[0]), BF16),
            VMEM(shift_mid.shape, F32),
            VMEM(shift_mid.shape, F32),
            VMEM((SECTORS, 32, LANES), BF16),
            VMEM((128, LANES), F32),
            VMEM((padded, LANES), BF16),
            VMEM((512, LANES), F32),
            VMEM((256, 256), BF16),
            VMEM((256, LANES), F32),
            VMEM((64, LANES), F32),
            VMEM((64, LANES), F32),
            VMEM((1024 * 8, LANES), F32),
            VMEM((offsets * 8, LANES), F32),
            VMEM((128 * 16, LANES), F32),
            VMEM((padded * 8, LANES), F32),
            VMEM((8 * 8, LANES), F32),
            VMEM((16 * 16, LANES), F32),
            VMEM((256, 1024), BF16),
            VMEM((256, 256), F32),
            VMEM((SECTORS, 16, 256), BF16),
            VMEM((SECTORS, 16, 256), BF16),
            VMEM((rows, 256), BF16),
            VMEM((rows, interp_mid.shape[0]), F32),
            DMA((4,)),
            DMA((7,)),
            DMA((4,)),
            DMA((SECTORS,)),
            DMA((SECTORS,)),
            DMA((2,)),
            DMA((3,)),
            DMA((3,)),
            DMA((8,)),
            DMA((8,)),
            DMA((8,)),
            DMA((8,)),
            DMA((8,)),
            DMA((8,)),
            DMA((SECTORS,)),
            DMA((SECTORS,)),
        ],
        compiler_params=pltpu.CompilerParams(
            collective_id=0, has_side_effects=True, vmem_limit_bytes=60 * 1024 * 1024
        ),
        name="far_field",
    )(*operands)
    return result * (interp_mid.shape[0] / interp_mid.shape[1])


def solution(mesh):
    return jax.shard_map(
        on_device,
        mesh=mesh,
        in_specs=(
            P(None, ("box", "dir"), None),
            P(),
            P(),
            P(None, None, "dir"),
            P(),
            P(),
            P("dir", None, None),
            P(None, "dir", None),
            P(None, None, "dir", "box"),
            P(),
            P(),
        ),
        out_specs=P(None, ("box", "dir"), None),
        check_vma=False,
    )
```

```python
import jax
import jax.numpy as jnp
from jax import lax
from jax.experimental import pallas as pl
from jax.experimental.pallas import tpu as pltpu
from jax.sharding import PartitionSpec as P

MESH = pl.DeviceIdType.MESH
F32 = jnp.float32
BF16 = jnp.bfloat16
VMEM = pltpu.VMEM
DMA = pltpu.SemaphoreType.DMA
PLANES = 4
SECTORS = 16
LANES = 128


def place():
    box = lax.axis_index("box")
    way = lax.axis_index("dir")
    low = box % 2
    core = way % 2
    return box // 2, way - core + low, core


def device_of(plane, sector, core):
    low = sector % 2
    return (plane * 2 + low, sector - low + core)


def sin_cos(angle):
    half = angle * 0.5
    sq = half * half
    s = sq * (-1.0 / 39916800.0) + (1.0 / 362880.0)
    s = sq * s - (1.0 / 5040.0)
    s = sq * s + (1.0 / 120.0)
    s = sq * s - (1.0 / 6.0)
    s = half + half * (sq * s)
    c = sq * (1.0 / 479001600.0) - (1.0 / 3628800.0)
    c = sq * c + (1.0 / 40320.0)
    c = sq * c - (1.0 / 720.0)
    c = sq * c + (1.0 / 24.0)
    c = sq * c - 0.5
    c = sq * c + 1.0
    return 2.0 * s * c, 1.0 - 2.0 * s * s


class Spread:
    def __init__(self, ref, send, recv):
        z, sector, core = place()
        self.ref, self.send, self.recv = ref, send, recv
        self.core = core
        self.z = z
        self.left = (z + PLANES - 1) % PLANES
        self.right = (z + 1) % PLANES
        self.far = (z + 2) % PLANES
        self.to_right = device_of(self.right, sector, core)
        self.to_left = device_of(self.left, sector, core)
        self.partner = device_of(z, sector, 1 - core)
        self.rows = ref.shape[2]
        self.crossing = ((4, self.z), (5, self.left), (6, self.right), (7, self.far))

    def copy(self, plane, core, half, index, target):
        rows = self.rows
        if half is None:
            part = self.ref.at[plane, core]
        else:
            part = self.ref.at[plane, core, pl.ds(half * (rows // 2), rows // 2)]
        return pltpu.make_async_remote_copy(
            src_ref=part,
            dst_ref=part,
            send_sem=self.send.at[index],
            recv_sem=self.recv.at[index],
            device_id=target,
            device_id_type=MESH,
        )

    def start_own(self):
        self.copy(self.z, self.core, 0, 0, self.to_right).start()
        self.copy(self.z, self.core, 1, 1, self.to_left).start()
        self.copy(self.z, self.core, 1, 8, self.to_right).start()
        self.copy(self.z, self.core, 0, 9, self.to_left).start()
        self.copy(self.z, self.core, None, 4, self.partner).start()

    def forward(self):
        self.copy(self.left, self.core, 0, 0, self.to_right).wait_recv()
        self.copy(self.left, self.core, 0, 2, self.to_right).start()
        self.copy(self.right, self.core, 1, 1, self.to_left).wait_recv()
        self.copy(self.right, self.core, 1, 3, self.to_left).start()

    def forward_rest(self):
        self.copy(self.left, self.core, 1, 8, self.to_right).wait_recv()
        self.copy(self.left, self.core, None, 5, self.partner).start()
        self.copy(self.right, self.core, 0, 9, self.to_left).wait_recv()
        self.copy(self.right, self.core, None, 6, self.partner).start()

    def forward_far(self):
        self.copy(self.far, self.core, 0, 2, self.to_right).wait_recv()
        self.copy(self.far, self.core, 1, 3, self.to_left).wait_recv()
        self.copy(self.far, self.core, None, 7, self.partner).start()

    def take(self, which):
        index, plane = self.crossing[which]
        self.copy(plane, 1 - self.core, None, index, self.partner).wait_recv()
        return plane

    def sent(self):
        self.copy(self.z, self.core, 0, 0, self.to_right).wait_send()
        self.copy(self.z, self.core, 1, 1, self.to_left).wait_send()
        self.copy(self.z, self.core, 1, 8, self.to_right).wait_send()
        self.copy(self.z, self.core, 0, 9, self.to_left).wait_send()
        self.copy(self.left, self.core, 0, 2, self.to_right).wait_send()
        self.copy(self.right, self.core, 1, 3, self.to_left).wait_send()
        for index, plane in self.crossing:
            self.copy(plane, self.core, None, index, self.partner).wait_send()


def kernel(
    leaf_ref,
    matrix_ref,
    shift_mid_ref,
    trans_top_ref,
    trans_mid_ref,
    interp_top_ref,
    shift_top_ref,
    list_mid_ref,
    offset_mid_ref,
    list_top_ref,
    offset_top_ref,
    out_ref,
    leaf,
    weights,
    shift_mid,
    trans_top,
    trans_mid,
    interp_top,
    shift_top,
    lists_mid,
    lists_top,
    scaled_mid,
    scaled_top,
    list_s,
    offset_s,
    list_ts,
    offset_ts,
    p_all,
    tp_all,
    t_all,
    leaf_rows,
    cos_mid,
    sin_mid,
    sending,
    stage,
    piece,
    block_f32,
    top_lhs,
    top_f32,
    cos_top,
    sin_top,
    p_tab,
    t_tab,
    p_top,
    t_top,
    mid_sum,
    top_sum,
    child_rows,
    down,
    pieces,
    received,
    children,
    total,
    weight_sem,
    load_sem,
    index_sem,
    a2a_send,
    a2a_recv,
    swap_sem,
    share_send,
    share_recv,
    t_send,
    t_recv,
    p_send,
    p_recv,
    tp_send,
    tp_recv,
    back_send,
    back_recv,
):
    z, sector, core = place()
    entries = list_mid_ref.shape[0]
    low = sector % 2
    own = low == core
    partner = device_of(z, sector, 1 - core)
    swap = device_of(z, sector - low + core, low)
    right = device_of((z + 1) % PLANES, sector, core)
    left = device_of((z + PLANES - 1) % PLANES, sector, core)
    t_spread = Spread(t_all, t_send, t_recv)
    p_spread = Spread(p_all, p_send, p_recv)
    tp_spread = Spread(tp_all, tp_send, tp_recv)

    group = sector // 4
    inside = sector % 4

    def apart(a, k):
        high = (a // 2 + k + 1) % 2
        return high * 2 + (a % 2 + 1 + k // 2) % 2

    def nth(k):
        return apart(group, k // 4) * 4 + apart(inside, k % 4)

    def other(k):
        return (sector + 1 + k) % SECTORS

    def to_sector(s):
        return device_of(z, s, core)

    barrier = pltpu.get_barrier_semaphore()

    def signal_peer(k, carry):
        pl.semaphore_signal(barrier, inc=1, device_id=to_sector(other(k)), device_id_type=MESH)
        return carry

    lax.fori_loop(0, SECTORS - 1, signal_peer, 0)
    for device in (right, left, partner):
        pl.semaphore_signal(barrier, inc=1, device_id=device, device_id_type=MESH)

    @pl.when(jnp.logical_not(own))
    def _():
        pl.semaphore_signal(barrier, inc=1, device_id=swap, device_id_type=MESH)

    slab = pl.ds(pl.multiple_of(z * 256, 256), 256)
    loads = [
        pltpu.make_async_copy(source, target, load_sem.at[index])
        for index, (source, target) in enumerate(
            (
                (leaf_ref, leaf),
                (trans_top_ref, trans_top),
                (shift_mid_ref, shift_mid),
                (list_mid_ref.at[:, slab], lists_mid.at[0]),
                (offset_mid_ref.at[:, slab], lists_mid.at[1]),
                (list_top_ref, lists_top.at[0]),
                (offset_top_ref, lists_top.at[1]),
            )
        )
    ]
    for copy in loads[:3]:
        copy.start()

    def weight_copy(piece_at):
        columns = pl.ds(pl.multiple_of(apart(group, piece_at) * 1024, 1024), 1024)
        return pltpu.make_async_copy(matrix_ref.at[:, columns], weights.at[:, columns], weight_sem.at[piece_at])

    for piece_at in range(4):
        weight_copy(piece_at).start()
    for copy in loads[3:]:
        copy.start()

    loads[0].wait()
    rows = 2 * leaf.shape[1]
    target = lax.broadcasted_iota(jnp.int32, (rows, rows), 0)
    source = lax.broadcasted_iota(jnp.int32, (rows, rows), 1)
    wanted = (target & 64) + ((target & 7) << 3) + ((target >> 3) & 7)
    order = (source == wanted).astype(BF16)
    both = jnp.concatenate([leaf[0], leaf[1]], axis=0)
    leaf_rows[...] = jnp.dot(order, both, preferred_element_type=F32).astype(BF16)

    loads[1].wait()
    used = trans_top.shape[0]
    piece[0:used, :] = trans_top[...].astype(BF16)
    piece[used:, :] = jnp.zeros((piece.shape[0] - used, LANES), BF16)

    swap_copy = pltpu.make_async_remote_copy(
        src_ref=piece,
        dst_ref=t_all.at[z, low],
        send_sem=swap_sem.at[0],
        recv_sem=swap_sem.at[1],
        device_id=swap,
        device_id_type=MESH,
    )
    shared = ((trans_mid_ref, trans_mid), (interp_top_ref, interp_top), (shift_top_ref, shift_top))

    def share_copy(index):
        return pltpu.make_async_remote_copy(
            src_ref=shared[index][0],
            dst_ref=shared[index][1],
            send_sem=share_send.at[index],
            recv_sem=share_recv.at[index],
            device_id=partner,
            device_id_type=MESH,
        )

    def local_copy(index):
        return pltpu.make_async_copy(shared[index][0], shared[index][1], share_recv.at[index])

    loads[2].wait()
    sines, cosines = sin_cos(shift_mid[...])
    cos_mid[...] = cosines
    sin_mid[...] = sines

    def parents(s, slot):
        columns = pl.ds(pl.multiple_of(s * 256, 256), 256)
        spread = jnp.dot(leaf_rows[...], weights[:, columns], preferred_element_type=F32)
        real_sum = jnp.zeros((8, 256), F32)
        imag_sum = jnp.zeros((8, 256), F32)
        for child in range(8):
            real = spread[child * 8 : child * 8 + 8]
            imag = spread[64 + child * 8 : 64 + child * 8 + 8]
            c = cos_mid[child : child + 1, columns]
            n = sin_mid[child : child + 1, columns]
            real_sum += real * c - imag * n
            imag_sum += real * n + imag * c
        for part in range(2):
            lanes = slice(part * LANES, part * LANES + LANES)
            stage[pl.ds(slot * 32 + part, 8, stride=4), :] = real_sum[:, lanes]
            stage[pl.ds(slot * 32 + 2 + part, 8, stride=4), :] = imag_sum[:, lanes]
        return stage[slot * 32 : slot * 32 + 32, :].astype(BF16)

    def rows_of(s):
        return p_all.at[z, core, pl.ds(pl.multiple_of(s * 32, 32), 32)]

    def a2a_copy(s, landing):
        return pltpu.make_async_remote_copy(
            src_ref=sending.at[s],
            dst_ref=rows_of(landing),
            send_sem=a2a_send.at[s],
            recv_sem=a2a_recv.at[landing],
            device_id=to_sector(s),
            device_id_type=MESH,
        )

    def make_four(piece_at):
        weight_copy(piece_at).wait()
        for slot in range(4):
            s = nth(piece_at * 4 + slot)
            sending[s] = parents(s, slot)

    def start_four(piece_at):
        for slot in range(4):
            a2a_copy(nth(piece_at * 4 + slot), sector).start()

    make_four(0)
    pl.semaphore_wait(barrier, SECTORS - 1 + 3 + (low + core) % 2)

    @pl.when(own)
    def _():
        for index in range(3):
            share_copy(index).start()
            local_copy(index).start()
        t_all[z, core] = piece[...]
        t_spread.start_own()

    @pl.when(jnp.logical_not(own))
    def _():
        swap_copy.start()

    start_four(0)

    def send_four(piece_at, carry):
        make_four(piece_at)
        start_four(piece_at)
        return carry

    lax.fori_loop(1, 3, send_four, 0)
    weight_copy(3).wait()
    for slot in range(3):
        s = nth(12 + slot)
        sending[s] = parents(s, slot)
        a2a_copy(s, sector).start()
    p_all[z, core, pl.ds(pl.multiple_of(sector * 32, 32), 32), :] = parents(sector, 3)


    for copy in loads[3:]:
        copy.wait()
    scaled = jnp.transpose(jnp.concatenate([lists_mid[0], lists_mid[1]], axis=0) * 8)
    scaled_mid[0] = scaled[:, :entries]
    scaled_mid[1] = scaled[:, entries:]
    scaled = jnp.transpose(jnp.concatenate([lists_top[0] * 16, lists_top[1] * 8], axis=0))
    scaled_top[0] = scaled[:, :entries]
    scaled_top[1] = scaled[:, entries:]
    to_smem = [
        pltpu.make_async_copy(scaled_mid.at[0], list_s, index_sem.at[0]),
        pltpu.make_async_copy(scaled_mid.at[1], offset_s, index_sem.at[1]),
        pltpu.make_async_copy(scaled_top.at[0], list_ts, index_sem.at[2]),
        pltpu.make_async_copy(scaled_top.at[1], offset_ts, index_sem.at[3]),
    ]
    for copy in to_smem:
        copy.start()

    @pl.when(own)
    def _():
        for index in range(3):
            local_copy(index).wait()

    @pl.when(jnp.logical_not(own))
    def _():
        for index in range(3):
            share_copy(index).wait_recv()

    offsets = trans_mid.shape[0] // 4

    def put_offsets(first, row):
        for quarter, places in enumerate(((0, 2), (4, 6), (1, 3), (5, 7))):
            v = trans_mid[pl.ds(first + quarter, 8, stride=4), :]
            for at in places:
                t_tab[pl.ds(row + at, 8, stride=8), :] = v

    def mid_offsets(k, carry):
        put_offsets(pl.multiple_of(k * 32, 32), pl.multiple_of(k * 64, 64))
        return carry

    lax.fori_loop(0, offsets // 8, mid_offsets, 0)
    if offsets % 8:
        put_offsets((offsets - 8) * 4, (offsets - 8) * 8)

    sines_t, cosines_t = sin_cos(shift_top[...])
    cos_top[...] = cosines_t
    sin_top[...] = sines_t

    def wait_sector(k, carry):
        s = other(k)
        a2a_copy(s, s).wait_recv()
        return carry

    lax.fori_loop(0, SECTORS - 1, wait_sector, 0)
    p_spread.start_own()

    block_f32[...] = p_all[z, core].astype(F32)
    for child in range(8):
        for part in range(2):
            for side in range(2):
                first = child * 4 + part * 2 + side
                a = block_f32[pl.ds(first, 8, stride=32), :]
                b = block_f32[pl.ds(256 + first, 8, stride=32), :]
                top_lhs[
                    part * 128 + child * 16 : part * 128 + child * 16 + 16, side * LANES : side * LANES + LANES
                ] = jnp.concatenate([a, b], axis=0).astype(BF16)

    def top_columns(k, carry):
        columns = pl.ds(pl.multiple_of(k * 256, 256), 256)
        spread = jnp.dot(top_lhs[...], interp_top[:, columns], preferred_element_type=F32)
        for part in range(2):
            lanes = slice(part * LANES, part * LANES + LANES)
            group = k * 2 + part
            real_sum = jnp.zeros((16, LANES), F32)
            imag_sum = jnp.zeros((16, LANES), F32)
            for child in range(8):
                real = spread[child * 16 : child * 16 + 16, lanes]
                imag = spread[128 + child * 16 : 128 + child * 16 + 16, lanes]
                c = cos_top[pl.ds(child * 8 + group, 1), :]
                n = sin_top[pl.ds(child * 8 + group, 1), :]
                real_sum += real * c - imag * n
                imag_sum += real * n + imag * c
            for half in range(2):
                boxes = slice(half * 8, half * 8 + 8)
                top_f32[pl.ds(half * 128 + group, 8, stride=16), :] = real_sum[boxes]
                top_f32[pl.ds(half * 128 + 8 + group, 8, stride=16), :] = imag_sum[boxes]
        return carry

    lax.fori_loop(0, 4, top_columns, 0)
    tp_all[z, core] = top_f32[...].astype(BF16)

    upper = lax.broadcasted_iota(jnp.int32, (8, LANES), 0) < 4

    def mid_table(plane, side):
        def four(k, carry):
            for part in range(4):
                odd = part % 2
                found = p_all[plane, side, pl.ds(pl.multiple_of(k * 128 + part * 32, 32), 32), :].astype(F32)
                first = ((2 * plane + odd) * 128 + (k * 4 + part - odd + side) * 8) * 8
                for pair in range(4):
                    v = found[pair * 8 : pair * 8 + 8]
                    r = pltpu.roll(v, 4, 0)
                    at = first + pair * 16
                    p_tab[pl.ds(pl.multiple_of(at, 8), 8), :] = jnp.where(upper, v, r)
                    p_tab[pl.ds(pl.multiple_of(at + 8, 8), 8), :] = jnp.where(upper, r, v)
            return carry

        lax.fori_loop(0, SECTORS // 4, four, 0)

    def top_table(plane, side):
        def four(k, carry):
            for part in range(4):
                odd = part % 2
                found = tp_all[plane, side, pl.ds(pl.multiple_of(k * 64 + part * 16, 16), 16), :].astype(F32)
                first = ((2 * plane + odd) * 16 + (k * 4 + part - odd + side)) * 16
                p_top[pl.ds(pl.multiple_of(first, 16), 16), :] = found
            return carry

        lax.fori_loop(0, SECTORS // 4, four, 0)

    def offset_table(plane, side):
        at = plane * 2 + side

        def four(k, carry):
            for part in range(4):
                found = t_all[plane, side, pl.ds(pl.multiple_of(k * 64 + part * 16, 16), 16), :].astype(F32)
                for half in range(2):
                    t_top[pl.ds(k * 512 + part * 128 + half * 64 + at, 8, stride=8), :] = found[
                        half * 8 : half * 8 + 8
                    ]
            return carry

        lax.fori_loop(0, t_all.shape[2] // 64, four, 0)

    mid_table(z, core)
    top_table(z, core)
    p_spread.forward()
    tp_spread.start_own()
    p_spread.forward_rest()

    @pl.when(jnp.logical_not(own))
    def _():
        swap_copy.wait()
        t_spread.start_own()

    mid_table(p_spread.left, core)
    mid_table(p_spread.right, core)
    mid_table(p_spread.take(0), 1 - core)
    for copy in to_smem:
        copy.wait()
    p_spread.forward_far()
    mid_table(p_spread.far, core)
    mid_table(p_spread.take(1), 1 - core)
    mid_table(p_spread.take(2), 1 - core)
    mid_table(p_spread.take(3), 1 - core)

    def middle(k):
        s = nth(k)
        odd = s % 2
        first = odd * 128 + (s - odd + core) * 8

        def mid_box(i, carry):
            kept = jnp.zeros((8, LANES), F32)
            for j in range(entries):
                p = p_tab[pl.ds(list_s[first + i, j], 8), :]
                t = t_tab[pl.ds(offset_s[first + i, j], 8), :]
                kept = kept + p * t
            mid_sum[pl.ds(pl.multiple_of(k * 64 + i * 8, 8), 8), :] = kept
            return carry

        lax.fori_loop(0, 8, mid_box, 0)

    def middle_early(k, carry):
        middle(k)
        return carry

    ahead = 8
    lax.fori_loop(0, 4, middle_early, 0)
    tp_spread.forward()
    t_spread.forward()
    tp_spread.forward_rest()
    t_spread.forward_rest()
    lax.fori_loop(4, ahead, middle_early, 0)
    tp_spread.forward_far()
    t_spread.forward_far()
    for plane in (z, t_spread.left, t_spread.right, t_spread.far):
        offset_table(plane, core)
    for plane in (tp_spread.left, tp_spread.right, tp_spread.far):
        top_table(plane, core)
    for which in range(4):
        offset_table(t_spread.take(which), 1 - core)
        top_table(tp_spread.take(which), 1 - core)

    behind = (trans_top_ref.shape[0] // 2) * 8

    def top_box(k, carry):
        odd = k % 2
        column = (2 * z + odd) * 16 + (k - odd + core)
        sums = [jnp.zeros((8, LANES), F32) for _ in range(4)]
        for j in range(entries):
            n = list_ts[column, j]
            o = offset_ts[column, j]
            pr = p_top[pl.ds(n, 8), :]
            pi = p_top[pl.ds(n + 8, 8), :]
            tr = t_top[pl.ds(o, 8), :]
            ti = t_top[pl.ds(o + behind, 8), :]
            sums = [sums[0] + pr * tr, sums[1] + pi * ti, sums[2] + pr * ti, sums[3] + pi * tr]
        real = (sums[0] - sums[1]).astype(BF16).astype(F32)
        imag = (sums[2] + sums[3]).astype(BF16).astype(F32)
        top_sum[pl.ds(pl.multiple_of(k * 16, 16), 8), :] = real
        top_sum[pl.ds(pl.multiple_of(k * 16 + 8, 8), 8), :] = imag
        return carry

    lax.fori_loop(0, SECTORS, top_box, 0)

    def top_children(part, carry):
        lanes = pl.ds(pl.multiple_of(part * LANES, LANES), LANES)
        c = cos_top[pl.ds(part, 8, stride=8), :]
        n = sin_top[pl.ds(part, 8, stride=8), :]
        for pair in range(8):
            reals = []
            imags = []
            for half in range(2):
                first = pair * 32 + half * 16
                real = jnp.broadcast_to(top_sum[pl.ds(first + part, 1), :], (8, LANES))
                imag = jnp.broadcast_to(top_sum[pl.ds(first + 8 + part, 1), :], (8, LANES))
                reals.append(real * c + imag * n)
                imags.append(imag * c - real * n)
            child_rows[pair * 16 : pair * 16 + 16, lanes] = jnp.concatenate(reals, axis=0).astype(BF16)
            child_rows[128 + pair * 16 : 144 + pair * 16, lanes] = jnp.concatenate(imags, axis=0).astype(BF16)
        return carry

    lax.fori_loop(0, 8, top_children, 0)
    scale = interp_top.shape[0] / interp_top.shape[1]
    down[...] = scale * lax.dot_general(
        child_rows[...], interp_top[...], (((1,), (1,)), ((), ())), preferred_element_type=F32
    )

    def back_copy(s, landing):
        return pltpu.make_async_remote_copy(
            src_ref=pieces.at[s],
            dst_ref=received.at[landing],
            send_sem=back_send.at[s],
            recv_sem=back_recv.at[landing],
            device_id=to_sector(s),
            device_id_type=MESH,
        )

    def combine(n):
        k = nth(n)
        at = pl.multiple_of(k * 8, 8)
        sides = []
        for side in range(2):
            lanes = slice(side * LANES, side * LANES + LANES)
            parts = [mid_sum[pl.ds(n * 64 + side + 2 * quarter, 8, stride=8), :] for quarter in range(4)]
            real = (parts[0] - parts[3]) + down[pl.ds(at, 8), lanes]
            imag = (parts[1] + parts[2]) + down[pl.ds(pl.multiple_of(128 + k * 8, 8), 8), lanes]
            sides.append(jnp.concatenate([real, imag], axis=0).astype(BF16))
        return jnp.concatenate(sides, axis=1)

    def make_children(s, at):
        columns = pl.ds(pl.multiple_of(s * 256, 256), 256)
        c = cos_mid[:, columns]
        n = sin_mid[:, columns]
        found = received[s].astype(F32)
        target = pl.ds(pl.multiple_of(at * 256, 256), 256)
        for pair in range(4):
            reals = []
            imags = []
            for half in range(2):
                box = pair * 2 + half
                real = jnp.broadcast_to(found[box : box + 1], (8, 256))
                imag = jnp.broadcast_to(found[8 + box : 9 + box], (8, 256))
                reals.append(real * c + imag * n)
                imags.append(imag * c - real * n)
            children[pair * 16 : pair * 16 + 16, target] = jnp.concatenate(reals, axis=0).astype(BF16)
            children[64 + pair * 16 : 80 + pair * 16, target] = jnp.concatenate(imags, axis=0).astype(BF16)

    def finish(piece_at, first, count):
        at = apart(group, piece_at)
        for slot in range(count):
            back_copy(at * 4 + apart(inside, slot), at * 4 + apart(inside, slot)).wait_recv()
        for slot in range(4):
            make_children(at * 4 + slot, slot)
        columns = pl.ds(pl.multiple_of(at * 1024, 1024), 1024)

        def quarter(k, carry):
            rows_at = pl.ds(pl.multiple_of(k * 256, 256), 256)
            part = lax.dot_general(
                weights[rows_at, columns], children[...], (((1,), (1,)), ((), ())), preferred_element_type=F32
            )
            if first:
                total[rows_at, :] = part
            else:
                total[rows_at, :] += part
            return carry

        lax.fori_loop(0, 4, quarter, 0)

    def send_back(k, carry):
        s = nth(k)
        pieces[s] = combine(k)
        back_copy(s, sector).start()
        return carry

    def middle_and_send(k, carry):
        middle(k)
        return send_back(k, carry)

    lax.fori_loop(0, ahead, send_back, 0)
    lax.fori_loop(ahead, SECTORS - 1, middle_and_send, 0)
    middle(SECTORS - 1)
    received[sector] = combine(SECTORS - 1)
    finish(0, True, 4)
    finish(1, False, 4)
    finish(2, False, 4)
    finish(3, False, 3)
    half_rows = out_ref.shape[1]
    for k in range(total.shape[0] // LANES):
        columns = slice(k * LANES, k * LANES + LANES)
        turned = jnp.transpose(total[columns, :])
        for part in range(2):
            out_ref[part, :, columns] = turned[part * half_rows : part * half_rows + half_rows]

    def wait_sent(k, carry):
        s = other(k)
        a2a_copy(s, sector).wait_send()
        back_copy(s, sector).wait_send()
        return carry

    lax.fori_loop(0, SECTORS - 1, wait_sent, 0)

    @pl.when(own)
    def _():
        for index in range(3):
            share_copy(index).wait_send()

    for each in (t_spread, p_spread, tp_spread):
        each.sent()


def on_device(
    leaf_out,
    interp_mid,
    shift_mid,
    trans_mid,
    list_mid,
    offset_mid,
    interp_top,
    shift_top,
    trans_top,
    list_top,
    offset_top,
):
    offsets = trans_mid.shape[1]
    entries = list_mid.shape[1]
    rows = 2 * leaf_out.shape[1]
    operands = (
        leaf_out,
        interp_mid,
        shift_mid,
        trans_top.reshape(2 * offsets, LANES),
        jnp.transpose(trans_mid.reshape(2, offsets, 2, LANES), (1, 2, 0, 3)).reshape(4 * offsets, LANES),
        interp_top[0],
        shift_top.reshape(64, LANES),
        list_mid.T,
        offset_mid.T,
        list_top.T,
        offset_top.T,
    )
    padded = 640
    result = pl.pallas_call(
        kernel,
        out_shape=VMEM(leaf_out.shape, F32),
        in_specs=[pl.BlockSpec(memory_space=pltpu.HBM)] * len(operands),
        out_specs=pl.BlockSpec(memory_space=VMEM),
        scratch_shapes=[
            VMEM(leaf_out.shape, BF16),
            VMEM(interp_mid.shape, BF16),
            VMEM(shift_mid.shape, F32),
            VMEM((2 * offsets, LANES), F32),
            VMEM((4 * offsets, LANES), F32),
            VMEM((256, 1024), BF16),
            VMEM((64, LANES), F32),
            VMEM((2, entries, 256), jnp.int32),
            VMEM((2, entries, 128), jnp.int32),
            VMEM((2, 256, entries), jnp.int32),
            VMEM((2, 128, entries), jnp.int32),
            pltpu.SMEM((256, entries), jnp.int32),
            pltpu.SMEM((256, entries), jnp.int32),
            pltpu.SMEM((128, entries), jnp.int32),
            pltpu.SMEM((128, entries), jnp.int32),
            VMEM((PLANES, 2, 512, LANES), BF16),
            VMEM((PLANES, 2, 256, LANES), BF16),
            VMEM((PLANES, 2, padded, LANES), BF16),
            VMEM((rows, interp_mid.shape[0]), BF16),
            VMEM(shift_mid.shape, F32),
            VMEM(shift_mid.shape, F32),
            VMEM((SECTORS, 32, LANES), BF16),
            VMEM((128, LANES), F32),
            VMEM((padded, LANES), BF16),
            VMEM((512, LANES), F32),
            VMEM((256, 256), BF16),
            VMEM((256, LANES), F32),
            VMEM((64, LANES), F32),
            VMEM((64, LANES), F32),
            VMEM((1024 * 8, LANES), F32),
            VMEM((offsets * 8, LANES), F32),
            VMEM((128 * 16, LANES), F32),
            VMEM((padded * 8, LANES), F32),
            VMEM((128 * 8, LANES), F32),
            VMEM((16 * 16, LANES), F32),
            VMEM((256, 1024), BF16),
            VMEM((256, 256), F32),
            VMEM((SECTORS, 16, 256), BF16),
            VMEM((SECTORS, 16, 256), BF16),
            VMEM((rows, 1024), BF16),
            VMEM((interp_mid.shape[0], rows), F32),
            DMA((4,)),
            DMA((7,)),
            DMA((4,)),
            DMA((SECTORS,)),
            DMA((SECTORS,)),
            DMA((2,)),
            DMA((3,)),
            DMA((3,)),
            DMA((10,)),
            DMA((10,)),
            DMA((10,)),
            DMA((10,)),
            DMA((10,)),
            DMA((10,)),
            DMA((SECTORS,)),
            DMA((SECTORS,)),
        ],
        compiler_params=pltpu.CompilerParams(
            collective_id=0, has_side_effects=True, vmem_limit_bytes=60 * 1024 * 1024
        ),
        name="far_field",
    )(*operands)
    return result * (interp_mid.shape[0] / interp_mid.shape[1])


def solution(mesh):
    return jax.shard_map(
        on_device,
        mesh=mesh,
        in_specs=(
            P(None, ("box", "dir"), None),
            P(),
            P(),
            P(None, None, "dir"),
            P(),
            P(),
            P("dir", None, None),
            P(None, "dir", None),
            P(None, None, "dir", "box"),
            P(),
            P(),
        ),
        out_specs=P(None, ("box", "dir"), None),
        check_vma=False,
    )
```

```python
import jax
import jax.numpy as jnp
from jax import lax
from jax.experimental import pallas as pl
from jax.experimental.pallas import tpu as pltpu
from jax.sharding import PartitionSpec as P

MESH = pl.DeviceIdType.MESH
F32 = jnp.float32
BF16 = jnp.bfloat16
VMEM = pltpu.VMEM
DMA = pltpu.SemaphoreType.DMA
PLANES = 4
SECTORS = 16
LANES = 128


def place():
    box = lax.axis_index("box")
    way = lax.axis_index("dir")
    low = box % 2
    core = way % 2
    return box // 2, way - core + low, core


def device_of(plane, sector, core):
    low = sector % 2
    return (plane * 2 + low, sector - low + core)


def sin_cos(angle):
    half = angle * 0.5
    sq = half * half
    s = sq * (-1.0 / 39916800.0) + (1.0 / 362880.0)
    s = sq * s - (1.0 / 5040.0)
    s = sq * s + (1.0 / 120.0)
    s = sq * s - (1.0 / 6.0)
    s = half + half * (sq * s)
    c = sq * (1.0 / 479001600.0) - (1.0 / 3628800.0)
    c = sq * c + (1.0 / 40320.0)
    c = sq * c - (1.0 / 720.0)
    c = sq * c + (1.0 / 24.0)
    c = sq * c - 0.5
    c = sq * c + 1.0
    return 2.0 * s * c, 1.0 - 2.0 * s * s


class Spread:
    def __init__(self, ref, send, recv):
        z, sector, core = place()
        self.ref, self.send, self.recv = ref, send, recv
        self.core = core
        self.z = z
        self.left = (z + PLANES - 1) % PLANES
        self.right = (z + 1) % PLANES
        self.far = (z + 2) % PLANES
        self.to_right = device_of(self.right, sector, core)
        self.to_left = device_of(self.left, sector, core)
        self.partner = device_of(z, sector, 1 - core)
        self.rows = ref.shape[2]
        self.crossing = ((4, self.z), (5, self.left), (6, self.right), (7, self.far))

    def copy(self, plane, core, half, index, target):
        rows = self.rows
        if half is None:
            part = self.ref.at[plane, core]
        else:
            part = self.ref.at[plane, core, pl.ds(half * (rows // 2), rows // 2)]
        return pltpu.make_async_remote_copy(
            src_ref=part,
            dst_ref=part,
            send_sem=self.send.at[index],
            recv_sem=self.recv.at[index],
            device_id=target,
            device_id_type=MESH,
        )

    def start_own(self):
        self.copy(self.z, self.core, 0, 0, self.to_right).start()
        self.copy(self.z, self.core, 1, 1, self.to_left).start()
        self.copy(self.z, self.core, 1, 8, self.to_right).start()
        self.copy(self.z, self.core, 0, 9, self.to_left).start()
        self.copy(self.z, self.core, None, 4, self.partner).start()

    def forward(self):
        self.copy(self.left, self.core, 0, 0, self.to_right).wait_recv()
        self.copy(self.left, self.core, 0, 2, self.to_right).start()
        self.copy(self.right, self.core, 1, 1, self.to_left).wait_recv()
        self.copy(self.right, self.core, 1, 3, self.to_left).start()

    def forward_rest(self):
        self.copy(self.left, self.core, 1, 8, self.to_right).wait_recv()
        self.copy(self.left, self.core, None, 5, self.partner).start()
        self.copy(self.right, self.core, 0, 9, self.to_left).wait_recv()
        self.copy(self.right, self.core, None, 6, self.partner).start()

    def forward_far(self):
        self.copy(self.far, self.core, 0, 2, self.to_right).wait_recv()
        self.copy(self.far, self.core, 1, 3, self.to_left).wait_recv()
        self.copy(self.far, self.core, None, 7, self.partner).start()

    def take(self, which):
        index, plane = self.crossing[which]
        self.copy(plane, 1 - self.core, None, index, self.partner).wait_recv()
        return plane

    def sent(self):
        self.copy(self.z, self.core, 0, 0, self.to_right).wait_send()
        self.copy(self.z, self.core, 1, 1, self.to_left).wait_send()
        self.copy(self.z, self.core, 1, 8, self.to_right).wait_send()
        self.copy(self.z, self.core, 0, 9, self.to_left).wait_send()
        self.copy(self.left, self.core, 0, 2, self.to_right).wait_send()
        self.copy(self.right, self.core, 1, 3, self.to_left).wait_send()
        for index, plane in self.crossing:
            self.copy(plane, self.core, None, index, self.partner).wait_send()


def kernel(
    leaf_ref,
    matrix_ref,
    shift_mid_ref,
    trans_top_ref,
    trans_mid_ref,
    interp_top_ref,
    shift_top_ref,
    list_mid_ref,
    offset_mid_ref,
    list_top_ref,
    offset_top_ref,
    out_ref,
    leaf,
    weights,
    shift_mid,
    trans_top,
    trans_mid,
    interp_top,
    shift_top,
    lists_mid,
    lists_top,
    scaled_mid,
    scaled_top,
    list_s,
    offset_s,
    list_ts,
    offset_ts,
    p_all,
    tp_all,
    t_all,
    leaf_rows,
    cos_mid,
    sin_mid,
    sending,
    stage,
    piece,
    block_f32,
    top_lhs,
    top_f32,
    cos_top,
    sin_top,
    p_tab,
    t_tab,
    p_top,
    t_top,
    mid_sum,
    top_sum,
    child_rows,
    down,
    pieces,
    received,
    children,
    total,
    weight_sem,
    load_sem,
    index_sem,
    a2a_send,
    a2a_recv,
    swap_sem,
    share_send,
    share_recv,
    t_send,
    t_recv,
    p_send,
    p_recv,
    tp_send,
    tp_recv,
    back_send,
    back_recv,
):
    z, sector, core = place()
    entries = list_mid_ref.shape[0]
    low = sector % 2
    own = low == core
    partner = device_of(z, sector, 1 - core)
    swap = device_of(z, sector - low + core, low)
    right = device_of((z + 1) % PLANES, sector, core)
    left = device_of((z + PLANES - 1) % PLANES, sector, core)
    t_spread = Spread(t_all, t_send, t_recv)
    p_spread = Spread(p_all, p_send, p_recv)
    tp_spread = Spread(tp_all, tp_send, tp_recv)

    group = sector // 4
    inside = sector % 4

    def apart(a, k):
        high = (a // 2 + k + 1) % 2
        return high * 2 + (a % 2 + 1 + k // 2) % 2

    def nth(k):
        return apart(group, k // 4) * 4 + apart(inside, k % 4)

    def other(k):
        return (sector + 1 + k) % SECTORS

    def to_sector(s):
        return device_of(z, s, core)

    barrier = pltpu.get_barrier_semaphore()

    def signal_peer(k, carry):
        pl.semaphore_signal(barrier, inc=1, device_id=to_sector(other(k)), device_id_type=MESH)
        return carry

    lax.fori_loop(0, SECTORS - 1, signal_peer, 0)
    for device in (right, left, partner):
        pl.semaphore_signal(barrier, inc=1, device_id=device, device_id_type=MESH)

    @pl.when(jnp.logical_not(own))
    def _():
        pl.semaphore_signal(barrier, inc=1, device_id=swap, device_id_type=MESH)

    slab = pl.ds(pl.multiple_of(z * 256, 256), 256)
    loads = [
        pltpu.make_async_copy(source, target, load_sem.at[index])
        for index, (source, target) in enumerate(
            (
                (leaf_ref, leaf),
                (trans_top_ref, trans_top),
                (shift_mid_ref, shift_mid),
                (list_mid_ref.at[:, slab], lists_mid.at[0]),
                (offset_mid_ref.at[:, slab], lists_mid.at[1]),
                (list_top_ref, lists_top.at[0]),
                (offset_top_ref, lists_top.at[1]),
            )
        )
    ]
    for copy in loads[:3]:
        copy.start()

    def weight_copy(piece_at):
        columns = pl.ds(pl.multiple_of(apart(group, piece_at) * 1024, 1024), 1024)
        return pltpu.make_async_copy(matrix_ref.at[:, columns], weights.at[:, columns], weight_sem.at[piece_at])

    for piece_at in range(4):
        weight_copy(piece_at).start()
    for copy in loads[3:]:
        copy.start()

    loads[0].wait()
    rows = 2 * leaf.shape[1]
    target = lax.broadcasted_iota(jnp.int32, (rows, rows), 0)
    source = lax.broadcasted_iota(jnp.int32, (rows, rows), 1)
    wanted = (target & 64) + ((target & 7) << 3) + ((target >> 3) & 7)
    order = (source == wanted).astype(BF16)
    both = jnp.concatenate([leaf[0], leaf[1]], axis=0)
    leaf_rows[...] = jnp.dot(order, both, preferred_element_type=F32).astype(BF16)

    loads[1].wait()
    used = trans_top.shape[0]
    piece[0:used, :] = trans_top[...].astype(BF16)
    piece[used:, :] = jnp.zeros((piece.shape[0] - used, LANES), BF16)

    swap_copy = pltpu.make_async_remote_copy(
        src_ref=piece,
        dst_ref=t_all.at[z, low],
        send_sem=swap_sem.at[0],
        recv_sem=swap_sem.at[1],
        device_id=swap,
        device_id_type=MESH,
    )
    shared = ((trans_mid_ref, trans_mid), (interp_top_ref, interp_top), (shift_top_ref, shift_top))

    def share_copy(index):
        return pltpu.make_async_remote_copy(
            src_ref=shared[index][0],
            dst_ref=shared[index][1],
            send_sem=share_send.at[index],
            recv_sem=share_recv.at[index],
            device_id=partner,
            device_id_type=MESH,
        )

    def local_copy(index):
        return pltpu.make_async_copy(shared[index][0], shared[index][1], share_recv.at[index])

    loads[2].wait()
    sines, cosines = sin_cos(shift_mid[...])
    cos_mid[...] = cosines
    sin_mid[...] = sines

    def parents(s, slot):
        columns = pl.ds(pl.multiple_of(s * 256, 256), 256)
        spread = jnp.dot(leaf_rows[...], weights[:, columns], preferred_element_type=F32)
        real_sum = jnp.zeros((8, 256), F32)
        imag_sum = jnp.zeros((8, 256), F32)
        for child in range(8):
            real = spread[child * 8 : child * 8 + 8]
            imag = spread[64 + child * 8 : 64 + child * 8 + 8]
            c = cos_mid[child : child + 1, columns]
            n = sin_mid[child : child + 1, columns]
            real_sum += real * c - imag * n
            imag_sum += real * n + imag * c
        for part in range(2):
            lanes = slice(part * LANES, part * LANES + LANES)
            stage[pl.ds(slot * 32 + part, 8, stride=4), :] = real_sum[:, lanes]
            stage[pl.ds(slot * 32 + 2 + part, 8, stride=4), :] = imag_sum[:, lanes]
        return stage[slot * 32 : slot * 32 + 32, :].astype(BF16)

    def rows_of(s):
        return p_all.at[z, core, pl.ds(pl.multiple_of(s * 32, 32), 32)]

    def a2a_copy(s, landing):
        return pltpu.make_async_remote_copy(
            src_ref=sending.at[s],
            dst_ref=rows_of(landing),
            send_sem=a2a_send.at[s],
            recv_sem=a2a_recv.at[landing],
            device_id=to_sector(s),
            device_id_type=MESH,
        )

    def make_four(piece_at):
        weight_copy(piece_at).wait()
        for slot in range(4):
            s = nth(piece_at * 4 + slot)
            sending[s] = parents(s, slot)

    def start_four(piece_at):
        for slot in range(4):
            a2a_copy(nth(piece_at * 4 + slot), sector).start()

    make_four(0)
    pl.semaphore_wait(barrier, SECTORS - 1 + 3 + (low + core) % 2)

    @pl.when(own)
    def _():
        for index in range(3):
            share_copy(index).start()
            local_copy(index).start()
        t_all[z, core] = piece[...]
        t_spread.start_own()

    @pl.when(jnp.logical_not(own))
    def _():
        swap_copy.start()

    start_four(0)

    def send_four(piece_at, carry):
        make_four(piece_at)
        start_four(piece_at)
        return carry

    lax.fori_loop(1, 3, send_four, 0)
    weight_copy(3).wait()
    for slot in range(3):
        s = nth(12 + slot)
        sending[s] = parents(s, slot)
        a2a_copy(s, sector).start()
    p_all[z, core, pl.ds(pl.multiple_of(sector * 32, 32), 32), :] = parents(sector, 3)

    total[...] = jnp.zeros_like(total)

    for copy in loads[3:]:
        copy.wait()
    scaled = jnp.transpose(jnp.concatenate([lists_mid[0], lists_mid[1]], axis=0) * 8)
    scaled_mid[0] = scaled[:, :entries]
    scaled_mid[1] = scaled[:, entries:]
    scaled = jnp.transpose(jnp.concatenate([lists_top[0] * 16, lists_top[1] * 8], axis=0))
    scaled_top[0] = scaled[:, :entries]
    scaled_top[1] = scaled[:, entries:]
    to_smem = [
        pltpu.make_async_copy(scaled_mid.at[0], list_s, index_sem.at[0]),
        pltpu.make_async_copy(scaled_mid.at[1], offset_s, index_sem.at[1]),
        pltpu.make_async_copy(scaled_top.at[0], list_ts, index_sem.at[2]),
        pltpu.make_async_copy(scaled_top.at[1], offset_ts, index_sem.at[3]),
    ]
    for copy in to_smem:
        copy.start()

    @pl.when(own)
    def _():
        for index in range(3):
            local_copy(index).wait()

    @pl.when(jnp.logical_not(own))
    def _():
        for index in range(3):
            share_copy(index).wait_recv()

    offsets = trans_mid.shape[0] // 4

    def put_offsets(first, row):
        for quarter, places in enumerate(((0, 2), (4, 6), (1, 3), (5, 7))):
            v = trans_mid[pl.ds(first + quarter, 8, stride=4), :]
            for at in places:
                t_tab[pl.ds(row + at, 8, stride=8), :] = v

    def mid_offsets(k, carry):
        put_offsets(pl.multiple_of(k * 32, 32), pl.multiple_of(k * 64, 64))
        return carry

    lax.fori_loop(0, offsets // 8, mid_offsets, 0)
    if offsets % 8:
        put_offsets((offsets - 8) * 4, (offsets - 8) * 8)

    sines_t, cosines_t = sin_cos(shift_top[...])
    cos_top[...] = cosines_t
    sin_top[...] = sines_t

    def wait_sector(k, carry):
        s = other(k)
        a2a_copy(s, s).wait_recv()
        return carry

    lax.fori_loop(0, SECTORS - 1, wait_sector, 0)
    p_spread.start_own()

    block_f32[...] = p_all[z, core].astype(F32)
    for child in range(8):
        for part in range(2):
            for side in range(2):
                first = child * 4 + part * 2 + side
                a = block_f32[pl.ds(first, 8, stride=32), :]
                b = block_f32[pl.ds(256 + first, 8, stride=32), :]
                top_lhs[
                    part * 128 + child * 16 : part * 128 + child * 16 + 16, side * LANES : side * LANES + LANES
                ] = jnp.concatenate([a, b], axis=0).astype(BF16)

    def top_columns(k, carry):
        columns = pl.ds(pl.multiple_of(k * 256, 256), 256)
        spread = jnp.dot(top_lhs[...], interp_top[:, columns], preferred_element_type=F32)
        for part in range(2):
            lanes = slice(part * LANES, part * LANES + LANES)
            group = k * 2 + part
            real_sum = jnp.zeros((16, LANES), F32)
            imag_sum = jnp.zeros((16, LANES), F32)
            for child in range(8):
                real = spread[child * 16 : child * 16 + 16, lanes]
                imag = spread[128 + child * 16 : 128 + child * 16 + 16, lanes]
                c = cos_top[pl.ds(child * 8 + group, 1), :]
                n = sin_top[pl.ds(child * 8 + group, 1), :]
                real_sum += real * c - imag * n
                imag_sum += real * n + imag * c
            for half in range(2):
                boxes = slice(half * 8, half * 8 + 8)
                top_f32[pl.ds(half * 128 + group, 8, stride=16), :] = real_sum[boxes]
                top_f32[pl.ds(half * 128 + 8 + group, 8, stride=16), :] = imag_sum[boxes]
        return carry

    lax.fori_loop(0, 4, top_columns, 0)
    tp_all[z, core] = top_f32[...].astype(BF16)

    upper = lax.broadcasted_iota(jnp.int32, (8, LANES), 0) < 4

    def mid_table(plane, side):
        def four(k, carry):
            for part in range(4):
                odd = part % 2
                found = p_all[plane, side, pl.ds(pl.multiple_of(k * 128 + part * 32, 32), 32), :].astype(F32)
                first = ((2 * plane + odd) * 128 + (k * 4 + part - odd + side) * 8) * 8
                for pair in range(4):
                    v = found[pair * 8 : pair * 8 + 8]
                    r = pltpu.roll(v, 4, 0)
                    at = first + pair * 16
                    p_tab[pl.ds(pl.multiple_of(at, 8), 8), :] = jnp.where(upper, v, r)
                    p_tab[pl.ds(pl.multiple_of(at + 8, 8), 8), :] = jnp.where(upper, r, v)
            return carry

        lax.fori_loop(0, SECTORS // 4, four, 0)

    def top_table(plane, side):
        def four(k, carry):
            for part in range(4):
                odd = part % 2
                found = tp_all[plane, side, pl.ds(pl.multiple_of(k * 64 + part * 16, 16), 16), :].astype(F32)
                first = ((2 * plane + odd) * 16 + (k * 4 + part - odd + side)) * 16
                p_top[pl.ds(pl.multiple_of(first, 16), 16), :] = found
            return carry

        lax.fori_loop(0, SECTORS // 4, four, 0)

    def offset_table(plane, side):
        at = plane * 2 + side

        def four(k, carry):
            for part in range(4):
                found = t_all[plane, side, pl.ds(pl.multiple_of(k * 64 + part * 16, 16), 16), :].astype(F32)
                for half in range(2):
                    t_top[pl.ds(k * 512 + part * 128 + half * 64 + at, 8, stride=8), :] = found[
                        half * 8 : half * 8 + 8
                    ]
            return carry

        lax.fori_loop(0, t_all.shape[2] // 64, four, 0)

    mid_table(z, core)
    top_table(z, core)
    p_spread.forward()
    tp_spread.start_own()
    p_spread.forward_rest()

    @pl.when(jnp.logical_not(own))
    def _():
        swap_copy.wait()
        t_spread.start_own()

    mid_table(p_spread.left, core)
    mid_table(p_spread.right, core)
    mid_table(p_spread.take(0), 1 - core)
    for copy in to_smem:
        copy.wait()
    p_spread.forward_far()
    mid_table(p_spread.far, core)
    mid_table(p_spread.take(1), 1 - core)
    mid_table(p_spread.take(2), 1 - core)
    mid_table(p_spread.take(3), 1 - core)

    def middle(k, beside=None):
        s = nth(k)
        odd = s % 2
        first = odd * 128 + (s - odd + core) * 8

        def mid_box(i, carry):
            kept = jnp.zeros((8, LANES), F32)
            for j in range(entries):
                p = p_tab[pl.ds(list_s[first + i, j], 8), :]
                t = t_tab[pl.ds(offset_s[first + i, j], 8), :]
                kept = kept + p * t
            mid_sum[pl.ds(pl.multiple_of(k * 64 + i * 8, 8), 8), :] = kept
            if beside is not None:
                beside(i)
            return carry

        lax.fori_loop(0, 8, mid_box, 0)

    def middle_early(k, carry):
        middle(k)
        return carry

    def offset_part(plane, side, i):
        at = plane * 2 + side
        for part in range(t_all.shape[2] // 128):
            row = i * (t_all.shape[2] // 8) + part * 16
            found = t_all[plane, side, pl.ds(pl.multiple_of(row, 16), 16), :].astype(F32)
            for half in range(2):
                t_top[pl.ds(row * 8 + half * 64 + at, 8, stride=8), :] = found[half * 8 : half * 8 + 8]

    def top_part(plane, side, i):
        for odd in range(2):
            found = tp_all[plane, side, pl.ds(pl.multiple_of(i * 32 + odd * 16, 16), 16), :].astype(F32)
            first = ((2 * plane + odd) * 16 + (i * 2 + side)) * 16
            p_top[pl.ds(pl.multiple_of(first, 16), 16), :] = found

    ahead = 8
    z_left, z_right, z_far = t_spread.left, t_spread.right, t_spread.far
    away = 1 - core
    lax.fori_loop(0, 2, middle_early, 0)
    tp_spread.forward()
    t_spread.forward()
    tp_spread.forward_rest()
    t_spread.forward_rest()

    def tables2(i):
        offset_part(z, core, i)
        offset_part(z_left, core, i)
        top_part(z_left, core, i)

    middle(2, tables2)
    t_spread.take(0)
    tp_spread.take(0)

    def tables3(i):
        offset_part(z_right, core, i)
        offset_part(z, away, i)
        top_part(z_right, core, i)
        top_part(z, away, i)

    middle(3, tables3)
    t_spread.take(1)
    t_spread.take(2)
    tp_spread.take(1)
    tp_spread.take(2)

    def tables4(i):
        offset_part(z_left, away, i)
        offset_part(z_right, away, i)
        top_part(z_left, away, i)
        top_part(z_right, away, i)

    middle(4, tables4)
    middle(5)
    tp_spread.forward_far()
    t_spread.forward_far()

    def tables6(i):
        offset_part(z_far, core, i)
        top_part(z_far, core, i)

    middle(6, tables6)
    middle(7)
    t_spread.take(3)
    tp_spread.take(3)
    offset_table(z_far, away)
    top_table(z_far, away)

    behind = (trans_top_ref.shape[0] // 2) * 8

    def top_box(k, carry):
        odd = k % 2
        column = (2 * z + odd) * 16 + (k - odd + core)
        sums = [jnp.zeros((8, LANES), F32) for _ in range(4)]
        for j in range(entries):
            n = list_ts[column, j]
            o = offset_ts[column, j]
            pr = p_top[pl.ds(n, 8), :]
            pi = p_top[pl.ds(n + 8, 8), :]
            tr = t_top[pl.ds(o, 8), :]
            ti = t_top[pl.ds(o + behind, 8), :]
            sums = [sums[0] + pr * tr, sums[1] + pi * ti, sums[2] + pr * ti, sums[3] + pi * tr]
        real = (sums[0] - sums[1]).astype(BF16).astype(F32)
        imag = (sums[2] + sums[3]).astype(BF16).astype(F32)
        top_sum[pl.ds(pl.multiple_of(k * 16, 16), 8), :] = real
        top_sum[pl.ds(pl.multiple_of(k * 16 + 8, 8), 8), :] = imag
        return carry

    lax.fori_loop(0, SECTORS, top_box, 0)

    def top_children(part, carry):
        lanes = pl.ds(pl.multiple_of(part * LANES, LANES), LANES)
        c = cos_top[pl.ds(part, 8, stride=8), :]
        n = sin_top[pl.ds(part, 8, stride=8), :]
        for pair in range(8):
            reals = []
            imags = []
            for half in range(2):
                first = pair * 32 + half * 16
                real = jnp.broadcast_to(top_sum[pl.ds(first + part, 1), :], (8, LANES))
                imag = jnp.broadcast_to(top_sum[pl.ds(first + 8 + part, 1), :], (8, LANES))
                reals.append(real * c + imag * n)
                imags.append(imag * c - real * n)
            child_rows[pair * 16 : pair * 16 + 16, lanes] = jnp.concatenate(reals, axis=0).astype(BF16)
            child_rows[128 + pair * 16 : 144 + pair * 16, lanes] = jnp.concatenate(imags, axis=0).astype(BF16)
        return carry

    lax.fori_loop(0, 8, top_children, 0)
    scale = interp_top.shape[0] / interp_top.shape[1]
    down[...] = scale * lax.dot_general(
        child_rows[...], interp_top[...], (((1,), (1,)), ((), ())), preferred_element_type=F32
    )

    def back_copy(s, landing):
        return pltpu.make_async_remote_copy(
            src_ref=pieces.at[s],
            dst_ref=received.at[landing],
            send_sem=back_send.at[s],
            recv_sem=back_recv.at[landing],
            device_id=to_sector(s),
            device_id_type=MESH,
        )

    def combine(n):
        k = nth(n)
        at = pl.multiple_of(k * 8, 8)
        sides = []
        for side in range(2):
            lanes = slice(side * LANES, side * LANES + LANES)
            parts = [mid_sum[pl.ds(n * 64 + side + 2 * quarter, 8, stride=8), :] for quarter in range(4)]
            real = (parts[0] - parts[3]) + down[pl.ds(at, 8), lanes]
            imag = (parts[1] + parts[2]) + down[pl.ds(pl.multiple_of(128 + k * 8, 8), 8), lanes]
            sides.append(jnp.concatenate([real, imag], axis=0).astype(BF16))
        return jnp.concatenate(sides, axis=1)

    def make_children(s, at):
        columns = pl.ds(pl.multiple_of(s * 256, 256), 256)
        c = cos_mid[:, columns]
        n = sin_mid[:, columns]
        found = received[s].astype(F32)
        target = pl.ds(pl.multiple_of(at * 256, 256), 256)
        for pair in range(4):
            reals = []
            imags = []
            for half in range(2):
                box = pair * 2 + half
                real = jnp.broadcast_to(found[box : box + 1], (8, 256))
                imag = jnp.broadcast_to(found[8 + box : 9 + box], (8, 256))
                reals.append(real * c + imag * n)
                imags.append(imag * c - real * n)
            children[pair * 16 : pair * 16 + 16, target] = jnp.concatenate(reals, axis=0).astype(BF16)
            children[64 + pair * 16 : 80 + pair * 16, target] = jnp.concatenate(imags, axis=0).astype(BF16)

    def take_piece(piece_at, count):
        at = apart(group, piece_at)
        for slot in range(count):
            s = at * 4 + apart(inside, slot)
            back_copy(s, s).wait_recv()
        for slot in range(4):
            make_children(at * 4 + slot, slot)

    block = 512

    def product(at, k):
        columns = pl.ds(pl.multiple_of(at * 1024, 1024), 1024)
        rows_at = pl.ds(k * block, block)
        return lax.dot_general(
            weights[rows_at, columns], children[...], (((1,), (1,)), ((), ())), preferred_element_type=F32
        )

    def finish_piece(piece_at, carry):
        take_piece(piece_at, 4)
        for k in range(total.shape[0] // block):
            total[k * block : k * block + block, :] += product(apart(group, piece_at), k)
        return carry

    def send_back(k, carry):
        s = nth(k)
        pieces[s] = combine(k)
        back_copy(s, sector).start()
        return carry

    def middle_and_send(k, carry):
        middle(k)
        return send_back(k, carry)

    lax.fori_loop(0, ahead, send_back, 0)
    lax.fori_loop(ahead, SECTORS - 1, middle_and_send, 0)
    middle(SECTORS - 1)
    received[sector] = combine(SECTORS - 1)
    lax.fori_loop(0, 3, finish_piece, 0)
    take_piece(3, 3)
    half_rows = out_ref.shape[1]
    for k in range(total.shape[0] // block):
        part = product(group, k)
        for n in range(k * block // 256, (k + 1) * block // 256):
            rows_at = slice(n * 256, n * 256 + 256)
            turned = jnp.transpose(total[rows_at, :] + part[n * 256 - k * block : n * 256 - k * block + 256])
            for which in range(2):
                out_ref[which, :, rows_at] = turned[which * half_rows : which * half_rows + half_rows]

    def wait_sent(k, carry):
        s = other(k)
        a2a_copy(s, sector).wait_send()
        back_copy(s, sector).wait_send()
        return carry

    lax.fori_loop(0, SECTORS - 1, wait_sent, 0)

    @pl.when(own)
    def _():
        for index in range(3):
            share_copy(index).wait_send()

    for each in (t_spread, p_spread, tp_spread):
        each.sent()


def on_device(
    leaf_out,
    interp_mid,
    shift_mid,
    trans_mid,
    list_mid,
    offset_mid,
    interp_top,
    shift_top,
    trans_top,
    list_top,
    offset_top,
):
    offsets = trans_mid.shape[1]
    entries = list_mid.shape[1]
    rows = 2 * leaf_out.shape[1]
    operands = (
        leaf_out,
        interp_mid,
        shift_mid,
        trans_top.reshape(2 * offsets, LANES),
        jnp.transpose(trans_mid.reshape(2, offsets, 2, LANES), (1, 2, 0, 3)).reshape(4 * offsets, LANES),
        interp_top[0],
        shift_top.reshape(64, LANES),
        list_mid.T,
        offset_mid.T,
        list_top.T,
        offset_top.T,
    )
    padded = 640
    result = pl.pallas_call(
        kernel,
        out_shape=VMEM(leaf_out.shape, F32),
        in_specs=[pl.BlockSpec(memory_space=pltpu.HBM)] * len(operands),
        out_specs=pl.BlockSpec(memory_space=VMEM),
        scratch_shapes=[
            VMEM(leaf_out.shape, BF16),
            VMEM(interp_mid.shape, BF16),
            VMEM(shift_mid.shape, F32),
            VMEM((2 * offsets, LANES), F32),
            VMEM((4 * offsets, LANES), F32),
            VMEM((256, 1024), BF16),
            VMEM((64, LANES), F32),
            VMEM((2, entries, 256), jnp.int32),
            VMEM((2, entries, 128), jnp.int32),
            VMEM((2, 256, entries), jnp.int32),
            VMEM((2, 128, entries), jnp.int32),
            pltpu.SMEM((256, entries), jnp.int32),
            pltpu.SMEM((256, entries), jnp.int32),
            pltpu.SMEM((128, entries), jnp.int32),
            pltpu.SMEM((128, entries), jnp.int32),
            VMEM((PLANES, 2, 512, LANES), BF16),
            VMEM((PLANES, 2, 256, LANES), BF16),
            VMEM((PLANES, 2, padded, LANES), BF16),
            VMEM((rows, interp_mid.shape[0]), BF16),
            VMEM(shift_mid.shape, F32),
            VMEM(shift_mid.shape, F32),
            VMEM((SECTORS, 32, LANES), BF16),
            VMEM((128, LANES), F32),
            VMEM((padded, LANES), BF16),
            VMEM((512, LANES), F32),
            VMEM((256, 256), BF16),
            VMEM((256, LANES), F32),
            VMEM((64, LANES), F32),
            VMEM((64, LANES), F32),
            VMEM((1024 * 8, LANES), F32),
            VMEM((offsets * 8, LANES), F32),
            VMEM((128 * 16, LANES), F32),
            VMEM((padded * 8, LANES), F32),
            VMEM((128 * 8, LANES), F32),
            VMEM((16 * 16, LANES), F32),
            VMEM((256, 1024), BF16),
            VMEM((256, 256), F32),
            VMEM((SECTORS, 16, 256), BF16),
            VMEM((SECTORS, 16, 256), BF16),
            VMEM((rows, 1024), BF16),
            VMEM((interp_mid.shape[0], rows), F32),
            DMA((4,)),
            DMA((7,)),
            DMA((4,)),
            DMA((SECTORS,)),
            DMA((SECTORS,)),
            DMA((2,)),
            DMA((3,)),
            DMA((3,)),
            DMA((10,)),
            DMA((10,)),
            DMA((10,)),
            DMA((10,)),
            DMA((10,)),
            DMA((10,)),
            DMA((SECTORS,)),
            DMA((SECTORS,)),
        ],
        compiler_params=pltpu.CompilerParams(
            collective_id=0, has_side_effects=True, vmem_limit_bytes=60 * 1024 * 1024
        ),
        name="far_field",
    )(*operands)
    return result * (interp_mid.shape[0] / interp_mid.shape[1])


def solution(mesh):
    return jax.shard_map(
        on_device,
        mesh=mesh,
        in_specs=(
            P(None, ("box", "dir"), None),
            P(),
            P(),
            P(None, None, "dir"),
            P(),
            P(),
            P("dir", None, None),
            P(None, "dir", None),
            P(None, None, "dir", "box"),
            P(),
            P(),
        ),
        out_specs=P(None, ("box", "dir"), None),
        check_vma=False,
    )
```

```python
import jax
import jax.numpy as jnp
from jax import lax
from jax.experimental import pallas as pl
from jax.experimental.pallas import tpu as pltpu
from jax.sharding import PartitionSpec as P

MESH = pl.DeviceIdType.MESH
F32 = jnp.float32
BF16 = jnp.bfloat16
VMEM = pltpu.VMEM
DMA = pltpu.SemaphoreType.DMA
PLANES = 4
SECTORS = 16
LANES = 128


def place():
    box = lax.axis_index("box")
    way = lax.axis_index("dir")
    low = box % 2
    core = way % 2
    return box // 2, way - core + low, core


def device_of(plane, sector, core):
    low = sector % 2
    return (plane * 2 + low, sector - low + core)


def sin_cos(angle):
    half = angle * 0.5
    sq = half * half
    s = sq * (-1.0 / 39916800.0) + (1.0 / 362880.0)
    s = sq * s - (1.0 / 5040.0)
    s = sq * s + (1.0 / 120.0)
    s = sq * s - (1.0 / 6.0)
    s = half + half * (sq * s)
    c = sq * (1.0 / 479001600.0) - (1.0 / 3628800.0)
    c = sq * c + (1.0 / 40320.0)
    c = sq * c - (1.0 / 720.0)
    c = sq * c + (1.0 / 24.0)
    c = sq * c - 0.5
    c = sq * c + 1.0
    return 2.0 * s * c, 1.0 - 2.0 * s * s


class Spread:
    def __init__(self, ref, send, recv):
        z, sector, core = place()
        self.ref, self.send, self.recv = ref, send, recv
        self.core = core
        self.z = z
        self.left = (z + PLANES - 1) % PLANES
        self.right = (z + 1) % PLANES
        self.far = (z + 2) % PLANES
        self.to_right = device_of(self.right, sector, core)
        self.to_left = device_of(self.left, sector, core)
        self.partner = device_of(z, sector, 1 - core)
        self.rows = ref.shape[2]
        self.crossing = ((4, self.z), (5, self.left), (6, self.right), (7, self.far))

    def copy(self, plane, core, half, index, target):
        rows = self.rows
        if half is None:
            part = self.ref.at[plane, core]
        else:
            part = self.ref.at[plane, core, pl.ds(half * (rows // 2), rows // 2)]
        return pltpu.make_async_remote_copy(
            src_ref=part,
            dst_ref=part,
            send_sem=self.send.at[index],
            recv_sem=self.recv.at[index],
            device_id=target,
            device_id_type=MESH,
        )

    def start_own(self):
        self.copy(self.z, self.core, 0, 0, self.to_right).start()
        self.copy(self.z, self.core, 1, 1, self.to_left).start()
        self.copy(self.z, self.core, 1, 8, self.to_right).start()
        self.copy(self.z, self.core, 0, 9, self.to_left).start()
        self.copy(self.z, self.core, None, 4, self.partner).start()

    def forward(self):
        self.copy(self.left, self.core, 0, 0, self.to_right).wait_recv()
        self.copy(self.left, self.core, 0, 2, self.to_right).start()
        self.copy(self.right, self.core, 1, 1, self.to_left).wait_recv()
        self.copy(self.right, self.core, 1, 3, self.to_left).start()

    def forward_rest(self):
        self.copy(self.left, self.core, 1, 8, self.to_right).wait_recv()
        self.copy(self.left, self.core, None, 5, self.partner).start()
        self.copy(self.right, self.core, 0, 9, self.to_left).wait_recv()
        self.copy(self.right, self.core, None, 6, self.partner).start()

    def forward_far(self):
        self.copy(self.far, self.core, 0, 2, self.to_right).wait_recv()
        self.copy(self.far, self.core, 1, 3, self.to_left).wait_recv()
        self.copy(self.far, self.core, None, 7, self.partner).start()

    def take(self, which):
        index, plane = self.crossing[which]
        self.copy(plane, 1 - self.core, None, index, self.partner).wait_recv()
        return plane

    def sent(self):
        self.copy(self.z, self.core, 0, 0, self.to_right).wait_send()
        self.copy(self.z, self.core, 1, 1, self.to_left).wait_send()
        self.copy(self.z, self.core, 1, 8, self.to_right).wait_send()
        self.copy(self.z, self.core, 0, 9, self.to_left).wait_send()
        self.copy(self.left, self.core, 0, 2, self.to_right).wait_send()
        self.copy(self.right, self.core, 1, 3, self.to_left).wait_send()
        for index, plane in self.crossing:
            self.copy(plane, self.core, None, index, self.partner).wait_send()


def kernel(
    leaf_ref,
    matrix_ref,
    shift_mid_ref,
    trans_top_ref,
    trans_mid_ref,
    interp_top_ref,
    shift_top_ref,
    list_mid_ref,
    offset_mid_ref,
    list_top_ref,
    offset_top_ref,
    out_ref,
    leaf,
    weights,
    shift_mid,
    trans_top,
    trans_mid,
    interp_top,
    shift_top,
    lists_mid,
    lists_top,
    scaled_mid,
    scaled_top,
    near,
    list_ts,
    offset_ts,
    p_all,
    tp_all,
    t_all,
    leaf_rows,
    cos_mid,
    sin_mid,
    sending,
    stage,
    piece,
    block_f32,
    top_lhs,
    top_f32,
    cos_top,
    sin_top,
    p_tab,
    t_tab,
    p_top,
    t_top,
    mid_sum,
    top_sum,
    child_rows,
    down,
    pieces,
    received,
    children,
    total,
    weight_sem,
    load_sem,
    index_sem,
    near_sem,
    a2a_send,
    a2a_recv,
    swap_sem,
    share_send,
    share_recv,
    t_send,
    t_recv,
    p_send,
    p_recv,
    tp_send,
    tp_recv,
    back_send,
    back_recv,
):
    z, sector, core = place()
    entries = list_mid_ref.shape[0]
    low = sector % 2
    own = low == core
    partner = device_of(z, sector, 1 - core)
    swap = device_of(z, sector - low + core, low)
    right = device_of((z + 1) % PLANES, sector, core)
    left = device_of((z + PLANES - 1) % PLANES, sector, core)
    t_spread = Spread(t_all, t_send, t_recv)
    p_spread = Spread(p_all, p_send, p_recv)
    tp_spread = Spread(tp_all, tp_send, tp_recv)

    group = sector // 4
    inside = sector % 4

    def apart(a, k):
        high = (a // 2 + k + 1) % 2
        return high * 2 + (a % 2 + 1 + k // 2) % 2

    def nth(k):
        return apart(group, k // 4) * 4 + apart(inside, k % 4)

    def other(k):
        return (sector + 1 + k) % SECTORS

    def to_sector(s):
        return device_of(z, s, core)

    barrier = pltpu.get_barrier_semaphore()

    def signal_peer(k, carry):
        pl.semaphore_signal(barrier, inc=1, device_id=to_sector(other(k)), device_id_type=MESH)
        return carry

    lax.fori_loop(0, SECTORS - 1, signal_peer, 0)
    for device in (right, left, partner):
        pl.semaphore_signal(barrier, inc=1, device_id=device, device_id_type=MESH)

    @pl.when(jnp.logical_not(own))
    def _():
        pl.semaphore_signal(barrier, inc=1, device_id=swap, device_id_type=MESH)

    slab = pl.ds(pl.multiple_of(z * 256, 256), 256)
    loads = [
        pltpu.make_async_copy(source, target, load_sem.at[index])
        for index, (source, target) in enumerate(
            (
                (leaf_ref, leaf),
                (trans_top_ref, trans_top),
                (shift_mid_ref, shift_mid),
                (list_mid_ref.at[:, slab], lists_mid.at[0]),
                (offset_mid_ref.at[:, slab], lists_mid.at[1]),
                (list_top_ref, lists_top.at[0]),
                (offset_top_ref, lists_top.at[1]),
            )
        )
    ]
    for copy in loads[:3]:
        copy.start()

    def weight_copy(piece_at):
        columns = pl.ds(pl.multiple_of(apart(group, piece_at) * 1024, 1024), 1024)
        return pltpu.make_async_copy(matrix_ref.at[:, columns], weights.at[:, columns], weight_sem.at[piece_at])

    for piece_at in range(4):
        weight_copy(piece_at).start()
    for copy in loads[3:]:
        copy.start()

    loads[0].wait()
    rows = 2 * leaf.shape[1]
    target = lax.broadcasted_iota(jnp.int32, (rows, rows), 0)
    source = lax.broadcasted_iota(jnp.int32, (rows, rows), 1)
    wanted = (target & 64) + ((target & 7) << 3) + ((target >> 3) & 7)
    order = (source == wanted).astype(BF16)
    both = jnp.concatenate([leaf[0], leaf[1]], axis=0)
    leaf_rows[...] = jnp.dot(order, both, preferred_element_type=F32).astype(BF16)

    loads[1].wait()
    used = trans_top.shape[0]
    piece[0:used, :] = trans_top[...].astype(BF16)
    piece[used:, :] = jnp.zeros((piece.shape[0] - used, LANES), BF16)

    swap_copy = pltpu.make_async_remote_copy(
        src_ref=piece,
        dst_ref=t_all.at[z, low],
        send_sem=swap_sem.at[0],
        recv_sem=swap_sem.at[1],
        device_id=swap,
        device_id_type=MESH,
    )
    shared = ((trans_mid_ref, trans_mid), (interp_top_ref, interp_top), (shift_top_ref, shift_top))

    def share_copy(index):
        return pltpu.make_async_remote_copy(
            src_ref=shared[index][0],
            dst_ref=shared[index][1],
            send_sem=share_send.at[index],
            recv_sem=share_recv.at[index],
            device_id=partner,
            device_id_type=MESH,
        )

    def local_copy(index):
        return pltpu.make_async_copy(shared[index][0], shared[index][1], share_recv.at[index])

    loads[2].wait()
    sines, cosines = sin_cos(shift_mid[...])
    cos_mid[...] = cosines
    sin_mid[...] = sines

    def parents(s, slot):
        columns = pl.ds(pl.multiple_of(s * 256, 256), 256)
        spread = jnp.dot(leaf_rows[...], weights[:, columns], preferred_element_type=F32)
        real_sum = jnp.zeros((8, 256), F32)
        imag_sum = jnp.zeros((8, 256), F32)
        for child in range(8):
            real = spread[child * 8 : child * 8 + 8]
            imag = spread[64 + child * 8 : 64 + child * 8 + 8]
            c = cos_mid[child : child + 1, columns]
            n = sin_mid[child : child + 1, columns]
            real_sum += real * c - imag * n
            imag_sum += real * n + imag * c
        for part in range(2):
            lanes = slice(part * LANES, part * LANES + LANES)
            stage[pl.ds(slot * 32 + part, 8, stride=4), :] = real_sum[:, lanes]
            stage[pl.ds(slot * 32 + 2 + part, 8, stride=4), :] = imag_sum[:, lanes]
        return stage[slot * 32 : slot * 32 + 32, :].astype(BF16)

    def rows_of(s):
        return p_all.at[z, core, pl.ds(pl.multiple_of(s * 32, 32), 32)]

    def a2a_copy(s, landing):
        return pltpu.make_async_remote_copy(
            src_ref=sending.at[s],
            dst_ref=rows_of(landing),
            send_sem=a2a_send.at[s],
            recv_sem=a2a_recv.at[landing],
            device_id=to_sector(s),
            device_id_type=MESH,
        )

    def make_four(piece_at):
        weight_copy(piece_at).wait()
        for slot in range(4):
            s = nth(piece_at * 4 + slot)
            sending[s] = parents(s, slot)

    def start_four(piece_at):
        for slot in range(4):
            a2a_copy(nth(piece_at * 4 + slot), sector).start()

    make_four(0)
    pl.semaphore_wait(barrier, SECTORS - 1 + 3 + (low + core) % 2)

    @pl.when(own)
    def _():
        for index in range(3):
            share_copy(index).start()
            local_copy(index).start()
        t_all[z, core] = piece[...]
        t_spread.start_own()

    @pl.when(jnp.logical_not(own))
    def _():
        swap_copy.start()

    start_four(0)

    def send_four(piece_at, carry):
        make_four(piece_at)
        start_four(piece_at)
        return carry

    lax.fori_loop(1, 3, send_four, 0)
    weight_copy(3).wait()
    for slot in range(3):
        s = nth(12 + slot)
        sending[s] = parents(s, slot)
        a2a_copy(s, sector).start()
    p_all[z, core, pl.ds(pl.multiple_of(sector * 32, 32), 32), :] = parents(sector, 3)

    total[...] = jnp.zeros_like(total)

    for copy in loads[3:]:
        copy.wait()
    scaled = jnp.transpose(jnp.concatenate([lists_mid[0], lists_mid[1]], axis=0) * 8)
    for quad_at in range(64):
        scaled_mid[quad_at] = scaled[quad_at * 4 : quad_at * 4 + 4]
    scaled = jnp.transpose(jnp.concatenate([lists_top[0] * 16, lists_top[1] * 8], axis=0))
    scaled_top[0] = scaled[:, :entries]
    scaled_top[1] = scaled[:, entries:]
    to_smem = [
        pltpu.make_async_copy(scaled_top.at[0], list_ts, index_sem.at[0]),
        pltpu.make_async_copy(scaled_top.at[1], offset_ts, index_sem.at[1]),
    ]
    for copy in to_smem:
        copy.start()

    def fetch(k, slot):
        s = nth(k)
        odd = s % 2
        quad_at = odd * 32 + (s - odd + core) * 2 + slot % 2
        return pltpu.make_async_copy(scaled_mid.at[quad_at], near.at[slot], near_sem.at[slot])

    for slot in range(4):
        fetch(slot // 2, slot).start()

    @pl.when(own)
    def _():
        for index in range(3):
            local_copy(index).wait()

    @pl.when(jnp.logical_not(own))
    def _():
        for index in range(3):
            share_copy(index).wait_recv()

    offsets = trans_mid.shape[0] // 4

    def put_offsets(first, row):
        for quarter, places in enumerate(((0, 2), (4, 6), (1, 3), (5, 7))):
            v = trans_mid[pl.ds(first + quarter, 8, stride=4), :]
            for at in places:
                t_tab[pl.ds(row + at, 8, stride=8), :] = v

    def mid_offsets(k, carry):
        put_offsets(pl.multiple_of(k * 32, 32), pl.multiple_of(k * 64, 64))
        return carry

    lax.fori_loop(0, offsets // 8, mid_offsets, 0)
    if offsets % 8:
        put_offsets((offsets - 8) * 4, (offsets - 8) * 8)

    sines_t, cosines_t = sin_cos(shift_top[...])
    cos_top[...] = cosines_t
    sin_top[...] = sines_t

    def wait_sector(k, carry):
        s = other(k)
        a2a_copy(s, s).wait_recv()
        return carry

    lax.fori_loop(0, SECTORS - 1, wait_sector, 0)
    p_spread.start_own()

    block_f32[...] = p_all[z, core].astype(F32)
    for child in range(8):
        for part in range(2):
            for side in range(2):
                first = child * 4 + part * 2 + side
                a = block_f32[pl.ds(first, 8, stride=32), :]
                b = block_f32[pl.ds(256 + first, 8, stride=32), :]
                top_lhs[
                    part * 128 + child * 16 : part * 128 + child * 16 + 16, side * LANES : side * LANES + LANES
                ] = jnp.concatenate([a, b], axis=0).astype(BF16)

    def top_columns(k, carry):
        columns = pl.ds(pl.multiple_of(k * 256, 256), 256)
        spread = jnp.dot(top_lhs[...], interp_top[:, columns], preferred_element_type=F32)
        for part in range(2):
            lanes = slice(part * LANES, part * LANES + LANES)
            group = k * 2 + part
            real_sum = jnp.zeros((16, LANES), F32)
            imag_sum = jnp.zeros((16, LANES), F32)
            for child in range(8):
                real = spread[child * 16 : child * 16 + 16, lanes]
                imag = spread[128 + child * 16 : 128 + child * 16 + 16, lanes]
                c = cos_top[pl.ds(child * 8 + group, 1), :]
                n = sin_top[pl.ds(child * 8 + group, 1), :]
                real_sum += real * c - imag * n
                imag_sum += real * n + imag * c
            for half in range(2):
                boxes = slice(half * 8, half * 8 + 8)
                top_f32[pl.ds(half * 128 + group, 8, stride=16), :] = real_sum[boxes]
                top_f32[pl.ds(half * 128 + 8 + group, 8, stride=16), :] = imag_sum[boxes]
        return carry

    lax.fori_loop(0, 4, top_columns, 0)
    tp_all[z, core] = top_f32[...].astype(BF16)

    upper = lax.broadcasted_iota(jnp.int32, (8, LANES), 0) < 4

    def mid_table(plane, side):
        def four(k, carry):
            for part in range(4):
                odd = part % 2
                found = p_all[plane, side, pl.ds(pl.multiple_of(k * 128 + part * 32, 32), 32), :].astype(F32)
                first = ((2 * plane + odd) * 128 + (k * 4 + part - odd + side) * 8) * 8
                for pair in range(4):
                    v = found[pair * 8 : pair * 8 + 8]
                    r = pltpu.roll(v, 4, 0)
                    at = first + pair * 16
                    p_tab[pl.ds(pl.multiple_of(at, 8), 8), :] = jnp.where(upper, v, r)
                    p_tab[pl.ds(pl.multiple_of(at + 8, 8), 8), :] = jnp.where(upper, r, v)
            return carry

        lax.fori_loop(0, SECTORS // 4, four, 0)

    def top_table(plane, side):
        def four(k, carry):
            for part in range(4):
                odd = part % 2
                found = tp_all[plane, side, pl.ds(pl.multiple_of(k * 64 + part * 16, 16), 16), :].astype(F32)
                first = ((2 * plane + odd) * 16 + (k * 4 + part - odd + side)) * 16
                p_top[pl.ds(pl.multiple_of(first, 16), 16), :] = found
            return carry

        lax.fori_loop(0, SECTORS // 4, four, 0)

    mid_table(z, core)
    top_table(z, core)
    p_spread.forward()
    tp_spread.start_own()
    p_spread.forward_rest()

    @pl.when(jnp.logical_not(own))
    def _():
        swap_copy.wait()
        t_spread.start_own()

    mid_table(p_spread.left, core)
    mid_table(p_spread.right, core)
    mid_table(p_spread.take(0), 1 - core)
    for copy in to_smem:
        copy.wait()
    p_spread.forward_far()
    mid_table(p_spread.far, core)
    mid_table(p_spread.take(1), 1 - core)
    mid_table(p_spread.take(2), 1 - core)
    mid_table(p_spread.take(3), 1 - core)

    def middle(k, parity, more=True, beside=None):
        for half in range(2):
            slot = parity * 2 + half
            fetch(k, slot).wait()
            for i in range(4):
                box = half * 4 + i
                kept = jnp.zeros((8, LANES), F32)
                for j in range(entries):
                    p = p_tab[pl.ds(near[slot, i, j], 8), :]
                    t = t_tab[pl.ds(near[slot, i, entries + j], 8), :]
                    kept = kept + p * t
                mid_sum[pl.ds(pl.multiple_of(k * 64 + box * 8, 8), 8), :] = kept
                if beside is not None:
                    beside(box)
            if more:
                fetch(k + 2, slot).start()

    def offset_part(plane, side, i):
        at = plane * 2 + side
        for part in range(t_all.shape[2] // 128):
            row = i * (t_all.shape[2] // 8) + part * 16
            found = t_all[plane, side, row : row + 16, :].astype(F32)
            for half in range(2):
                t_top[pl.ds(row * 8 + half * 64 + at, 8, stride=8), :] = found[half * 8 : half * 8 + 8]

    def top_part(plane, side, i):
        for odd in range(2):
            found = tp_all[plane, side, i * 32 + odd * 16 : i * 32 + odd * 16 + 16, :].astype(F32)
            first = ((2 * plane + odd) * 16 + (i * 2 + side)) * 16
            p_top[pl.ds(pl.multiple_of(first, 16), 16), :] = found

    ahead = 10
    z_left, z_right, z_far = t_spread.left, t_spread.right, t_spread.far
    away = 1 - core
    middle(0, 0)
    middle(1, 1)
    tp_spread.forward()
    t_spread.forward()
    tp_spread.forward_rest()
    t_spread.forward_rest()

    def tables2(i):
        offset_part(z, core, i)
        offset_part(z_left, core, i)
        top_part(z_left, core, i)

    middle(2, 0, True, tables2)
    t_spread.take(0)
    tp_spread.take(0)

    def tables3(i):
        offset_part(z_right, core, i)
        offset_part(z, away, i)
        top_part(z_right, core, i)
        top_part(z, away, i)

    middle(3, 1, True, tables3)
    t_spread.take(1)
    t_spread.take(2)
    tp_spread.take(1)
    tp_spread.take(2)

    def tables4(i):
        offset_part(z_left, away, i)
        offset_part(z_right, away, i)
        top_part(z_left, away, i)
        top_part(z_right, away, i)

    middle(4, 0, True, tables4)
    middle(5, 1)
    middle(6, 0)
    tp_spread.forward_far()
    t_spread.forward_far()

    def tables7(i):
        offset_part(z_far, core, i)
        top_part(z_far, core, i)

    middle(7, 1, True, tables7)
    middle(8, 0)
    t_spread.take(3)
    tp_spread.take(3)

    def tables9(i):
        offset_part(z_far, away, i)
        top_part(z_far, away, i)

    middle(9, 1, True, tables9)

    behind = (trans_top_ref.shape[0] // 2) * 8

    def top_box(k, carry):
        odd = k % 2
        column = (2 * z + odd) * 16 + (k - odd + core)
        sums = [jnp.zeros((8, LANES), F32) for _ in range(4)]
        for j in range(entries):
            n = list_ts[column, j]
            o = offset_ts[column, j]
            pr = p_top[pl.ds(n, 8), :]
            pi = p_top[pl.ds(n + 8, 8), :]
            tr = t_top[pl.ds(o, 8), :]
            ti = t_top[pl.ds(o + behind, 8), :]
            sums = [sums[0] + pr * tr, sums[1] + pi * ti, sums[2] + pr * ti, sums[3] + pi * tr]
        real = (sums[0] - sums[1]).astype(BF16).astype(F32)
        imag = (sums[2] + sums[3]).astype(BF16).astype(F32)
        top_sum[pl.ds(pl.multiple_of(k * 16, 16), 8), :] = real
        top_sum[pl.ds(pl.multiple_of(k * 16 + 8, 8), 8), :] = imag
        return carry

    lax.fori_loop(0, SECTORS, top_box, 0)

    def top_children(part, carry):
        lanes = pl.ds(pl.multiple_of(part * LANES, LANES), LANES)
        c = cos_top[pl.ds(part, 8, stride=8), :]
        n = sin_top[pl.ds(part, 8, stride=8), :]
        for pair in range(8):
            reals = []
            imags = []
            for half in range(2):
                first = pair * 32 + half * 16
                real = jnp.broadcast_to(top_sum[pl.ds(first + part, 1), :], (8, LANES))
                imag = jnp.broadcast_to(top_sum[pl.ds(first + 8 + part, 1), :], (8, LANES))
                reals.append(real * c + imag * n)
                imags.append(imag * c - real * n)
            child_rows[pair * 16 : pair * 16 + 16, lanes] = jnp.concatenate(reals, axis=0).astype(BF16)
            child_rows[128 + pair * 16 : 144 + pair * 16, lanes] = jnp.concatenate(imags, axis=0).astype(BF16)
        return carry

    lax.fori_loop(0, 8, top_children, 0)
    scale = interp_top.shape[0] / interp_top.shape[1]
    down[...] = scale * lax.dot_general(
        child_rows[...], interp_top[...], (((1,), (1,)), ((), ())), preferred_element_type=F32
    )

    def back_copy(s, landing):
        return pltpu.make_async_remote_copy(
            src_ref=pieces.at[s],
            dst_ref=received.at[landing],
            send_sem=back_send.at[s],
            recv_sem=back_recv.at[landing],
            device_id=to_sector(s),
            device_id_type=MESH,
        )

    def combine(n):
        k = nth(n)
        at = pl.multiple_of(k * 8, 8)
        sides = []
        for side in range(2):
            lanes = slice(side * LANES, side * LANES + LANES)
            parts = [mid_sum[pl.ds(n * 64 + side + 2 * quarter, 8, stride=8), :] for quarter in range(4)]
            real = (parts[0] - parts[3]) + down[pl.ds(at, 8), lanes]
            imag = (parts[1] + parts[2]) + down[pl.ds(pl.multiple_of(128 + k * 8, 8), 8), lanes]
            sides.append(jnp.concatenate([real, imag], axis=0).astype(BF16))
        return jnp.concatenate(sides, axis=1)

    def make_children(s, at):
        columns = pl.ds(pl.multiple_of(s * 256, 256), 256)
        c = cos_mid[:, columns]
        n = sin_mid[:, columns]
        found = received[s].astype(F32)
        target = pl.ds(pl.multiple_of(at * 256, 256), 256)
        for pair in range(4):
            reals = []
            imags = []
            for half in range(2):
                box = pair * 2 + half
                real = jnp.broadcast_to(found[box : box + 1], (8, 256))
                imag = jnp.broadcast_to(found[8 + box : 9 + box], (8, 256))
                reals.append(real * c + imag * n)
                imags.append(imag * c - real * n)
            children[pair * 16 : pair * 16 + 16, target] = jnp.concatenate(reals, axis=0).astype(BF16)
            children[64 + pair * 16 : 80 + pair * 16, target] = jnp.concatenate(imags, axis=0).astype(BF16)

    def take_piece(piece_at, count):
        at = apart(group, piece_at)
        for slot in range(count):
            s = at * 4 + apart(inside, slot)
            back_copy(s, s).wait_recv()
        for slot in range(4):
            make_children(at * 4 + slot, slot)

    block = 512

    def product(at, k):
        columns = pl.ds(pl.multiple_of(at * 1024, 1024), 1024)
        rows_at = pl.ds(k * block, block)
        return lax.dot_general(
            weights[rows_at, columns], children[...], (((1,), (1,)), ((), ())), preferred_element_type=F32
        )

    def finish_piece(piece_at, carry):
        take_piece(piece_at, 4)
        for k in range(total.shape[0] // block):
            total[k * block : k * block + block, :] += product(apart(group, piece_at), k)
        return carry

    def send_back(k, carry):
        s = nth(k)
        pieces[s] = combine(k)
        back_copy(s, sector).start()
        return carry

    def pair_and_send(pair_at, carry):
        for parity in range(2):
            middle(pair_at * 2 + parity, parity)
            send_back(pair_at * 2 + parity, carry)
        return carry

    lax.fori_loop(0, ahead, send_back, 0)
    lax.fori_loop(ahead // 2, SECTORS // 2 - 1, pair_and_send, 0)
    middle(SECTORS - 2, 0, False)
    send_back(SECTORS - 2, 0)
    middle(SECTORS - 1, 1, False)
    received[sector] = combine(SECTORS - 1)
    lax.fori_loop(0, 3, finish_piece, 0)
    take_piece(3, 3)
    half_rows = out_ref.shape[1]
    for k in range(total.shape[0] // block):
        part = product(group, k)
        for n in range(k * block // 256, (k + 1) * block // 256):
            rows_at = slice(n * 256, n * 256 + 256)
            turned = jnp.transpose(total[rows_at, :] + part[n * 256 - k * block : n * 256 - k * block + 256])
            for which in range(2):
                out_ref[which, :, rows_at] = turned[which * half_rows : which * half_rows + half_rows]

    def wait_sent(k, carry):
        s = other(k)
        a2a_copy(s, sector).wait_send()
        back_copy(s, sector).wait_send()
        return carry

    lax.fori_loop(0, SECTORS - 1, wait_sent, 0)

    @pl.when(own)
    def _():
        for index in range(3):
            share_copy(index).wait_send()

    for each in (t_spread, p_spread, tp_spread):
        each.sent()


def on_device(
    leaf_out,
    interp_mid,
    shift_mid,
    trans_mid,
    list_mid,
    offset_mid,
    interp_top,
    shift_top,
    trans_top,
    list_top,
    offset_top,
):
    offsets = trans_mid.shape[1]
    entries = list_mid.shape[1]
    rows = 2 * leaf_out.shape[1]
    operands = (
        leaf_out,
        interp_mid,
        shift_mid,
        trans_top.reshape(2 * offsets, LANES),
        jnp.transpose(trans_mid.reshape(2, offsets, 2, LANES), (1, 2, 0, 3)).reshape(4 * offsets, LANES),
        interp_top[0],
        shift_top.reshape(64, LANES),
        list_mid.T,
        offset_mid.T,
        list_top.T,
        offset_top.T,
    )
    padded = 640
    result = pl.pallas_call(
        kernel,
        out_shape=VMEM(leaf_out.shape, F32),
        in_specs=[pl.BlockSpec(memory_space=pltpu.HBM)] * len(operands),
        out_specs=pl.BlockSpec(memory_space=VMEM),
        scratch_shapes=[
            VMEM(leaf_out.shape, BF16),
            VMEM(interp_mid.shape, BF16),
            VMEM(shift_mid.shape, F32),
            VMEM((2 * offsets, LANES), F32),
            VMEM((4 * offsets, LANES), F32),
            VMEM((256, 1024), BF16),
            VMEM((64, LANES), F32),
            VMEM((2, entries, 256), jnp.int32),
            VMEM((2, entries, 128), jnp.int32),
            VMEM((64, 4, 2 * entries), jnp.int32),
            VMEM((2, 128, entries), jnp.int32),
            pltpu.SMEM((4, 4, 2 * entries), jnp.int32),
            pltpu.SMEM((128, entries), jnp.int32),
            pltpu.SMEM((128, entries), jnp.int32),
            VMEM((PLANES, 2, 512, LANES), BF16),
            VMEM((PLANES, 2, 256, LANES), BF16),
            VMEM((PLANES, 2, padded, LANES), BF16),
            VMEM((rows, interp_mid.shape[0]), BF16),
            VMEM(shift_mid.shape, F32),
            VMEM(shift_mid.shape, F32),
            VMEM((SECTORS, 32, LANES), BF16),
            VMEM((128, LANES), F32),
            VMEM((padded, LANES), BF16),
            VMEM((512, LANES), F32),
            VMEM((256, 256), BF16),
            VMEM((256, LANES), F32),
            VMEM((64, LANES), F32),
            VMEM((64, LANES), F32),
            VMEM((1024 * 8, LANES), F32),
            VMEM((offsets * 8, LANES), F32),
            VMEM((128 * 16, LANES), F32),
            VMEM((padded * 8, LANES), F32),
            VMEM((128 * 8, LANES), F32),
            VMEM((16 * 16, LANES), F32),
            VMEM((256, 1024), BF16),
            VMEM((256, 256), F32),
            VMEM((SECTORS, 16, 256), BF16),
            VMEM((SECTORS, 16, 256), BF16),
            VMEM((rows, 1024), BF16),
            VMEM((interp_mid.shape[0], rows), F32),
            DMA((4,)),
            DMA((7,)),
            DMA((2,)),
            DMA((4,)),
            DMA((SECTORS,)),
            DMA((SECTORS,)),
            DMA((2,)),
            DMA((3,)),
            DMA((3,)),
            DMA((10,)),
            DMA((10,)),
            DMA((10,)),
            DMA((10,)),
            DMA((10,)),
            DMA((10,)),
            DMA((SECTORS,)),
            DMA((SECTORS,)),
        ],
        compiler_params=pltpu.CompilerParams(
            collective_id=0, has_side_effects=True, vmem_limit_bytes=60 * 1024 * 1024
        ),
        name="far_field",
    )(*operands)
    return result * (interp_mid.shape[0] / interp_mid.shape[1])


def solution(mesh):
    return jax.shard_map(
        on_device,
        mesh=mesh,
        in_specs=(
            P(None, ("box", "dir"), None),
            P(),
            P(),
            P(None, None, "dir"),
            P(),
            P(),
            P("dir", None, None),
            P(None, "dir", None),
            P(None, None, "dir", "box"),
            P(),
            P(),
        ),
        out_specs=P(None, ("box", "dir"), None),
        check_vma=False,
    )
```

```python
import jax
import jax.numpy as jnp
from jax import lax
from jax.experimental import pallas as pl
from jax.experimental.pallas import tpu as pltpu
from jax.sharding import PartitionSpec as P

MESH = pl.DeviceIdType.MESH
F32 = jnp.float32
BF16 = jnp.bfloat16
VMEM = pltpu.VMEM
DMA = pltpu.SemaphoreType.DMA
PLANES = 4
SECTORS = 16
LANES = 128


def place():
    box = lax.axis_index("box")
    way = lax.axis_index("dir")
    low = box % 2
    core = way % 2
    return box // 2, way - core + low, core


def device_of(plane, sector, core):
    low = sector % 2
    return (plane * 2 + low, sector - low + core)


def sin_cos(angle):
    half = angle * 0.5
    sq = half * half
    s = sq * (-1.0 / 39916800.0) + (1.0 / 362880.0)
    s = sq * s - (1.0 / 5040.0)
    s = sq * s + (1.0 / 120.0)
    s = sq * s - (1.0 / 6.0)
    s = half + half * (sq * s)
    c = sq * (1.0 / 479001600.0) - (1.0 / 3628800.0)
    c = sq * c + (1.0 / 40320.0)
    c = sq * c - (1.0 / 720.0)
    c = sq * c + (1.0 / 24.0)
    c = sq * c - 0.5
    c = sq * c + 1.0
    return 2.0 * s * c, 1.0 - 2.0 * s * s


class Spread:
    def __init__(self, ref, send, recv):
        z, sector, core = place()
        self.ref, self.send, self.recv = ref, send, recv
        self.core = core
        self.z = z
        self.left = (z + PLANES - 1) % PLANES
        self.right = (z + 1) % PLANES
        self.far = (z + 2) % PLANES
        self.to_right = device_of(self.right, sector, core)
        self.to_left = device_of(self.left, sector, core)
        self.partner = device_of(z, sector, 1 - core)
        self.rows = ref.shape[2]
        self.crossing = ((4, self.z), (5, self.left), (6, self.right), (7, self.far))

    def copy(self, plane, core, half, index, target):
        rows = self.rows
        if half is None:
            part = self.ref.at[plane, core]
        else:
            part = self.ref.at[plane, core, pl.ds(half * (rows // 2), rows // 2)]
        return pltpu.make_async_remote_copy(
            src_ref=part,
            dst_ref=part,
            send_sem=self.send.at[index],
            recv_sem=self.recv.at[index],
            device_id=target,
            device_id_type=MESH,
        )

    def start_own(self):
        self.copy(self.z, self.core, 0, 0, self.to_right).start()
        self.copy(self.z, self.core, 1, 1, self.to_left).start()
        self.copy(self.z, self.core, 1, 8, self.to_right).start()
        self.copy(self.z, self.core, 0, 9, self.to_left).start()
        self.copy(self.z, self.core, None, 4, self.partner).start()

    def forward(self):
        self.copy(self.left, self.core, 0, 0, self.to_right).wait_recv()
        self.copy(self.left, self.core, 0, 2, self.to_right).start()
        self.copy(self.right, self.core, 1, 1, self.to_left).wait_recv()
        self.copy(self.right, self.core, 1, 3, self.to_left).start()

    def forward_rest(self):
        self.copy(self.left, self.core, 1, 8, self.to_right).wait_recv()
        self.copy(self.left, self.core, None, 5, self.partner).start()
        self.copy(self.right, self.core, 0, 9, self.to_left).wait_recv()
        self.copy(self.right, self.core, None, 6, self.partner).start()

    def forward_far(self):
        self.copy(self.far, self.core, 0, 2, self.to_right).wait_recv()
        self.copy(self.far, self.core, 1, 3, self.to_left).wait_recv()
        self.copy(self.far, self.core, None, 7, self.partner).start()

    def take(self, which):
        index, plane = self.crossing[which]
        self.copy(plane, 1 - self.core, None, index, self.partner).wait_recv()
        return plane

    def sent(self):
        self.copy(self.z, self.core, 0, 0, self.to_right).wait_send()
        self.copy(self.z, self.core, 1, 1, self.to_left).wait_send()
        self.copy(self.z, self.core, 1, 8, self.to_right).wait_send()
        self.copy(self.z, self.core, 0, 9, self.to_left).wait_send()
        self.copy(self.left, self.core, 0, 2, self.to_right).wait_send()
        self.copy(self.right, self.core, 1, 3, self.to_left).wait_send()
        for index, plane in self.crossing:
            self.copy(plane, self.core, None, index, self.partner).wait_send()


def kernel(
    leaf_ref,
    matrix_ref,
    shift_mid_ref,
    trans_top_ref,
    trans_mid_ref,
    interp_top_ref,
    shift_top_ref,
    list_mid_ref,
    offset_mid_ref,
    list_top_ref,
    offset_top_ref,
    out_ref,
    leaf,
    weights,
    shift_mid,
    trans_top,
    trans_mid,
    interp_top,
    shift_top,
    lists_mid,
    lists_top,
    scaled_mid,
    scaled_top,
    near,
    own_top,
    near_top,
    p_all,
    tp_all,
    t_all,
    leaf_rows,
    cos_mid,
    sin_mid,
    sending,
    stage,
    piece,
    block_f32,
    top_lhs,
    top_f32,
    cos_top,
    sin_top,
    p_tab,
    t_tab,
    p_top,
    t_top,
    mid_sum,
    top_sum,
    child_rows,
    down,
    pieces,
    received,
    children,
    total,
    weight_sem,
    load_sem,
    index_sem,
    near_sem,
    a2a_send,
    a2a_recv,
    swap_sem,
    share_send,
    share_recv,
    t_send,
    t_recv,
    p_send,
    p_recv,
    tp_send,
    tp_recv,
    back_send,
    back_recv,
):
    z, sector, core = place()
    entries = list_mid_ref.shape[0]
    low = sector % 2
    own = low == core
    partner = device_of(z, sector, 1 - core)
    swap = device_of(z, sector - low + core, low)
    right = device_of((z + 1) % PLANES, sector, core)
    left = device_of((z + PLANES - 1) % PLANES, sector, core)
    t_spread = Spread(t_all, t_send, t_recv)
    p_spread = Spread(p_all, p_send, p_recv)
    tp_spread = Spread(tp_all, tp_send, tp_recv)

    group = sector // 4
    inside = sector % 4

    def apart(a, k):
        high = (a // 2 + k + 1) % 2
        return high * 2 + (a % 2 + 1 + k // 2) % 2

    def nth(k):
        return apart(group, k // 4) * 4 + apart(inside, k % 4)

    def other(k):
        return (sector + 1 + k) % SECTORS

    def to_sector(s):
        return device_of(z, s, core)

    barrier = pltpu.get_barrier_semaphore()

    def signal_peer(k, carry):
        pl.semaphore_signal(barrier, inc=1, device_id=to_sector(other(k)), device_id_type=MESH)
        return carry

    lax.fori_loop(0, SECTORS - 1, signal_peer, 0)
    for device in (right, left, partner):
        pl.semaphore_signal(barrier, inc=1, device_id=device, device_id_type=MESH)

    @pl.when(jnp.logical_not(own))
    def _():
        pl.semaphore_signal(barrier, inc=1, device_id=swap, device_id_type=MESH)

    slab = pl.ds(pl.multiple_of(z * 256, 256), 256)
    loads = [
        pltpu.make_async_copy(source, target, load_sem.at[index])
        for index, (source, target) in enumerate(
            (
                (leaf_ref, leaf),
                (trans_top_ref, trans_top),
                (shift_mid_ref, shift_mid),
                (list_mid_ref.at[:, slab], lists_mid.at[0]),
                (offset_mid_ref.at[:, slab], lists_mid.at[1]),
                (list_top_ref, lists_top.at[0]),
                (offset_top_ref, lists_top.at[1]),
            )
        )
    ]
    for copy in loads[:3]:
        copy.start()

    def weight_copies(piece_at):
        columns = pl.ds(pl.multiple_of(apart(group, piece_at) * 1024, 1024), 1024)
        size = matrix_ref.shape[0] // 4
        return [
            pltpu.make_async_copy(
                matrix_ref.at[part * size : part * size + size, columns],
                weights.at[part * size : part * size + size, columns],
                weight_sem.at[piece_at * 4 + part],
            )
            for part in range(4)
        ]

    for copy in weight_copies(0):
        copy.start()

    loads[0].wait()
    for copy in weight_copies(1):
        copy.start()
    rows = 2 * leaf.shape[1]
    target = lax.broadcasted_iota(jnp.int32, (rows, rows), 0)
    source = lax.broadcasted_iota(jnp.int32, (rows, rows), 1)
    wanted = (target & 64) + ((target & 7) << 3) + ((target >> 3) & 7)
    order = (source == wanted).astype(BF16)
    both = jnp.concatenate([leaf[0], leaf[1]], axis=0)
    leaf_rows[...] = jnp.dot(order, both, preferred_element_type=F32).astype(BF16)

    loads[1].wait()
    for piece_at in (2, 3):
        for copy in weight_copies(piece_at):
            copy.start()
    for copy in loads[3:]:
        copy.start()
    used = trans_top.shape[0]
    piece[0:used, :] = trans_top[...].astype(BF16)
    piece[used:, :] = jnp.zeros((piece.shape[0] - used, LANES), BF16)

    swap_copy = pltpu.make_async_remote_copy(
        src_ref=piece,
        dst_ref=t_all.at[z, low],
        send_sem=swap_sem.at[0],
        recv_sem=swap_sem.at[1],
        device_id=swap,
        device_id_type=MESH,
    )
    shared = ((trans_mid_ref, trans_mid), (interp_top_ref, interp_top), (shift_top_ref, shift_top))

    def share_copy(index):
        return pltpu.make_async_remote_copy(
            src_ref=shared[index][0],
            dst_ref=shared[index][1],
            send_sem=share_send.at[index],
            recv_sem=share_recv.at[index],
            device_id=partner,
            device_id_type=MESH,
        )

    def local_copy(index):
        return pltpu.make_async_copy(shared[index][0], shared[index][1], share_recv.at[index])

    loads[2].wait()
    sines, cosines = sin_cos(shift_mid[...])
    cos_mid[...] = cosines
    sin_mid[...] = sines

    def parents(s, slot):
        columns = pl.ds(pl.multiple_of(s * 256, 256), 256)
        spread = jnp.dot(leaf_rows[...], weights[:, columns], preferred_element_type=F32)
        real_sum = jnp.zeros((8, 256), F32)
        imag_sum = jnp.zeros((8, 256), F32)
        for child in range(8):
            real = spread[child * 8 : child * 8 + 8]
            imag = spread[64 + child * 8 : 64 + child * 8 + 8]
            c = cos_mid[child : child + 1, columns]
            n = sin_mid[child : child + 1, columns]
            real_sum += real * c - imag * n
            imag_sum += real * n + imag * c
        for part in range(2):
            lanes = slice(part * LANES, part * LANES + LANES)
            stage[pl.ds(slot * 32 + part, 8, stride=4), :] = real_sum[:, lanes]
            stage[pl.ds(slot * 32 + 2 + part, 8, stride=4), :] = imag_sum[:, lanes]
        return stage[slot * 32 : slot * 32 + 32, :].astype(BF16)

    def rows_of(s):
        return p_all.at[z, core, pl.ds(pl.multiple_of(s * 32, 32), 32)]

    def a2a_copy(s, landing):
        return pltpu.make_async_remote_copy(
            src_ref=sending.at[s],
            dst_ref=rows_of(landing),
            send_sem=a2a_send.at[s],
            recv_sem=a2a_recv.at[landing],
            device_id=to_sector(s),
            device_id_type=MESH,
        )

    def make_four(piece_at):
        for copy in weight_copies(piece_at):
            copy.wait()
        for slot in range(4):
            s = nth(piece_at * 4 + slot)
            sending[s] = parents(s, slot)

    def start_four(piece_at):
        for slot in range(4):
            a2a_copy(nth(piece_at * 4 + slot), sector).start()

    make_four(0)
    pl.semaphore_wait(barrier, SECTORS - 1 + 3 + (low + core) % 2)

    @pl.when(own)
    def _():
        for index in range(3):
            share_copy(index).start()
            local_copy(index).start()
        t_all[z, core] = piece[...]
        t_spread.start_own()

    @pl.when(jnp.logical_not(own))
    def _():
        swap_copy.start()

    start_four(0)

    def send_four(piece_at, carry):
        make_four(piece_at)
        start_four(piece_at)
        return carry

    lax.fori_loop(1, 3, send_four, 0)
    for copy in weight_copies(3):
        copy.wait()
    for slot in range(3):
        s = nth(12 + slot)
        sending[s] = parents(s, slot)
    p_all[z, core, pl.ds(pl.multiple_of(sector * 32, 32), 32), :] = parents(sector, 3)
    for slot in range(3):
        a2a_copy(nth(12 + slot), sector).start()

    total[...] = jnp.zeros_like(total)

    for copy in loads[3:]:
        copy.wait()
    scaled = jnp.transpose(jnp.concatenate([lists_mid[0], lists_mid[1]], axis=0) * 8)
    for quad_at in range(64):
        scaled_mid[quad_at] = scaled[quad_at * 4 : quad_at * 4 + 4]
    scaled = jnp.transpose(jnp.concatenate([lists_top[0] * 16, lists_top[1] * 8], axis=0))
    scaled_top[...] = scaled
    own_top[...] = scaled_top[pl.ds(z * 32 + core, 16, stride=2), :]
    to_smem = [pltpu.make_async_copy(own_top, near_top, index_sem.at[0])]
    for copy in to_smem:
        copy.start()

    def fetch(k, slot):
        s = nth(k)
        odd = s % 2
        quad_at = odd * 32 + (s - odd + core) * 2 + slot % 2
        return pltpu.make_async_copy(scaled_mid.at[quad_at], near.at[slot], near_sem.at[slot])

    for slot in range(4):
        fetch(slot // 2, slot).start()

    @pl.when(own)
    def _():
        for index in range(3):
            local_copy(index).wait()

    @pl.when(jnp.logical_not(own))
    def _():
        for index in range(3):
            share_copy(index).wait_recv()

    offsets = trans_mid.shape[0] // 4

    def put_offsets(first, row):
        for quarter, places in enumerate(((0, 2), (4, 6), (1, 3), (5, 7))):
            v = trans_mid[pl.ds(first + quarter, 8, stride=4), :]
            for at in places:
                t_tab[pl.ds(row + at, 8, stride=8), :] = v

    def mid_offsets(k, carry):
        put_offsets(pl.multiple_of(k * 32, 32), pl.multiple_of(k * 64, 64))
        return carry

    lax.fori_loop(0, offsets // 8, mid_offsets, 0)
    if offsets % 8:
        put_offsets((offsets - 8) * 4, (offsets - 8) * 8)

    sines_t, cosines_t = sin_cos(shift_top[...])
    cos_top[...] = cosines_t
    sin_top[...] = sines_t

    def wait_sector(k, carry):
        s = other(k)
        a2a_copy(s, s).wait_recv()
        return carry

    lax.fori_loop(0, SECTORS - 1, wait_sector, 0)
    p_spread.start_own()

    block_f32[...] = p_all[z, core].astype(F32)
    for child in range(8):
        for part in range(2):
            for side in range(2):
                first = child * 4 + part * 2 + side
                a = block_f32[pl.ds(first, 8, stride=32), :]
                b = block_f32[pl.ds(256 + first, 8, stride=32), :]
                top_lhs[
                    part * 128 + child * 16 : part * 128 + child * 16 + 16, side * LANES : side * LANES + LANES
                ] = jnp.concatenate([a, b], axis=0).astype(BF16)

    def top_columns(k, carry):
        columns = pl.ds(pl.multiple_of(k * 256, 256), 256)
        spread = jnp.dot(top_lhs[...], interp_top[:, columns], preferred_element_type=F32)
        for part in range(2):
            lanes = slice(part * LANES, part * LANES + LANES)
            group = k * 2 + part
            real_sum = jnp.zeros((16, LANES), F32)
            imag_sum = jnp.zeros((16, LANES), F32)
            for child in range(8):
                real = spread[child * 16 : child * 16 + 16, lanes]
                imag = spread[128 + child * 16 : 128 + child * 16 + 16, lanes]
                c = cos_top[pl.ds(child * 8 + group, 1), :]
                n = sin_top[pl.ds(child * 8 + group, 1), :]
                real_sum += real * c - imag * n
                imag_sum += real * n + imag * c
            for half in range(2):
                boxes = slice(half * 8, half * 8 + 8)
                top_f32[pl.ds(half * 128 + group, 8, stride=16), :] = real_sum[boxes]
                top_f32[pl.ds(half * 128 + 8 + group, 8, stride=16), :] = imag_sum[boxes]
        return carry

    lax.fori_loop(0, 4, top_columns, 0)
    tp_all[z, core] = top_f32[...].astype(BF16)

    upper = lax.broadcasted_iota(jnp.int32, (8, LANES), 0) < 4

    def mid_table(plane, side):
        def four(k, carry):
            for part in range(4):
                odd = part % 2
                found = p_all[plane, side, pl.ds(pl.multiple_of(k * 128 + part * 32, 32), 32), :].astype(F32)
                first = ((2 * plane + odd) * 128 + (k * 4 + part - odd + side) * 8) * 8
                for pair in range(4):
                    v = found[pair * 8 : pair * 8 + 8]
                    r = pltpu.roll(v, 4, 0)
                    at = first + pair * 16
                    p_tab[pl.ds(pl.multiple_of(at, 8), 8), :] = jnp.where(upper, v, r)
                    p_tab[pl.ds(pl.multiple_of(at + 8, 8), 8), :] = jnp.where(upper, r, v)
            return carry

        lax.fori_loop(0, SECTORS // 4, four, 0)

    def top_table(plane, side):
        def four(k, carry):
            for part in range(4):
                odd = part % 2
                found = tp_all[plane, side, pl.ds(pl.multiple_of(k * 64 + part * 16, 16), 16), :].astype(F32)
                first = ((2 * plane + odd) * 16 + (k * 4 + part - odd + side)) * 16
                p_top[pl.ds(pl.multiple_of(first, 16), 16), :] = found
            return carry

        lax.fori_loop(0, SECTORS // 4, four, 0)

    mid_table(z, core)
    top_table(z, core)
    p_spread.forward()
    tp_spread.start_own()

    @pl.when(jnp.logical_not(own))
    def _():
        swap_copy.wait()
        t_spread.start_own()

    p_spread.forward_rest()

    mid_table(p_spread.left, core)
    mid_table(p_spread.right, core)
    mid_table(p_spread.take(0), 1 - core)
    for copy in to_smem:
        copy.wait()
    p_spread.forward_far()
    mid_table(p_spread.far, core)
    mid_table(p_spread.take(1), 1 - core)
    mid_table(p_spread.take(2), 1 - core)
    mid_table(p_spread.take(3), 1 - core)

    def middle(k, parity, more=True, beside=None):
        for half in range(2):
            slot = parity * 2 + half
            fetch(k, slot).wait()
            for i in range(4):
                box = half * 4 + i
                kept = jnp.zeros((8, LANES), F32)
                for j in range(entries):
                    p = p_tab[pl.ds(near[slot, i, j], 8), :]
                    t = t_tab[pl.ds(near[slot, i, entries + j], 8), :]
                    kept = kept + p * t
                mid_sum[pl.ds(pl.multiple_of(k * 64 + box * 8, 8), 8), :] = kept
                if beside is not None:
                    beside(box)
            if more:
                fetch(k + 2, slot).start()

    def offset_part(plane, side, i):
        at = plane * 2 + side
        for part in range(t_all.shape[2] // 128):
            row = i * (t_all.shape[2] // 8) + part * 16
            found = t_all[plane, side, row : row + 16, :].astype(F32)
            for half in range(2):
                t_top[pl.ds(row * 8 + half * 64 + at, 8, stride=8), :] = found[half * 8 : half * 8 + 8]

    def top_part(plane, side, i):
        for odd in range(2):
            found = tp_all[plane, side, i * 32 + odd * 16 : i * 32 + odd * 16 + 16, :].astype(F32)
            first = ((2 * plane + odd) * 16 + (i * 2 + side)) * 16
            p_top[pl.ds(pl.multiple_of(first, 16), 16), :] = found

    ahead = 10
    z_left, z_right, z_far = t_spread.left, t_spread.right, t_spread.far
    away = 1 - core
    middle(0, 0)
    middle(1, 1)
    tp_spread.forward()
    t_spread.forward()
    tp_spread.forward_rest()
    t_spread.forward_rest()

    def tables2(i):
        offset_part(z, core, i)
        offset_part(z_left, core, i)
        top_part(z_left, core, i)

    middle(2, 0, True, tables2)
    t_spread.take(0)
    tp_spread.take(0)

    def tables3(i):
        offset_part(z_right, core, i)
        offset_part(z, away, i)
        top_part(z_right, core, i)
        top_part(z, away, i)

    middle(3, 1, True, tables3)
    t_spread.take(1)
    t_spread.take(2)
    tp_spread.take(1)
    tp_spread.take(2)

    def tables4(i):
        offset_part(z_left, away, i)
        offset_part(z_right, away, i)
        top_part(z_left, away, i)
        top_part(z_right, away, i)

    middle(4, 0, True, tables4)
    middle(5, 1)
    middle(6, 0)
    tp_spread.forward_far()
    t_spread.forward_far()

    def tables7(i):
        offset_part(z_far, core, i)
        top_part(z_far, core, i)

    middle(7, 1, True, tables7)
    middle(8, 0)
    t_spread.take(3)
    tp_spread.take(3)

    def tables9(i):
        offset_part(z_far, away, i)
        top_part(z_far, away, i)

    middle(9, 1, True, tables9)

    behind = (trans_top_ref.shape[0] // 2) * 8

    def top_box(k):
        row = (k % 2) * 8 + k // 2
        sums = [jnp.zeros((8, LANES), F32) for _ in range(4)]
        for j in range(entries):
            n = near_top[row, j]
            o = near_top[row, entries + j]
            pr = p_top[pl.ds(n, 8), :]
            pi = p_top[pl.ds(n + 8, 8), :]
            tr = t_top[pl.ds(o, 8), :]
            ti = t_top[pl.ds(o + behind, 8), :]
            sums = [sums[0] + pr * tr, sums[1] + pi * ti, sums[2] + pr * ti, sums[3] + pi * tr]
        real = (sums[0] - sums[1]).astype(BF16).astype(F32)
        imag = (sums[2] + sums[3]).astype(BF16).astype(F32)
        top_sum[k * 16 : k * 16 + 8, :] = real
        top_sum[k * 16 + 8 : k * 16 + 16, :] = imag

    for k in range(SECTORS):
        top_box(k)

    def top_children(part, carry):
        lanes = pl.ds(pl.multiple_of(part * LANES, LANES), LANES)
        c = cos_top[pl.ds(part, 8, stride=8), :]
        n = sin_top[pl.ds(part, 8, stride=8), :]
        for pair in range(8):
            reals = []
            imags = []
            for half in range(2):
                first = pair * 32 + half * 16
                real = jnp.broadcast_to(top_sum[pl.ds(first + part, 1), :], (8, LANES))
                imag = jnp.broadcast_to(top_sum[pl.ds(first + 8 + part, 1), :], (8, LANES))
                reals.append(real * c + imag * n)
                imags.append(imag * c - real * n)
            child_rows[pair * 16 : pair * 16 + 16, lanes] = jnp.concatenate(reals, axis=0).astype(BF16)
            child_rows[128 + pair * 16 : 144 + pair * 16, lanes] = jnp.concatenate(imags, axis=0).astype(BF16)
        return carry

    lax.fori_loop(0, 8, top_children, 0)
    scale = interp_top.shape[0] / interp_top.shape[1]
    down[...] = scale * lax.dot_general(
        child_rows[...], interp_top[...], (((1,), (1,)), ((), ())), preferred_element_type=F32
    )

    def back_copy(s, landing):
        return pltpu.make_async_remote_copy(
            src_ref=pieces.at[s],
            dst_ref=received.at[landing],
            send_sem=back_send.at[s],
            recv_sem=back_recv.at[landing],
            device_id=to_sector(s),
            device_id_type=MESH,
        )

    def combine(n):
        k = nth(n)
        at = pl.multiple_of(k * 8, 8)
        sides = []
        for side in range(2):
            lanes = slice(side * LANES, side * LANES + LANES)
            parts = [mid_sum[pl.ds(n * 64 + side + 2 * quarter, 8, stride=8), :] for quarter in range(4)]
            real = (parts[0] - parts[3]) + down[pl.ds(at, 8), lanes]
            imag = (parts[1] + parts[2]) + down[pl.ds(pl.multiple_of(128 + k * 8, 8), 8), lanes]
            sides.append(jnp.concatenate([real, imag], axis=0).astype(BF16))
        return jnp.concatenate(sides, axis=1)

    def make_children(s, at):
        columns = pl.ds(pl.multiple_of(s * 256, 256), 256)
        c = cos_mid[:, columns]
        n = sin_mid[:, columns]
        found = received[s].astype(F32)
        target = pl.ds(pl.multiple_of(at * 256, 256), 256)
        for pair in range(4):
            reals = []
            imags = []
            for half in range(2):
                box = pair * 2 + half
                real = jnp.broadcast_to(found[box : box + 1], (8, 256))
                imag = jnp.broadcast_to(found[8 + box : 9 + box], (8, 256))
                reals.append(real * c + imag * n)
                imags.append(imag * c - real * n)
            children[pair * 16 : pair * 16 + 16, target] = jnp.concatenate(reals, axis=0).astype(BF16)
            children[64 + pair * 16 : 80 + pair * 16, target] = jnp.concatenate(imags, axis=0).astype(BF16)

    def take_piece(piece_at, count):
        at = apart(group, piece_at)
        for slot in range(count):
            s = at * 4 + apart(inside, slot)
            back_copy(s, s).wait_recv()
        for slot in range(4):
            make_children(at * 4 + slot, slot)

    block = 512

    def product(at, k):
        columns = pl.ds(pl.multiple_of(at * 1024, 1024), 1024)
        rows_at = pl.ds(k * block, block)
        return lax.dot_general(
            weights[rows_at, columns], children[...], (((1,), (1,)), ((), ())), preferred_element_type=F32
        )

    def finish_piece(piece_at, carry):
        take_piece(piece_at, 4)
        for k in range(total.shape[0] // block):
            total[k * block : k * block + block, :] += product(apart(group, piece_at), k)
        return carry

    def send_back(k, carry):
        s = nth(k)
        pieces[s] = combine(k)
        back_copy(s, sector).start()
        return carry

    def pair_and_send(pair_at, carry):
        for parity in range(2):
            middle(pair_at * 2 + parity, parity)
            send_back(pair_at * 2 + parity, carry)
        return carry

    lax.fori_loop(0, ahead, send_back, 0)
    lax.fori_loop(ahead // 2, SECTORS // 2 - 1, pair_and_send, 0)
    middle(SECTORS - 2, 0, False)
    send_back(SECTORS - 2, 0)
    middle(SECTORS - 1, 1, False)
    received[sector] = combine(SECTORS - 1)
    lax.fori_loop(0, 3, finish_piece, 0)
    take_piece(3, 3)
    half_rows = out_ref.shape[1]
    for k in range(total.shape[0] // block):
        part = product(group, k)
        for n in range(k * block // 256, (k + 1) * block // 256):
            rows_at = slice(n * 256, n * 256 + 256)
            turned = jnp.transpose(total[rows_at, :] + part[n * 256 - k * block : n * 256 - k * block + 256])
            for which in range(2):
                out_ref[which, :, rows_at] = turned[which * half_rows : which * half_rows + half_rows]

    def wait_sent(k, carry):
        s = other(k)
        a2a_copy(s, sector).wait_send()
        back_copy(s, sector).wait_send()
        return carry

    lax.fori_loop(0, SECTORS - 1, wait_sent, 0)

    @pl.when(own)
    def _():
        for index in range(3):
            share_copy(index).wait_send()

    for each in (t_spread, p_spread, tp_spread):
        each.sent()


def on_device(
    leaf_out,
    interp_mid,
    shift_mid,
    trans_mid,
    list_mid,
    offset_mid,
    interp_top,
    shift_top,
    trans_top,
    list_top,
    offset_top,
):
    offsets = trans_mid.shape[1]
    entries = list_mid.shape[1]
    rows = 2 * leaf_out.shape[1]
    operands = (
        leaf_out,
        interp_mid,
        shift_mid,
        trans_top.reshape(2 * offsets, LANES),
        jnp.transpose(trans_mid.reshape(2, offsets, 2, LANES), (1, 2, 0, 3)).reshape(4 * offsets, LANES),
        interp_top[0],
        shift_top.reshape(64, LANES),
        list_mid.T,
        offset_mid.T,
        list_top.T,
        offset_top.T,
    )
    padded = 640
    result = pl.pallas_call(
        kernel,
        out_shape=VMEM(leaf_out.shape, F32),
        in_specs=[pl.BlockSpec(memory_space=pltpu.HBM)] * len(operands),
        out_specs=pl.BlockSpec(memory_space=VMEM),
        scratch_shapes=[
            VMEM(leaf_out.shape, BF16),
            VMEM(interp_mid.shape, BF16),
            VMEM(shift_mid.shape, F32),
            VMEM((2 * offsets, LANES), F32),
            VMEM((4 * offsets, LANES), F32),
            VMEM((256, 1024), BF16),
            VMEM((64, LANES), F32),
            VMEM((2, entries, 256), jnp.int32),
            VMEM((2, entries, 128), jnp.int32),
            VMEM((64, 4, 2 * entries), jnp.int32),
            VMEM((128, 2 * entries), jnp.int32),
            pltpu.SMEM((4, 4, 2 * entries), jnp.int32),
            VMEM((16, 2 * entries), jnp.int32),
            pltpu.SMEM((16, 2 * entries), jnp.int32),
            VMEM((PLANES, 2, 512, LANES), BF16),
            VMEM((PLANES, 2, 256, LANES), BF16),
            VMEM((PLANES, 2, padded, LANES), BF16),
            VMEM((rows, interp_mid.shape[0]), BF16),
            VMEM(shift_mid.shape, F32),
            VMEM(shift_mid.shape, F32),
            VMEM((SECTORS, 32, LANES), BF16),
            VMEM((128, LANES), F32),
            VMEM((padded, LANES), BF16),
            VMEM((512, LANES), F32),
            VMEM((256, 256), BF16),
            VMEM((256, LANES), F32),
            VMEM((64, LANES), F32),
            VMEM((64, LANES), F32),
            VMEM((1024 * 8, LANES), F32),
            VMEM((offsets * 8, LANES), F32),
            VMEM((128 * 16, LANES), F32),
            VMEM((padded * 8, LANES), F32),
            VMEM((128 * 8, LANES), F32),
            VMEM((16 * 16, LANES), F32),
            VMEM((256, 1024), BF16),
            VMEM((256, 256), F32),
            VMEM((SECTORS, 16, 256), BF16),
            VMEM((SECTORS, 16, 256), BF16),
            VMEM((rows, 1024), BF16),
            VMEM((interp_mid.shape[0], rows), F32),
            DMA((16,)),
            DMA((7,)),
            DMA((2,)),
            DMA((4,)),
            DMA((SECTORS,)),
            DMA((SECTORS,)),
            DMA((2,)),
            DMA((3,)),
            DMA((3,)),
            DMA((10,)),
            DMA((10,)),
            DMA((10,)),
            DMA((10,)),
            DMA((10,)),
            DMA((10,)),
            DMA((SECTORS,)),
            DMA((SECTORS,)),
        ],
        compiler_params=pltpu.CompilerParams(
            collective_id=0, has_side_effects=True, vmem_limit_bytes=60 * 1024 * 1024
        ),
        name="far_field",
    )(*operands)
    return result * (interp_mid.shape[0] / interp_mid.shape[1])


def solution(mesh):
    return jax.shard_map(
        on_device,
        mesh=mesh,
        in_specs=(
            P(None, ("box", "dir"), None),
            P(),
            P(),
            P(None, None, "dir"),
            P(),
            P(),
            P("dir", None, None),
            P(None, "dir", None),
            P(None, None, "dir", "box"),
            P(),
            P(),
        ),
        out_specs=P(None, ("box", "dir"), None),
        check_vma=False,
    )
```

```python
import jax
import jax.numpy as jnp
from jax import lax
from jax.experimental import pallas as pl
from jax.experimental.pallas import tpu as pltpu
from jax.sharding import PartitionSpec as P

MESH = pl.DeviceIdType.MESH
F32 = jnp.float32
BF16 = jnp.bfloat16
VMEM = pltpu.VMEM
DMA = pltpu.SemaphoreType.DMA
PLANES = 4
SECTORS = 16
LANES = 128


def place():
    box = lax.axis_index("box")
    way = lax.axis_index("dir")
    low = box % 2
    core = way % 2
    return box // 2, way - core + low, core


def device_of(plane, sector, core):
    low = sector % 2
    return (plane * 2 + low, sector - low + core)


def sin_cos(angle):
    half = angle * 0.5
    sq = half * half
    s = sq * (-1.0 / 39916800.0) + (1.0 / 362880.0)
    s = sq * s - (1.0 / 5040.0)
    s = sq * s + (1.0 / 120.0)
    s = sq * s - (1.0 / 6.0)
    s = half + half * (sq * s)
    c = sq * (1.0 / 479001600.0) - (1.0 / 3628800.0)
    c = sq * c + (1.0 / 40320.0)
    c = sq * c - (1.0 / 720.0)
    c = sq * c + (1.0 / 24.0)
    c = sq * c - 0.5
    c = sq * c + 1.0
    return 2.0 * s * c, 1.0 - 2.0 * s * s


class Spread:
    def __init__(self, ref, send, recv):
        z, sector, core = place()
        self.ref, self.send, self.recv = ref, send, recv
        self.core = core
        self.z = z
        self.left = (z + PLANES - 1) % PLANES
        self.right = (z + 1) % PLANES
        self.far = (z + 2) % PLANES
        self.to_right = device_of(self.right, sector, core)
        self.to_left = device_of(self.left, sector, core)
        self.partner = device_of(z, sector, 1 - core)
        self.rows = ref.shape[2]
        self.crossing = ((4, self.z), (5, self.left), (6, self.right), (7, self.far))

    def copy(self, plane, core, half, index, target):
        rows = self.rows
        if half is None:
            part = self.ref.at[plane, core]
        else:
            part = self.ref.at[plane, core, pl.ds(half * (rows // 2), rows // 2)]
        return pltpu.make_async_remote_copy(
            src_ref=part,
            dst_ref=part,
            send_sem=self.send.at[index],
            recv_sem=self.recv.at[index],
            device_id=target,
            device_id_type=MESH,
        )

    def start_own(self):
        self.copy(self.z, self.core, 0, 0, self.to_right).start()
        self.copy(self.z, self.core, 1, 1, self.to_left).start()
        self.copy(self.z, self.core, 1, 8, self.to_right).start()
        self.copy(self.z, self.core, 0, 9, self.to_left).start()
        self.copy(self.z, self.core, None, 4, self.partner).start()

    def forward(self):
        self.copy(self.left, self.core, 0, 0, self.to_right).wait_recv()
        self.copy(self.left, self.core, 0, 2, self.to_right).start()
        self.copy(self.right, self.core, 1, 1, self.to_left).wait_recv()
        self.copy(self.right, self.core, 1, 3, self.to_left).start()

    def forward_rest(self):
        self.copy(self.left, self.core, 1, 8, self.to_right).wait_recv()
        self.copy(self.left, self.core, None, 5, self.partner).start()
        self.copy(self.right, self.core, 0, 9, self.to_left).wait_recv()
        self.copy(self.right, self.core, None, 6, self.partner).start()

    def forward_far(self):
        self.copy(self.far, self.core, 0, 2, self.to_right).wait_recv()
        self.copy(self.far, self.core, 1, 3, self.to_left).wait_recv()
        self.copy(self.far, self.core, None, 7, self.partner).start()

    def take(self, which):
        index, plane = self.crossing[which]
        self.copy(plane, 1 - self.core, None, index, self.partner).wait_recv()
        return plane

    def sent(self):
        self.copy(self.z, self.core, 0, 0, self.to_right).wait_send()
        self.copy(self.z, self.core, 1, 1, self.to_left).wait_send()
        self.copy(self.z, self.core, 1, 8, self.to_right).wait_send()
        self.copy(self.z, self.core, 0, 9, self.to_left).wait_send()
        self.copy(self.left, self.core, 0, 2, self.to_right).wait_send()
        self.copy(self.right, self.core, 1, 3, self.to_left).wait_send()
        for index, plane in self.crossing:
            self.copy(plane, self.core, None, index, self.partner).wait_send()


def kernel(
    leaf_ref,
    matrix_ref,
    shift_mid_ref,
    trans_top_ref,
    trans_mid_ref,
    interp_top_ref,
    shift_top_ref,
    list_mid_ref,
    offset_mid_ref,
    list_top_ref,
    offset_top_ref,
    out_ref,
    leaf,
    weights,
    shift_mid,
    trans_top,
    trans_mid,
    interp_top,
    shift_top,
    lists_mid,
    lists_top,
    scaled_mid,
    scaled_top,
    near,
    own_top,
    near_top,
    p_all,
    tp_all,
    t_all,
    leaf_rows,
    cos_mid,
    sin_mid,
    sending,
    stage,
    piece,
    block_f32,
    top_lhs,
    top_f32,
    cos_top,
    sin_top,
    p_tab,
    t_tab,
    p_top,
    t_top,
    mid_sum,
    top_sum,
    child_rows,
    down,
    pieces,
    received,
    children,
    total,
    weight_sem,
    load_sem,
    index_sem,
    near_sem,
    a2a_send,
    a2a_recv,
    swap_sem,
    share_send,
    share_recv,
    t_send,
    t_recv,
    p_send,
    p_recv,
    tp_send,
    tp_recv,
    back_send,
    back_recv,
):
    z, sector, core = place()
    entries = list_mid_ref.shape[0]
    low = sector % 2
    own = low == core
    partner = device_of(z, sector, 1 - core)
    swap = device_of(z, sector - low + core, low)
    right = device_of((z + 1) % PLANES, sector, core)
    left = device_of((z + PLANES - 1) % PLANES, sector, core)
    t_spread = Spread(t_all, t_send, t_recv)
    p_spread = Spread(p_all, p_send, p_recv)
    tp_spread = Spread(tp_all, tp_send, tp_recv)

    group = sector // 4
    inside = sector % 4

    def apart(a, k):
        high = (a // 2 + k + 1) % 2
        return high * 2 + (a % 2 + 1 + k // 2) % 2

    def nth(k):
        return apart(group, k // 4) * 4 + apart(inside, k % 4)

    def other(k):
        return (sector + 1 + k) % SECTORS

    def to_sector(s):
        return device_of(z, s, core)

    barrier = pltpu.get_barrier_semaphore()

    def signal_peer(k, carry):
        pl.semaphore_signal(barrier, inc=1, device_id=to_sector(other(k)), device_id_type=MESH)
        return carry

    lax.fori_loop(0, SECTORS - 1, signal_peer, 0)
    for device in (right, left, partner):
        pl.semaphore_signal(barrier, inc=1, device_id=device, device_id_type=MESH)

    @pl.when(jnp.logical_not(own))
    def _():
        pl.semaphore_signal(barrier, inc=1, device_id=swap, device_id_type=MESH)

    slab = pl.ds(pl.multiple_of(z * 256, 256), 256)
    loads = [
        pltpu.make_async_copy(source, target, load_sem.at[index])
        for index, (source, target) in enumerate(
            (
                (leaf_ref, leaf),
                (trans_top_ref, trans_top),
                (shift_mid_ref, shift_mid),
                (list_mid_ref.at[:, slab], lists_mid.at[0]),
                (offset_mid_ref.at[:, slab], lists_mid.at[1]),
                (list_top_ref, lists_top.at[0]),
                (offset_top_ref, lists_top.at[1]),
            )
        )
    ]
    for copy in loads[:3]:
        copy.start()

    def weight_copies(piece_at):
        columns = pl.ds(pl.multiple_of(apart(group, piece_at) * 1024, 1024), 1024)
        size = matrix_ref.shape[0] // 4
        return [
            pltpu.make_async_copy(
                matrix_ref.at[part * size : part * size + size, columns],
                weights.at[part * size : part * size + size, columns],
                weight_sem.at[piece_at * 4 + part],
            )
            for part in range(4)
        ]

    for copy in weight_copies(0):
        copy.start()

    loads[0].wait()
    for copy in weight_copies(1):
        copy.start()
    rows = 2 * leaf.shape[1]
    target = lax.broadcasted_iota(jnp.int32, (rows, rows), 0)
    source = lax.broadcasted_iota(jnp.int32, (rows, rows), 1)
    wanted = (target & 64) + ((target & 7) << 3) + ((target >> 3) & 7)
    order = (source == wanted).astype(BF16)
    both = jnp.concatenate([leaf[0], leaf[1]], axis=0)
    leaf_rows[...] = jnp.dot(order, both, preferred_element_type=F32).astype(BF16)

    loads[1].wait()
    for piece_at in (2, 3):
        for copy in weight_copies(piece_at):
            copy.start()
    for copy in loads[3:]:
        copy.start()
    used = trans_top.shape[0]
    piece[0:used, :] = trans_top[...].astype(BF16)
    piece[used:, :] = jnp.zeros((piece.shape[0] - used, LANES), BF16)

    swap_copy = pltpu.make_async_remote_copy(
        src_ref=piece,
        dst_ref=t_all.at[z, low],
        send_sem=swap_sem.at[0],
        recv_sem=swap_sem.at[1],
        device_id=swap,
        device_id_type=MESH,
    )
    shared = ((trans_mid_ref, trans_mid), (interp_top_ref, interp_top), (shift_top_ref, shift_top))

    def share_copy(index):
        return pltpu.make_async_remote_copy(
            src_ref=shared[index][0],
            dst_ref=shared[index][1],
            send_sem=share_send.at[index],
            recv_sem=share_recv.at[index],
            device_id=partner,
            device_id_type=MESH,
        )

    def local_copy(index):
        return pltpu.make_async_copy(shared[index][0], shared[index][1], share_recv.at[index])

    loads[2].wait()
    sines, cosines = sin_cos(shift_mid[...])
    cos_mid[...] = cosines
    sin_mid[...] = sines

    def parents(s, slot):
        columns = pl.ds(pl.multiple_of(s * 256, 256), 256)
        spread = jnp.dot(leaf_rows[...], weights[:, columns], preferred_element_type=F32)
        real_sum = jnp.zeros((8, 256), F32)
        imag_sum = jnp.zeros((8, 256), F32)
        for child in range(8):
            real = spread[child * 8 : child * 8 + 8]
            imag = spread[64 + child * 8 : 64 + child * 8 + 8]
            c = cos_mid[child : child + 1, columns]
            n = sin_mid[child : child + 1, columns]
            real_sum += real * c - imag * n
            imag_sum += real * n + imag * c
        for part in range(2):
            lanes = slice(part * LANES, part * LANES + LANES)
            stage[pl.ds(slot * 32 + part, 8, stride=4), :] = real_sum[:, lanes]
            stage[pl.ds(slot * 32 + 2 + part, 8, stride=4), :] = imag_sum[:, lanes]
        return stage[slot * 32 : slot * 32 + 32, :].astype(BF16)

    def rows_of(s):
        return p_all.at[z, core, pl.ds(pl.multiple_of(s * 32, 32), 32)]

    def a2a_copy(s, landing):
        return pltpu.make_async_remote_copy(
            src_ref=sending.at[s],
            dst_ref=rows_of(landing),
            send_sem=a2a_send.at[s],
            recv_sem=a2a_recv.at[landing],
            device_id=to_sector(s),
            device_id_type=MESH,
        )

    def make_four(piece_at):
        for copy in weight_copies(piece_at):
            copy.wait()
        for slot in range(4):
            s = nth(piece_at * 4 + slot)
            sending[s] = parents(s, slot)

    def start_four(piece_at):
        for slot in range(4):
            a2a_copy(nth(piece_at * 4 + slot), sector).start()

    make_four(0)
    pl.semaphore_wait(barrier, SECTORS - 1 + 3 + (low + core) % 2)

    @pl.when(own)
    def _():
        for index in range(3):
            share_copy(index).start()
            local_copy(index).start()
        t_all[z, core] = piece[...]
        t_spread.start_own()

    @pl.when(jnp.logical_not(own))
    def _():
        swap_copy.start()

    start_four(0)

    def send_four(piece_at, carry):
        make_four(piece_at)
        start_four(piece_at)
        return carry

    lax.fori_loop(1, 3, send_four, 0)
    for copy in weight_copies(3):
        copy.wait()
    for slot in range(3):
        s = nth(12 + slot)
        sending[s] = parents(s, slot)
    p_all[z, core, pl.ds(pl.multiple_of(sector * 32, 32), 32), :] = parents(sector, 3)
    for slot in range(3):
        a2a_copy(nth(12 + slot), sector).start()

    total[...] = jnp.zeros_like(total)

    for copy in loads[3:]:
        copy.wait()
    scaled = jnp.transpose(jnp.concatenate([lists_mid[0], lists_mid[1]], axis=0) * 8)
    for quad_at in range(64):
        scaled_mid[quad_at] = scaled[quad_at * 4 : quad_at * 4 + 4]
    scaled = jnp.transpose(jnp.concatenate([lists_top[0] * 16, lists_top[1] * 8], axis=0))
    scaled_top[...] = scaled
    own_top[...] = scaled_top[pl.ds(z * 32 + core, 16, stride=2), :]
    to_smem = [pltpu.make_async_copy(own_top, near_top, index_sem.at[0])]
    for copy in to_smem:
        copy.start()

    def fetch(k, slot):
        s = nth(k)
        odd = s % 2
        quad_at = odd * 32 + (s - odd + core) * 2 + slot % 2
        return pltpu.make_async_copy(scaled_mid.at[quad_at], near.at[slot], near_sem.at[slot])

    for slot in range(4):
        fetch(slot // 2, slot).start()

    @pl.when(own)
    def _():
        for index in range(3):
            local_copy(index).wait()

    @pl.when(jnp.logical_not(own))
    def _():
        for index in range(3):
            share_copy(index).wait_recv()

    offsets = trans_mid.shape[0] // 4

    def put_offsets(first, row):
        for quarter, places in enumerate(((0, 2), (4, 6), (1, 3), (5, 7))):
            v = trans_mid[pl.ds(first + quarter, 8, stride=4), :]
            for at in places:
                t_tab[pl.ds(row + at, 8, stride=8), :] = v

    def mid_offsets(k, carry):
        put_offsets(pl.multiple_of(k * 32, 32), pl.multiple_of(k * 64, 64))
        return carry

    lax.fori_loop(0, offsets // 8, mid_offsets, 0)
    if offsets % 8:
        put_offsets((offsets - 8) * 4, (offsets - 8) * 8)

    sines_t, cosines_t = sin_cos(shift_top[...])
    cos_top[...] = cosines_t
    sin_top[...] = sines_t

    def wait_sector(k, carry):
        s = other(k)
        a2a_copy(s, s).wait_recv()
        return carry

    lax.fori_loop(0, SECTORS - 1, wait_sector, 0)
    p_spread.start_own()

    block_f32[...] = p_all[z, core].astype(F32)
    for child in range(8):
        for part in range(2):
            for side in range(2):
                first = child * 4 + part * 2 + side
                a = block_f32[pl.ds(first, 8, stride=32), :]
                b = block_f32[pl.ds(256 + first, 8, stride=32), :]
                top_lhs[
                    part * 128 + child * 16 : part * 128 + child * 16 + 16, side * LANES : side * LANES + LANES
                ] = jnp.concatenate([a, b], axis=0).astype(BF16)

    def top_columns(k, carry):
        columns = pl.ds(pl.multiple_of(k * 256, 256), 256)
        spread = jnp.dot(top_lhs[...], interp_top[:, columns], preferred_element_type=F32)
        for part in range(2):
            lanes = slice(part * LANES, part * LANES + LANES)
            group = k * 2 + part
            real_sum = jnp.zeros((16, LANES), F32)
            imag_sum = jnp.zeros((16, LANES), F32)
            for child in range(8):
                real = spread[child * 16 : child * 16 + 16, lanes]
                imag = spread[128 + child * 16 : 128 + child * 16 + 16, lanes]
                c = cos_top[pl.ds(child * 8 + group, 1), :]
                n = sin_top[pl.ds(child * 8 + group, 1), :]
                real_sum += real * c - imag * n
                imag_sum += real * n + imag * c
            for half in range(2):
                boxes = slice(half * 8, half * 8 + 8)
                top_f32[pl.ds(half * 128 + group, 8, stride=16), :] = real_sum[boxes]
                top_f32[pl.ds(half * 128 + 8 + group, 8, stride=16), :] = imag_sum[boxes]
        return carry

    lax.fori_loop(0, 4, top_columns, 0)
    tp_all[z, core] = top_f32[...].astype(BF16)

    upper = lax.broadcasted_iota(jnp.int32, (8, LANES), 0) < 4

    def mid_table(plane, side):
        def four(k, carry):
            for part in range(4):
                odd = part % 2
                found = p_all[plane, side, pl.ds(pl.multiple_of(k * 128 + part * 32, 32), 32), :].astype(F32)
                first = ((2 * plane + odd) * 128 + (k * 4 + part - odd + side) * 8) * 8
                for pair in range(4):
                    v = found[pair * 8 : pair * 8 + 8]
                    r = pltpu.roll(v, 4, 0)
                    at = first + pair * 16
                    p_tab[pl.ds(pl.multiple_of(at, 8), 8), :] = jnp.where(upper, v, r)
                    p_tab[pl.ds(pl.multiple_of(at + 8, 8), 8), :] = jnp.where(upper, r, v)
            return carry

        lax.fori_loop(0, SECTORS // 4, four, 0)

    def top_table(plane, side):
        def four(k, carry):
            for part in range(4):
                odd = part % 2
                found = tp_all[plane, side, pl.ds(pl.multiple_of(k * 64 + part * 16, 16), 16), :].astype(F32)
                first = ((2 * plane + odd) * 16 + (k * 4 + part - odd + side)) * 16
                p_top[pl.ds(pl.multiple_of(first, 16), 16), :] = found
            return carry

        lax.fori_loop(0, SECTORS // 4, four, 0)

    mid_table(z, core)
    top_table(z, core)
    p_spread.forward()
    tp_spread.start_own()

    @pl.when(jnp.logical_not(own))
    def _():
        swap_copy.wait()
        t_spread.start_own()

    p_spread.forward_rest()

    mid_table(p_spread.left, core)
    mid_table(p_spread.right, core)
    mid_table(p_spread.take(0), 1 - core)
    for copy in to_smem:
        copy.wait()
    p_spread.forward_far()
    mid_table(p_spread.far, core)
    mid_table(p_spread.take(1), 1 - core)
    mid_table(p_spread.take(2), 1 - core)
    mid_table(p_spread.take(3), 1 - core)

    def middle(k, parity, more=True, beside=None):
        for half in range(2):
            slot = parity * 2 + half
            fetch(k, slot).wait()
            for i in range(4):
                box = half * 4 + i
                kept = jnp.zeros((8, LANES), F32)
                for j in range(entries):
                    p = p_tab[pl.ds(near[slot, i, j], 8), :]
                    t = t_tab[pl.ds(near[slot, i, entries + j], 8), :]
                    kept = kept + p * t
                mid_sum[pl.ds(pl.multiple_of(k * 64 + box * 8, 8), 8), :] = kept
                if beside is not None:
                    beside(box)
            if more:
                fetch(k + 2, slot).start()

    def offset_part(plane, side, i):
        at = plane * 2 + side
        for part in range(t_all.shape[2] // 128):
            row = i * (t_all.shape[2] // 8) + part * 16
            found = t_all[plane, side, row : row + 16, :].astype(F32)
            for half in range(2):
                t_top[pl.ds(row * 8 + half * 64 + at, 8, stride=8), :] = found[half * 8 : half * 8 + 8]

    def top_part(plane, side, i):
        for odd in range(2):
            found = tp_all[plane, side, i * 32 + odd * 16 : i * 32 + odd * 16 + 16, :].astype(F32)
            first = ((2 * plane + odd) * 16 + (i * 2 + side)) * 16
            p_top[pl.ds(pl.multiple_of(first, 16), 16), :] = found

    ahead = 10
    z_left, z_right, z_far = t_spread.left, t_spread.right, t_spread.far
    away = 1 - core
    middle(0, 0)
    tp_spread.forward()
    t_spread.forward()
    tp_spread.forward_rest()
    t_spread.forward_rest()

    middle(1, 1)

    def tables2(i):
        offset_part(z, core, i)
        offset_part(z_left, core, i)
        top_part(z_left, core, i)

    middle(2, 0, True, tables2)
    t_spread.take(0)
    tp_spread.take(0)

    def tables3(i):
        offset_part(z_right, core, i)
        offset_part(z, away, i)
        top_part(z_right, core, i)
        top_part(z, away, i)

    middle(3, 1, True, tables3)
    t_spread.take(1)
    t_spread.take(2)
    tp_spread.take(1)
    tp_spread.take(2)

    def tables4(i):
        offset_part(z_left, away, i)
        offset_part(z_right, away, i)
        top_part(z_left, away, i)
        top_part(z_right, away, i)

    middle(4, 0, True, tables4)
    middle(5, 1)
    middle(6, 0)
    tp_spread.forward_far()
    t_spread.forward_far()

    def tables7(i):
        offset_part(z_far, core, i)
        top_part(z_far, core, i)

    middle(7, 1, True, tables7)
    middle(8, 0)
    t_spread.take(3)
    tp_spread.take(3)

    def tables9(i):
        offset_part(z_far, away, i)
        top_part(z_far, away, i)

    middle(9, 1, True, tables9)

    behind = (trans_top_ref.shape[0] // 2) * 8

    def top_box(k):
        row = (k % 2) * 8 + k // 2
        sums = [jnp.zeros((8, LANES), F32) for _ in range(4)]
        for j in range(entries):
            n = near_top[row, j]
            o = near_top[row, entries + j]
            pr = p_top[pl.ds(n, 8), :]
            pi = p_top[pl.ds(n + 8, 8), :]
            tr = t_top[pl.ds(o, 8), :]
            ti = t_top[pl.ds(o + behind, 8), :]
            sums = [sums[0] + pr * tr, sums[1] + pi * ti, sums[2] + pr * ti, sums[3] + pi * tr]
        real = (sums[0] - sums[1]).astype(BF16).astype(F32)
        imag = (sums[2] + sums[3]).astype(BF16).astype(F32)
        top_sum[k * 16 : k * 16 + 8, :] = real
        top_sum[k * 16 + 8 : k * 16 + 16, :] = imag

    for k in range(SECTORS):
        top_box(k)

    def top_children(part, carry):
        lanes = pl.ds(pl.multiple_of(part * LANES, LANES), LANES)
        c = cos_top[pl.ds(part, 8, stride=8), :]
        n = sin_top[pl.ds(part, 8, stride=8), :]
        for pair in range(8):
            reals = []
            imags = []
            for half in range(2):
                first = pair * 32 + half * 16
                real = jnp.broadcast_to(top_sum[pl.ds(first + part, 1), :], (8, LANES))
                imag = jnp.broadcast_to(top_sum[pl.ds(first + 8 + part, 1), :], (8, LANES))
                reals.append(real * c + imag * n)
                imags.append(imag * c - real * n)
            child_rows[pair * 16 : pair * 16 + 16, lanes] = jnp.concatenate(reals, axis=0).astype(BF16)
            child_rows[128 + pair * 16 : 144 + pair * 16, lanes] = jnp.concatenate(imags, axis=0).astype(BF16)
        return carry

    lax.fori_loop(0, 8, top_children, 0)
    scale = interp_top.shape[0] / interp_top.shape[1]
    down[...] = scale * lax.dot_general(
        child_rows[...], interp_top[...], (((1,), (1,)), ((), ())), preferred_element_type=F32
    )

    def back_copy(s, landing):
        return pltpu.make_async_remote_copy(
            src_ref=pieces.at[s],
            dst_ref=received.at[landing],
            send_sem=back_send.at[s],
            recv_sem=back_recv.at[landing],
            device_id=to_sector(s),
            device_id_type=MESH,
        )

    def combine(n):
        k = nth(n)
        at = pl.multiple_of(k * 8, 8)
        sides = []
        for side in range(2):
            lanes = slice(side * LANES, side * LANES + LANES)
            parts = [mid_sum[pl.ds(n * 64 + side + 2 * quarter, 8, stride=8), :] for quarter in range(4)]
            real = (parts[0] - parts[3]) + down[pl.ds(at, 8), lanes]
            imag = (parts[1] + parts[2]) + down[pl.ds(pl.multiple_of(128 + k * 8, 8), 8), lanes]
            sides.append(jnp.concatenate([real, imag], axis=0).astype(BF16))
        return jnp.concatenate(sides, axis=1)

    def make_children(s, at):
        columns = pl.ds(pl.multiple_of(s * 256, 256), 256)
        c = cos_mid[:, columns]
        n = sin_mid[:, columns]
        found = received[s].astype(F32)
        target = pl.ds(pl.multiple_of(at * 256, 256), 256)
        for pair in range(4):
            reals = []
            imags = []
            for half in range(2):
                box = pair * 2 + half
                real = jnp.broadcast_to(found[box : box + 1], (8, 256))
                imag = jnp.broadcast_to(found[8 + box : 9 + box], (8, 256))
                reals.append(real * c + imag * n)
                imags.append(imag * c - real * n)
            children[pair * 16 : pair * 16 + 16, target] = jnp.concatenate(reals, axis=0).astype(BF16)
            children[64 + pair * 16 : 80 + pair * 16, target] = jnp.concatenate(imags, axis=0).astype(BF16)

    def take_piece(piece_at, count):
        at = apart(group, piece_at)
        for slot in range(count):
            s = at * 4 + apart(inside, slot)
            back_copy(s, s).wait_recv()
        for slot in range(4):
            make_children(at * 4 + slot, slot)

    block = 512

    def product(at, k):
        columns = pl.ds(pl.multiple_of(at * 1024, 1024), 1024)
        rows_at = pl.ds(k * block, block)
        return lax.dot_general(
            weights[rows_at, columns], children[...], (((1,), (1,)), ((), ())), preferred_element_type=F32
        )

    def finish_piece(piece_at, carry):
        take_piece(piece_at, 4)
        for k in range(total.shape[0] // block):
            total[k * block : k * block + block, :] += product(apart(group, piece_at), k)
        return carry

    def send_back(k, carry):
        s = nth(k)
        pieces[s] = combine(k)
        back_copy(s, sector).start()
        return carry

    def pair_and_send(pair_at, carry):
        for parity in range(2):
            middle(pair_at * 2 + parity, parity)
            send_back(pair_at * 2 + parity, carry)
        return carry

    lax.fori_loop(0, ahead, send_back, 0)
    lax.fori_loop(ahead // 2, SECTORS // 2 - 1, pair_and_send, 0)
    middle(SECTORS - 2, 0, False)
    send_back(SECTORS - 2, 0)
    middle(SECTORS - 1, 1, False)
    received[sector] = combine(SECTORS - 1)
    lax.fori_loop(0, 3, finish_piece, 0)
    take_piece(3, 3)
    half_rows = out_ref.shape[1]
    for k in range(total.shape[0] // block):
        part = product(group, k)
        for n in range(k * block // 256, (k + 1) * block // 256):
            rows_at = slice(n * 256, n * 256 + 256)
            turned = jnp.transpose(total[rows_at, :] + part[n * 256 - k * block : n * 256 - k * block + 256])
            for which in range(2):
                out_ref[which, :, rows_at] = turned[which * half_rows : which * half_rows + half_rows]

    def wait_sent(k, carry):
        s = other(k)
        a2a_copy(s, sector).wait_send()
        back_copy(s, sector).wait_send()
        return carry

    lax.fori_loop(0, SECTORS - 1, wait_sent, 0)

    @pl.when(own)
    def _():
        for index in range(3):
            share_copy(index).wait_send()

    for each in (t_spread, p_spread, tp_spread):
        each.sent()


def on_device(
    leaf_out,
    interp_mid,
    shift_mid,
    trans_mid,
    list_mid,
    offset_mid,
    interp_top,
    shift_top,
    trans_top,
    list_top,
    offset_top,
):
    offsets = trans_mid.shape[1]
    entries = list_mid.shape[1]
    rows = 2 * leaf_out.shape[1]
    operands = (
        leaf_out,
        interp_mid,
        shift_mid,
        trans_top.reshape(2 * offsets, LANES),
        jnp.transpose(trans_mid.reshape(2, offsets, 2, LANES), (1, 2, 0, 3)).reshape(4 * offsets, LANES),
        interp_top[0],
        shift_top.reshape(64, LANES),
        list_mid.T,
        offset_mid.T,
        list_top.T,
        offset_top.T,
    )
    padded = 640
    result = pl.pallas_call(
        kernel,
        out_shape=VMEM(leaf_out.shape, F32),
        in_specs=[pl.BlockSpec(memory_space=pltpu.HBM)] * len(operands),
        out_specs=pl.BlockSpec(memory_space=VMEM),
        scratch_shapes=[
            VMEM(leaf_out.shape, BF16),
            VMEM(interp_mid.shape, BF16),
            VMEM(shift_mid.shape, F32),
            VMEM((2 * offsets, LANES), F32),
            VMEM((4 * offsets, LANES), F32),
            VMEM((256, 1024), BF16),
            VMEM((64, LANES), F32),
            VMEM((2, entries, 256), jnp.int32),
            VMEM((2, entries, 128), jnp.int32),
            VMEM((64, 4, 2 * entries), jnp.int32),
            VMEM((128, 2 * entries), jnp.int32),
            pltpu.SMEM((4, 4, 2 * entries), jnp.int32),
            VMEM((16, 2 * entries), jnp.int32),
            pltpu.SMEM((16, 2 * entries), jnp.int32),
            VMEM((PLANES, 2, 512, LANES), BF16),
            VMEM((PLANES, 2, 256, LANES), BF16),
            VMEM((PLANES, 2, padded, LANES), BF16),
            VMEM((rows, interp_mid.shape[0]), BF16),
            VMEM(shift_mid.shape, F32),
            VMEM(shift_mid.shape, F32),
            VMEM((SECTORS, 32, LANES), BF16),
            VMEM((128, LANES), F32),
            VMEM((padded, LANES), BF16),
            VMEM((512, LANES), F32),
            VMEM((256, 256), BF16),
            VMEM((256, LANES), F32),
            VMEM((64, LANES), F32),
            VMEM((64, LANES), F32),
            VMEM((1024 * 8, LANES), F32),
            VMEM((offsets * 8, LANES), F32),
            VMEM((128 * 16, LANES), F32),
            VMEM((padded * 8, LANES), F32),
            VMEM((128 * 8, LANES), F32),
            VMEM((16 * 16, LANES), F32),
            VMEM((256, 1024), BF16),
            VMEM((256, 256), F32),
            VMEM((SECTORS, 16, 256), BF16),
            VMEM((SECTORS, 16, 256), BF16),
            VMEM((rows, 1024), BF16),
            VMEM((interp_mid.shape[0], rows), F32),
            DMA((16,)),
            DMA((7,)),
            DMA((2,)),
            DMA((4,)),
            DMA((SECTORS,)),
            DMA((SECTORS,)),
            DMA((2,)),
            DMA((3,)),
            DMA((3,)),
            DMA((10,)),
            DMA((10,)),
            DMA((10,)),
            DMA((10,)),
            DMA((10,)),
            DMA((10,)),
            DMA((SECTORS,)),
            DMA((SECTORS,)),
        ],
        compiler_params=pltpu.CompilerParams(
            collective_id=0, has_side_effects=True, vmem_limit_bytes=60 * 1024 * 1024
        ),
        name="far_field",
    )(*operands)
    return result * (interp_mid.shape[0] / interp_mid.shape[1])


def solution(mesh):
    return jax.shard_map(
        on_device,
        mesh=mesh,
        in_specs=(
            P(None, ("box", "dir"), None),
            P(),
            P(),
            P(None, None, "dir"),
            P(),
            P(),
            P("dir", None, None),
            P(None, "dir", None),
            P(None, None, "dir", "box"),
            P(),
            P(),
        ),
        out_specs=P(None, ("box", "dir"), None),
        check_vma=False,
    )
```
